32 devices in a mesh: fsdp: 4 (over y, core), sp: 8 (over z, x).
Axes of the slice: x: 2, y: 2, z: 4, core: 2. Of those that a mesh axis runs over, the one named last changes fastest.
Arguments:
- hidden: bfloat16 [2048, 8192], P('sp', 'fsdp'), may hold values from -23 to 23
- w_query: bfloat16 [8192, 1024], P('fsdp', 'sp'), may hold values from -0.125 to 0.125
- w_keyvalue: bfloat16 [8192, 256], P('fsdp', 'sp'), may hold values from -0.125 to 0.125
- w_output: bfloat16 [1024, 8192], P('sp', 'fsdp'), may hold values from -0.75 to 0.75
- segment_ids: int32 [2048], P('sp'), may hold values from 0 to 7, never falling along the last dimension, each value on 1 to 512 neighbouring positions
Outputs:
- attended: bfloat16 [2048, 8192], P('sp', 'fsdp')
The draws below stay inside these ranges and needn't reach their ends.
Inputs may be any that keep to these rules, and one draw needn't show every extreme that they name: `segment_ids`: segment ids never fall along the sequence; every episode has between 1 and 512 tokens.
All inputs are finite; a program needn't handle non-finite values.
Results may differ from the reference program's by a relative error of at most 0.0085.
The reference program's roundings to bfloat16 on the way count: a program that leaves them out, or rounds other values in their place, can miss the bound.
Values may be sent and summed in bfloat16 or wider, within the bound.
A program may use at most 128 MiB of HBM per device.

```python
import math
import jax
import jax.numpy as jnp
import numpy as np
from jax import lax

D = 8192
HD = 128
GROUP = 8
HEADS = 8
KV_HEADS = 1
SEQ = 2048


def draw_hidden(key, part):
    base_key = jax.random.fold_in(jax.random.fold_in(key, 11), 0)
    entries = jnp.clip(jax.random.normal(base_key, (SEQ, D), jnp.float32), -6.0, 6.0)
    return entries.astype(jnp.bfloat16)


def steps_of(own_key, shape, pieces, low, largest):
    def one(position, blocks):
        heights = jax.random.uniform(jax.random.fold_in(jax.random.fold_in(own_key, 6), position), (blocks,), jnp.float32, low / len(pieces), largest / len(pieces))
        return jnp.repeat(jnp.exp(heights), shape[position] // blocks).reshape((-1,) + (1,) * (len(shape) - position - 1))

    loudness = one(*pieces[0])
    for cut in pieces[1:]:
        loudness = loudness * one(*cut)
    return loudness


def profile(count, total, limit, slope):
    weights = [(1 << 20) // math.isqrt(grade ** slope) + 1 for grade in range(2, count + 1)]
    surplus, holding = total - limit - (count - 1), [1] * (count - 1)
    while surplus > 0:
        candidates = [i for i in range(count - 1) if holding[i] < limit]
        pool, remaining = sum([weights[i] for i in candidates]), surplus
        for i in candidates:
            addition = min(limit - holding[i], max(1, remaining * weights[i] // pool), surplus)
            holding[i] = holding[i] + addition
            surplus = surplus - addition
    return np.array([limit] + holding)


def ragged_sizes(own_key, number_of, total, reach, skew):
    if number_of == 2:
        one = jax.random.randint(own_key, (), max(1, total - reach), min(reach, total - 1) + 1)
        return jnp.stack([one, total - one])
    lengths = jnp.asarray(profile(number_of, total, reach, skew), jnp.int32)
    couples = (number_of - 1) // 2
    source_of, sink = lengths[1:1 + 2 * couples:2], lengths[2:2 + 2 * couples:2]
    room = jnp.minimum(source_of - 1, reach - sink)
    shifted = jax.random.randint(jax.random.fold_in(own_key, 1), (couples,), 0, 1 << 20) % (room + 1)
    lengths = lengths.at[1:1 + 2 * couples:2].set(source_of - shifted).at[2:2 + 2 * couples:2].set(sink + shifted)
    return lengths[jax.random.permutation(jax.random.fold_in(own_key, 2), number_of)]


def scatter_about(own_key, dims, spread, bound, pieces=(), held_as=jnp.bfloat16):
    values = jax.random.normal(own_key, dims, jnp.float32) * spread
    if len(pieces) > 0:
        values = steps_of(own_key, dims, pieces, -0.22, 0.18) * values
    return jnp.clip(values, min=-bound, max=bound).astype(held_as)


def setup_inputs(seed: int = 0) -> dict:
    arg_keys = jax.random.split(jax.random.key(seed), 6)
    return {
        "hidden": draw_hidden(jax.random.fold_in(arg_keys[5], 71), 0),
        "w_query": scatter_about(arg_keys[1], (D, HEADS * HD), (D // 4) ** -0.5, 0.125, ((0, 4), (1, 8))),
        "w_keyvalue": scatter_about(arg_keys[2], (D, 2 * KV_HEADS * HD), (D // 4) ** -0.5, 0.125, ((0, 4), (1, 8))),
        "w_output": scatter_about(arg_keys[3], (HEADS * HD, D), (HEADS * HD // 16) ** -0.5, 0.75, ((0, 8), (1, 4))),
        "segment_ids": jnp.searchsorted(jnp.cumsum(ragged_sizes(arg_keys[4], 8, SEQ, SEQ // 4, 0)), jnp.arange(SEQ), side="right").astype(jnp.int32),
    }


ROPE_BASE = 500000.0
NEG_FILL = -1.0e30


def rotate(values, positions, head_count, width):
    row_count = values.shape[0]
    shaped = values.reshape(row_count, head_count, width)
    half_width = width // 2
    frequency = jnp.exp(jnp.arange(half_width, dtype=jnp.float32) * (-2.0 * math.log(ROPE_BASE) / width))
    angles = positions.astype(jnp.float32)[:, None] * frequency[None, :]
    cosine = jnp.cos(angles)[:, None, :]
    sine_part = jnp.sin(angles)[:, None, :]
    lower_half = shaped[:, :, :half_width]
    upper_half = shaped[:, :, half_width:]
    turned = jnp.concatenate([lower_half * cosine - upper_half * sine_part, upper_half * cosine + lower_half * sine_part], axis=2)
    return turned.reshape(row_count, head_count * width)


def split_keys(kv_sum, positions, kv_count, width):
    row_count = kv_sum.shape[0]
    shaped = kv_sum.reshape(row_count, kv_count, 2, width)
    key_part = rotate(shaped[:, :, 0, :].reshape(row_count, kv_count * width), positions, kv_count, width)
    key_part = key_part.reshape(row_count, kv_count, 1, width)
    return jnp.concatenate([key_part, shaped[:, :, 1:2, :]], axis=2).astype(jnp.bfloat16)


def reference(hidden, w_query, w_keyvalue, w_output, segment_ids):
    seq_len = hidden.shape[0]
    positions = jnp.arange(seq_len, dtype=jnp.int32)
    query = rotate(jnp.dot(hidden, w_query, preferred_element_type=jnp.float32), positions, HEADS, HD).astype(jnp.bfloat16)
    pairs = split_keys(jnp.dot(hidden, w_keyvalue, preferred_element_type=jnp.float32), positions, KV_HEADS, HD)
    key_all = pairs[:, :, 0, :]
    value_all = pairs[:, :, 1, :]
    block_len = min(512, seq_len)
    block_count = seq_len // block_len
    score_scale = HD ** -0.5

    def one_block(item_index):
        head_id = item_index // block_count
        block_id = item_index % block_count
        first_row = (block_id * block_len).astype(jnp.int32)
        query_block = lax.dynamic_slice(query, (first_row, (head_id * HD).astype(jnp.int32)), (block_len, HD))
        group_id = (head_id // GROUP).astype(jnp.int32)
        key_block = lax.dynamic_index_in_dim(key_all, group_id, axis=1, keepdims=False)
        value_block = lax.dynamic_index_in_dim(value_all, group_id, axis=1, keepdims=False)
        scores = lax.dot_general(query_block, key_block, (((1,), (1,)), ((), ())), preferred_element_type=jnp.float32) * score_scale
        query_pos = first_row + jnp.arange(block_len, dtype=jnp.int32)
        query_seg = lax.dynamic_slice_in_dim(segment_ids, first_row, block_len)
        allowed = (positions[None, :] <= query_pos[:, None]) & (segment_ids[None, :] == query_seg[:, None])
        masked = jnp.where(allowed, scores, NEG_FILL)
        row_max = jnp.max(masked, axis=1, keepdims=True)
        weights = jnp.where(allowed, jnp.exp(masked - row_max), 0.0)
        row_total = jnp.sum(weights, axis=1, keepdims=True)
        mixed_block = jnp.dot(weights.astype(jnp.bfloat16), value_block, preferred_element_type=jnp.float32)
        return (mixed_block / row_total).astype(jnp.bfloat16)

    blocks = lax.map(one_block, jnp.arange(HEADS * block_count, dtype=jnp.int32))
    mixed = blocks.reshape(HEADS, seq_len, HD).transpose(1, 0, 2).reshape(seq_len, HEADS * HD)
    return jnp.dot(mixed, w_output, preferred_element_type=jnp.float32).astype(jnp.bfloat16)
```

```python
import functools
import math

import jax
import jax.numpy as jnp
from jax import lax
from jax.experimental import pallas as pl
from jax.experimental.pallas import tpu as pltpu
from jax.sharding import PartitionSpec as P

HD = 128
GROUP = 8


ROPE_BASE = 500000.0
NEG_FILL = -1e30


def rotate(values, positions, head_count, width):
    row_count = values.shape[0]
    shaped = values.reshape(row_count, head_count, width)
    half_width = width // 2
    frequency = jnp.exp(
        jnp.arange(half_width, dtype=jnp.float32) * (-2.0 * math.log(ROPE_BASE) / width)
    )
    angles = positions.astype(jnp.float32)[:, None] * frequency[None, :]
    cosine = jnp.cos(angles)[:, None, :]
    sine_part = jnp.sin(angles)[:, None, :]
    lower_half = shaped[:, :, :half_width]
    upper_half = shaped[:, :, half_width:]
    turned = jnp.concatenate(
        [
            lower_half * cosine - upper_half * sine_part,
            upper_half * cosine + lower_half * sine_part,
        ],
        axis=2,
    )
    return turned.reshape(row_count, head_count * width)


def split_keys(kv_sum, positions, kv_count, width):
    row_count = kv_sum.shape[0]
    shaped = kv_sum.reshape(row_count, kv_count, 2, width)
    key_part = rotate(
        shaped[:, :, 0, :].reshape(row_count, kv_count * width), positions, kv_count, width
    )
    key_part = key_part.reshape(row_count, kv_count, 1, width)
    return jnp.concatenate([key_part, shaped[:, :, 1:2, :]], axis=2).astype(jnp.bfloat16)


def merge_keys(
    state_in, query_tile, query_pos_tile, query_seg_tile, key_tile, key_pos_tile, key_seg_tile
):
    running_max, running_sum, weighted = state_in
    allowed = (key_pos_tile[None, :] <= query_pos_tile[:, None]) & (
        key_seg_tile[None, :] == query_seg_tile[:, None]
    )
    key_part = key_tile[:, :HD]
    value_part = key_tile[:, HD:]
    scores = lax.dot_general(
        query_tile, key_part, (((1,), (1,)), ((), ())), preferred_element_type=jnp.float32
    ) * HD ** (-0.5)
    masked = jnp.where(allowed, scores, NEG_FILL)
    new_max = jnp.maximum(running_max, jnp.max(masked, axis=1))
    weights = jnp.where(allowed, jnp.exp(masked - new_max[:, None]), 0.0)
    new_sum = jnp.sum(weights, axis=1)
    new_weighted = jnp.dot(
        weights.astype(jnp.bfloat16), value_part, preferred_element_type=jnp.float32
    )
    return (new_max, new_sum, new_weighted)


def on_device(hidden, w_query, w_keyvalue, w_output, segment_ids):
    fsdp_count = lax.axis_size("fsdp")
    seq_count = lax.axis_size("sp")
    fsdp_index = lax.axis_index("fsdp")
    seq_index = lax.axis_index("sp")
    tok_rows = hidden.shape[0]
    sub_rows = tok_rows // fsdp_count
    kv_count = seq_count // GROUP
    query_rows = seq_count * sub_rows
    offsets = jnp.arange(query_rows, dtype=jnp.int32)
    query_pos = offsets // sub_rows * tok_rows + fsdp_index * sub_rows + offsets % sub_rows
    own_positions = (
        seq_index * tok_rows + fsdp_index * sub_rows + jnp.arange(sub_rows, dtype=jnp.int32)
    )

    def project(weight_block):
        return jnp.dot(hidden, weight_block, preferred_element_type=jnp.float32)

    query_part = project(lax.all_gather(w_query, "sp", axis=1, tiled=True))
    kv_part = project(lax.all_gather(w_keyvalue, "sp", axis=1, tiled=True))
    query_sum, kv_sum = (
        lax.psum_scatter(query_part, "fsdp", scatter_dimension=0, tiled=True),
        lax.psum_scatter(kv_part, "fsdp", scatter_dimension=0, tiled=True),
    )
    query_local = rotate(query_sum, own_positions, seq_count, HD).astype(jnp.bfloat16)
    pairs = split_keys(kv_sum, own_positions, kv_count, HD)
    expanded = jnp.repeat(pairs, GROUP, axis=1).reshape(sub_rows, seq_count * 2 * HD)
    query_head, kv_head = (
        lax.all_to_all(query_local, "sp", split_axis=1, concat_axis=0, tiled=True),
        lax.all_to_all(expanded, "sp", split_axis=1, concat_axis=0, tiled=True),
    )
    segment_all = lax.all_gather(segment_ids, "sp", axis=0, tiled=True)
    query_seg = segment_all[query_pos]
    initial = (
        jnp.full((query_rows,), NEG_FILL, jnp.float32),
        jnp.zeros((query_rows,), jnp.float32),
        jnp.zeros((query_rows, HD), jnp.float32),
    )
    block_keys = lax.all_gather(kv_head, "fsdp", axis=0, tiled=True)
    piece_rows = block_keys.shape[0]
    row_ids = jnp.arange(piece_rows, dtype=jnp.int32)
    source_id = row_ids // query_rows
    within = row_ids % query_rows
    key_pos = within // sub_rows * tok_rows + source_id * sub_rows + within % sub_rows
    key_seg = segment_all[key_pos]
    final_max, final_sum, final_weighted = merge_keys(
        initial, query_head, query_pos, query_seg, block_keys, key_pos, key_seg
    )
    attention = (final_weighted / final_sum[:, None]).astype(jnp.bfloat16)
    back_rows = lax.all_to_all(attention, "sp", split_axis=0, concat_axis=1, tiled=True)
    mixed_rows = lax.all_gather(back_rows, "fsdp", axis=0, tiled=True)
    result = jnp.dot(
        mixed_rows,
        lax.all_gather(w_output, "sp", axis=0, tiled=True),
        preferred_element_type=jnp.float32,
    )
    return result.astype(jnp.bfloat16)


NEG_POS = -1
WO_CHUNKS = 4


def fused_kernel(
    nf, nz, nx, hid, wq, wkv, wo, seg, out,
    h_buf, wq_buf, wkv_buf, wo_buf, seg_buf,
    q_part, q_recv, kv_part, kv_recv, kv_piece, kv_all, mix_own, mix_buf, q_cos, q_sin,
    out_buf, out_away,
    s_loc, s_hid, r_hid, s_seg, r_seg, s_wkv, r_wkv, s_wq, r_wq,
    s_q, r_q, s_kvp, r_kvp, s_kv, r_kv, s_wo, r_wo, s_wox, r_wox, s_mix, r_mix,
    s_out, r_out, s_res,
):
    f = lax.axis_index("fsdp")
    s = lax.axis_index("sp")
    z, x = s // nx, s % nx
    tok, kdim = hid.shape
    rows = tok * nx
    sub = rows // nf
    kvw = wkv.shape[0]
    other = 1 - x
    half_cols = wo.shape[1] // nx
    chunk = half_cols // WO_CHUNKS
    f32, bf16 = jnp.float32, jnp.bfloat16
    is_end = (z == 0) | (z == nz - 1)
    is_inner = jnp.logical_not(is_end)
    low = z < nz // 2
    e = jnp.where(low, 0, nz - 1)
    n = jnp.where(low, 1, nz - 2)
    m = nz - 1 - n
    e2 = nz - 1 - e

    def dev(ff, zz, xx):
        return (ff, zz * nx + xx)

    def remote(src, dst, ss, rs, target):
        return pltpu.make_async_remote_copy(
            src_ref=src, dst_ref=dst, send_sem=ss, recv_sem=rs,
            device_id=target, device_id_type=pl.DeviceIdType.MESH,
        )

    def tile(ref, count):
        return pl.ds(pl.multiple_of(ref * count, count), count)

    here = (f, s)
    pending = {"all": [], "end": [], "inner": []}

    def go(kind, make):
        make().start()
        pending[kind].append(make)

    def cols(c):
        return slice(c * chunk, (c + 1) * chunk)

    own_h = pltpu.make_async_copy(hid, h_buf.at[tile(x, tok)], s_loc.at[0])
    own_wq = pltpu.make_async_copy(wq, wq_buf.at[z], s_loc.at[1])
    own_wkv = pltpu.make_async_copy(wkv, wkv_buf.at[tile(z, kvw)], s_loc.at[2])
    own_wo = [
        pltpu.make_async_copy(
            wo.at[:, h * half_cols : (h + 1) * half_cols],
            wo_buf.at[h, tile(s, HD)], s_loc.at[3 + h],
        )
        for h in range(nx)
    ]
    own_seg = pltpu.make_async_copy(seg, seg_buf.at[1, x], s_loc.at[5])
    for copy in (own_wkv, own_wq, own_h, *own_wo, own_seg):
        copy.start()

    def hid_send():
        return remote(
            h_buf.at[tile(x, tok)], h_buf.at[tile(x, tok)], s_hid, r_hid, dev(f, z, other)
        )

    def hid_wait():
        remote(
            h_buf.at[tile(other, tok)], h_buf.at[tile(other, tok)], s_hid, r_hid, here
        ).wait_recv()

    def wkv_z(j, d, target):
        ref = wkv_buf.at[tile(j, kvw)]
        return remote(ref, ref, s_wkv.at[d, j], r_wkv.at[j], dev(f, target, x))

    def wkv_wait(j):
        wkv_z(j, 0, z).wait_recv()

    def wq_z(j, d, target):
        ref = wq_buf.at[j]
        return remote(ref, ref, s_wq.at[d, j], r_wq.at[j], dev(f, target, x))

    def wq_wait(j):
        wq_z(j, 0, z).wait_recv()

    def wo_unit(h, j, xx, c):
        return wo_buf.at[h, tile(j * nx + xx, HD), cols(c)]

    def wo_z(j, xx, c, d, target):
        ref = wo_unit(x, j, xx, c)
        return remote(ref, ref, s_wo.at[d, j, xx, c], r_wo.at[j, xx, c], dev(f, target, x))

    def wo_pair(c):
        ref = wo_unit(other, z, x, c)
        return remote(ref, ref, s_wox.at[nz, x, c], r_wo.at[z, x, c], dev(f, z, other))

    def wo_wait(j, xx, c):
        ref = wo_unit(x, j, xx, c)
        remote(ref, ref, s_wox.at[0, 0, c], r_wo.at[j, xx, c], here).wait_recv()

    def wo_cross(j, xx, c):
        ref = wo_unit(x, j, xx, c)
        return remote(ref, ref, s_wox.at[j, xx, c], r_wox.at[j, xx, c], dev(f, z, other))

    def wox_wait(j, xx, c):
        ref = wo_unit(other, j, xx, c)
        remote(ref, ref, s_wox.at[0, 0, c], r_wox.at[j, xx, c], here).wait_recv()

    def seg_same():
        return remote(seg_buf.at[1, x], seg_buf.at[1, x], s_seg.at[0], r_seg.at[1, x], dev(f, z, other))

    def seg_next(xx):
        return remote(
            seg_buf.at[1, x], seg_buf.at[0, x], s_seg.at[1 + xx], r_seg.at[0, x], dev(f, z + 1, xx)
        )

    barrier = pltpu.get_barrier_semaphore()

    def greet(ff, zz, xx):
        pl.semaphore_signal(
            barrier, inc=1, device_id=dev(ff, zz, xx), device_id_type=pl.DeviceIdType.MESH
        )

    plane = nf * nx
    for step in (1, -1):
        @pl.when((z + step >= 0) & (z + step < nz))
        def _():
            for xx in range(nx):
                greet(f, z + step, xx)

    for d in range(1, plane):
        greet(lax.rem(f + d, nf), z, lax.rem(x + d // nf, nx))
    pl.semaphore_wait(barrier, plane - 1 + jnp.where(is_end, nx, 2 * nx))

    own_wkv.wait()
    own_wq.wait()

    @pl.when(is_end)
    def _():
        go("end", lambda: wkv_z(z, 1, n))
        go("end", lambda: wq_z(z, 1, n))

    @pl.when(is_inner)
    def _():
        for d, target in ((0, e), (1, m)):
            go("inner", lambda d=d, target=target: wkv_z(z, d, target))
            go("inner", lambda d=d, target=target: wq_z(z, d, target))

    own_h.wait()
    go("all", hid_send)
    own_seg.wait()
    go("all", seg_same)

    @pl.when(z < nz - 1)
    def _():
        for xx in range(nx):
            seg_next(xx).start()

    for copy in own_wo:
        copy.wait()
    for c in range(WO_CHUNKS):
        go("all", lambda c=c: wo_pair(c))

    @pl.when(is_end)
    def _():
        for c in range(WO_CHUNKS):
            go("end", lambda c=c: wo_z(z, x, c, 1, n))
        for c in range(WO_CHUNKS):
            go("end", lambda c=c: wo_cross(z, x, c))

    @pl.when(z == 0)
    def _():
        kv_all[0] = jnp.zeros(kv_all.shape[1:], bf16)
        seg_buf[0] = jnp.full(seg_buf.shape[1:], NEG_POS, jnp.int32)

    def table(row_count, first, lane_index):
        position = (first + lax.broadcasted_iota(jnp.int32, (row_count, HD), 0)).astype(f32)
        frequency = jnp.exp(lane_index.astype(f32) * (-2.0 * math.log(ROPE_BASE) / HD))
        return position * frequency

    lane = lax.broadcasted_iota(jnp.int32, (1, HD), 1)
    half = HD // 2
    quarter = half // nx
    kv_angle = table(sub, z * rows + f * sub, x * quarter + lane % quarter)
    is_key = lane < half
    kv_cos = jnp.where(is_key, jnp.cos(kv_angle), 1.0)
    kv_sin = jnp.where(is_key, jnp.sin(kv_angle), 0.0)
    kv_sin = jnp.where(lane < quarter, -kv_sin, kv_sin)
    q_angle = table(rows, z * rows, lane % half)
    q_sine = jnp.sin(q_angle)
    q_cos[...] = jnp.cos(q_angle)
    q_sin[...] = jnp.where(lane < half, -q_sine, q_sine)

    def q_send(j):
        return remote(q_part.at[j], q_recv.at[f], s_q.at[j], r_q.at[f], (j, s))

    def q_project(j):
        q_part[j] = jnp.dot(h_buf[...], wq_buf[j], preferred_element_type=f32)

        @pl.when(j != f)
        def _():
            q_send(j).start()

    @pl.when(is_inner)
    def _():
        wkv_wait(e)
        go("inner", lambda: wkv_z(e, 1, m))
        wkv_wait(m)
        go("inner", lambda: wkv_z(m, 0, e))
        wq_wait(e)
        go("inner", lambda: wq_z(e, 1, m))
        for c in range(WO_CHUNKS):
            go("inner", lambda c=c: wo_z(z, x, c, 1, m))
        wq_wait(m)
        go("inner", lambda: wq_z(m, 0, e))
        wkv_wait(e2)
        go("inner", lambda: wkv_z(e2, 0, e))

    hid_wait()
    q_project(z)

    @pl.when(is_inner)
    def _():
        q_project(e)
        q_project(m)
        wq_wait(e2)
        go("inner", lambda: wq_z(e2, 0, e))

    @pl.when(is_end)
    def _():
        wq_wait(n)
        q_project(n)
        for c in range(WO_CHUNKS):
            wo_wait(z, other, c)
            go("end", lambda c=c: wo_z(z, other, c, 1, n))
        wq_wait(m)
        q_project(m)
        for j in (n, m, e2):
            wkv_wait(j)

    kv_part[...] = lax.dot_general(
        h_buf[...], wkv_buf[...], (((1,), (1,)), ((), ())), preferred_element_type=f32
    )

    def kvp_send(d):
        ff = lax.rem(f + d, nf)
        return remote(
            kv_part.at[tile(ff, sub)], kv_recv.at[f], s_kvp.at[d - 1], r_kvp.at[f], (ff, s)
        )

    def kvp_wait(d):
        ff = lax.rem(f + d, nf)
        remote(
            kv_part.at[tile(ff, sub)], kv_recv.at[ff], s_kvp.at[d - 1], r_kvp.at[ff], here
        ).wait_recv()

    for d in range(1, nf):
        go("all", lambda d=d: kvp_send(d))

    @pl.when(is_inner)
    def _():
        q_project(e2)
        for c in range(WO_CHUNKS):
            go("inner", lambda c=c: wo_z(z, x, c, 0, e))
        for c in range(WO_CHUNKS):
            wo_wait(z, other, c)
            go("inner", lambda c=c: wo_z(z, other, c, 1, m))
        for c in range(WO_CHUNKS):
            go("inner", lambda c=c: wo_z(z, other, c, 0, e))

    total = kv_part[tile(f, sub), :]
    for d in range(1, nf):
        kvp_wait(d)
        total = total + kv_recv[lax.rem(f + d, nf)]
    partner = jnp.where(
        lane < quarter, pltpu.roll(total, HD - quarter, 1), pltpu.roll(total, quarter, 1)
    )
    kv_piece[...] = (total * kv_cos + partner * kv_sin).astype(bf16)
    piece_rows = tile(f, sub)
    own_piece = pltpu.make_async_copy(kv_piece, kv_all.at[1, x, piece_rows], s_loc.at[6])
    own_piece.start()

    def kv_send(plane, dx, d):
        ff, xx = lax.rem(f + d, nf), lax.rem(x + dx, nx)
        slot = kv_all.at[plane, x, piece_rows]
        return remote(
            kv_piece if plane else slot, slot,
            s_kv.at[plane, dx, d], r_kv.at[plane, x, f], dev(ff, z, xx),
        )

    def kv_next():
        return remote(
            kv_piece, kv_all.at[0, x, piece_rows],
            s_kv.at[0, 0, 0], r_kv.at[0, x, f], dev(f, z + 1, x),
        )

    def kv_wait(plane, dx, d):
        ff, xx = lax.rem(f + d, nf), lax.rem(x + dx, nx)
        remote(
            kv_piece, kv_all.at[plane, xx, tile(ff, sub)],
            s_kv.at[plane, dx, d], r_kv.at[plane, xx, ff], here,
        ).wait_recv()

    pairs = [(dx, d) for dx in range(nx) for d in range(nf)]
    for pair in pairs[1:]:
        go("all", lambda pair=pair: kv_send(1, *pair))

    @pl.when(z < nz - 1)
    def _():
        kv_next().start()

    @pl.when(is_inner)
    def _():
        for xx in range(nx):
            for c in range(WO_CHUNKS):
                wo_wait(e, xx, c)
                go("inner", lambda xx=xx, c=c: wo_z(e, xx, c, 1, m))

    @pl.when(z > 0)
    def _():
        kv_wait(0, 0, 0)
        for pair in pairs[1:]:
            kv_send(0, *pair).start()

    @pl.when(is_end)
    def _():
        wq_wait(e2)
        q_project(e2)

    q_total = q_part[f]
    for d in range(1, nf):
        ff = lax.rem(f + d, nf)
        remote(q_part.at[0], q_recv.at[ff], s_q.at[0], r_q.at[ff], here).wait_recv()
        q_total = q_total + q_recv[ff]
    q_turned = q_total * q_cos[...] + pltpu.roll(q_total, half, 1) * q_sin[...]
    q_head = q_turned.astype(bf16).astype(f32)
    quarters = []
    for xx in range(nx):
        first = q_head if xx == 0 else pltpu.roll(q_head, HD - xx * quarter, 1)
        second = pltpu.roll(q_head, (HD - half - xx * quarter + quarter) % HD, 1)
        picked = jnp.where(lane < quarter, first, jnp.where(lane < half, second, 0.0))
        quarters.append(picked.astype(bf16))

    seg_wait = lambda plane, xx: remote(
        seg_buf.at[plane, xx], seg_buf.at[plane, xx], s_seg.at[0], r_seg.at[plane, xx], here
    ).wait_recv()
    seg_wait(1, other)
    own_piece.wait()
    for pair in pairs[1:]:
        kv_wait(1, *pair)

    @pl.when(z > 0)
    def _():
        for xx in range(nx):
            seg_wait(0, xx)
        for pair in pairs[1:]:
            kv_wait(0, *pair)

    key_seg = jnp.concatenate(
        [seg_buf[plane, xx] for plane in range(2) for xx in range(nx)], axis=1
    )
    own_seg_row = key_seg[:, rows:]
    seg_column = jnp.transpose(jnp.broadcast_to(own_seg_row, (HD, rows)))[:, :1]
    key_pos = lax.broadcasted_iota(jnp.int32, (1, 2 * rows), 1) - rows
    keys = [
        jnp.concatenate([kv_all[0, xx], kv_all[1, xx]], axis=0) for xx in range(nx)
    ]
    step_rows = rows // nf
    for b in range(nf):
        span = slice(b * step_rows, (b + 1) * step_rows)
        query_pos = b * step_rows + lax.broadcasted_iota(jnp.int32, (step_rows, 1), 0)
        score = None
        for xx in range(nx):
            term = lax.dot_general(
                quarters[xx][span], keys[xx], (((1,), (1,)), ((), ())),
                preferred_element_type=f32,
            )
            score = term if score is None else score + term
        allowed = (key_pos <= query_pos) & (key_seg == seg_column[span])
        masked = jnp.where(allowed, score * HD ** (-0.5), NEG_FILL)
        row_max = jnp.max(masked, axis=1, keepdims=True)
        weight = jnp.where(allowed, jnp.exp(masked - row_max), 0.0)
        row_total = jnp.sum(weight, axis=1, keepdims=True)
        rounded = weight.astype(bf16)
        product = [
            jnp.dot(rounded, keys[xx], preferred_element_type=f32) for xx in range(nx)
        ]
        mixed = None
        for xx in reversed(range(nx)):
            first = pltpu.roll(product[xx], (half + xx * quarter) % HD, 1)
            second = pltpu.roll(product[xx], (HD - (nx - 1 - xx) * quarter) % HD, 1)
            lane_block = lane // quarter
            value = jnp.where(lane_block < nx, first, second)
            mixed = value if mixed is None else jnp.where(lane_block % nx == xx, value, mixed)
        mix_own[span, :] = (mixed / row_total).astype(bf16)

    head = f * nx + x

    def mix_part(dx, d):
        ff, xx = lax.rem(f + d, nf), lax.rem(x + dx, nx)
        return remote(
            mix_own.at[tile(xx, tok)], mix_buf.at[0:tok, tile(head, HD)],
            s_mix.at[dx, d], r_mix.at[x, f], dev(ff, z, xx),
        )

    def mix_whole(dx, d):
        ff, xx = lax.rem(f + d, nf), lax.rem(x + dx, nx)
        return remote(
            mix_own, mix_buf.at[:, tile(head, HD)],
            s_mix.at[dx, d], r_mix.at[x, f], dev(ff, z, xx),
        )

    def mix_wait(dx, d, count):
        ff, xx = lax.rem(f + d, nf), lax.rem(x + dx, nx)
        ref = mix_buf.at[0:count, tile(ff * nx + xx, HD)]
        remote(
            ref, ref, s_mix.at[dx, d], r_mix.at[xx, ff], here,
        ).wait_recv()

    far = [pair for pair in pairs[1:] if pair[0]] + [pair for pair in pairs[1:] if not pair[0]]

    @pl.when(is_end)
    def _():
        for pair in far:
            go("end", lambda pair=pair: mix_part(*pair))
        mix_buf[0:tok, tile(head, HD)] = mix_own[tile(x, tok), :]

    @pl.when(is_inner)
    def _():
        for pair in far:
            go("inner", lambda pair=pair: mix_whole(*pair))
        mix_buf[:, tile(head, HD)] = mix_own[...]

    def result(h, c):
        where = pl.ds(pl.multiple_of(h * half_cols + c * chunk, chunk), chunk)
        return pltpu.make_async_copy(out_buf.at[h, :, cols(c)], out.at[:, where], s_res.at[h, c])

    @pl.when(is_inner)
    def _():
        for j in (m, e2):
            for xx in range(nx):
                for c in range(WO_CHUNKS):
                    wo_wait(j, xx, c)
                    go("inner", lambda j=j, xx=xx, c=c: wo_z(j, xx, c, 0, e))
        for pair in far:
            mix_wait(*pair, rows)

        def away(c):
            return remote(
                out_away.at[c], out_buf.at[x, :, cols(c)], s_out.at[c], r_out.at[c], dev(f, z, other)
            )

        for c in range(WO_CHUNKS):
            block = wo_buf[x, :, cols(c)]
            out_away[c] = jnp.dot(
                mix_buf[tile(other, tok), :], block, preferred_element_type=f32
            ).astype(bf16)
            go("inner", lambda c=c: away(c))
            out_buf[x, :, cols(c)] = jnp.dot(
                mix_buf[tile(x, tok), :], block, preferred_element_type=f32
            ).astype(bf16)
            result(x, c).start()
        for c in range(WO_CHUNKS):
            ref = out_buf.at[other, :, cols(c)]
            remote(ref, ref, s_out.at[c], r_out.at[c], here).wait_recv()
            result(other, c).start()

    @pl.when(is_end)
    def _():
        def cross(j):
            for xx in range(nx):
                for c in range(WO_CHUNKS):
                    wo_wait(j, xx, c)
                    go("end", lambda xx=xx, c=c: wo_cross(j, xx, c))

        cross(n)
        for pair in far:
            mix_wait(*pair, tok)
        cross(m)
        cross(e2)
        for c in range(WO_CHUNKS):
            out_buf[x, :, cols(c)] = jnp.dot(
                mix_buf[0:tok, :], wo_buf[x, :, cols(c)], preferred_element_type=f32
            ).astype(bf16)
            result(x, c).start()
        for c in range(WO_CHUNKS):
            wox_wait(z, other, c)
            for j in (n, m, e2):
                for xx in range(nx):
                    wox_wait(j, xx, c)
        for c in range(WO_CHUNKS):
            out_buf[other, :, cols(c)] = jnp.dot(
                mix_buf[0:tok, :], wo_buf[other, :, cols(c)], preferred_element_type=f32
            ).astype(bf16)
            result(other, c).start()

    for make in pending["all"]:
        make().wait_send()
    for kind, cond in (("end", is_end), ("inner", is_inner)):
        @pl.when(cond)
        def _():
            for make in pending[kind]:
                make().wait_send()

    for d in range(1, nf):
        q_send(lax.rem(f + d, nf)).wait_send()

    @pl.when(z < nz - 1)
    def _():
        for xx in range(nx):
            seg_next(xx).wait_send()
        kv_next().wait_send()

    @pl.when(z > 0)
    def _():
        for pair in pairs[1:]:
            kv_send(0, *pair).wait_send()

    for h in range(nx):
        for c in range(WO_CHUNKS):
            result(h, c).wait()


def fused_on_device(nf, nz, nx, hidden, w_query, w_keyvalue, w_output, segment_ids):
    tok, kdim = hidden.shape
    cols = w_output.shape[1]
    rows = tok * nx
    sub = rows // nf
    kvw = w_keyvalue.shape[1]
    heads = nz * nx
    part = cols // nx
    f32, bf16 = jnp.float32, jnp.bfloat16
    dma = pltpu.SemaphoreType.DMA
    vmem = pl.BlockSpec(memory_space=pltpu.VMEM)
    anywhere = pl.BlockSpec(memory_space=pl.ANY)
    scratch = [
        pltpu.VMEM((rows, kdim), bf16),
        pltpu.VMEM((nz, kdim, HD), bf16),
        pltpu.VMEM((nz * kvw, kdim), bf16),
        pltpu.VMEM((nx, heads * HD, part), bf16),
        pltpu.VMEM((2, nx, 1, tok), jnp.int32),
        pltpu.VMEM((nz, rows, HD), f32),
        pltpu.VMEM((nf, rows, HD), f32),
        pltpu.VMEM((rows, nz * kvw), f32),
        pltpu.VMEM((nf, sub, nz * kvw), f32),
        pltpu.VMEM((sub, HD), bf16),
        pltpu.VMEM((2, nx, rows, HD), bf16),
        pltpu.VMEM((rows, HD), bf16),
        pltpu.VMEM((rows, heads * HD), bf16),
        pltpu.VMEM((rows, HD), f32),
        pltpu.VMEM((rows, HD), f32),
        pltpu.VMEM((nx, tok, part), bf16),
        pltpu.VMEM((WO_CHUNKS, tok, part // WO_CHUNKS), bf16),
        dma((7,)), dma, dma, dma((1 + nx,)), dma((2, nx)),
        dma((2, nz)), dma((nz,)), dma((2, nz)), dma((nz,)),
        dma((nz,)), dma((nf,)), dma((nf,)), dma((nf,)),
        dma((2, nx, nf)), dma((2, nx, nf)),
        dma((2, nz, nx, WO_CHUNKS)), dma((nz, nx, WO_CHUNKS)),
        dma((nz + 1, nx, WO_CHUNKS)), dma((nz, nx, WO_CHUNKS)),
        dma((nx, nf)), dma((nx, nf)),
        dma((WO_CHUNKS,)), dma((WO_CHUNKS,)), dma((nx, WO_CHUNKS)),
    ]
    return pl.pallas_call(
        functools.partial(fused_kernel, nf, nz, nx),
        out_shape=jax.ShapeDtypeStruct((tok, cols), bf16),
        in_specs=[anywhere] * 4 + [vmem],
        out_specs=anywhere,
        scratch_shapes=scratch,
        name="fused_sublayer",
        compiler_params=pltpu.CompilerParams(
            collective_id=0, has_side_effects=True, vmem_limit_bytes=60 * 1024 * 1024
        ),
    )(hidden, w_query, w_keyvalue.T, w_output, segment_ids.reshape(1, tok))


def solution(mesh):
    in_specs = (P("sp", "fsdp"), P("fsdp", "sp"), P("fsdp", "sp"), P("sp", "fsdp"), P("sp"))
    out_specs = P("sp", "fsdp")
    nf, sp = mesh.shape["fsdp"], mesh.shape["sp"]
    if sp == GROUP and sp == 2 * nf:
        body = functools.partial(fused_on_device, nf, nf, sp // nf)
    else:
        body = on_device
    return jax.shard_map(
        body, mesh=mesh, in_specs=in_specs, out_specs=out_specs, check_vma=False
    )
```

```python
import functools
import math

import jax
import jax.numpy as jnp
from jax import lax
from jax.experimental import pallas as pl
from jax.experimental.pallas import tpu as pltpu
from jax.sharding import PartitionSpec as P

HD = 128
GROUP = 8


ROPE_BASE = 500000.0
NEG_FILL = -1e30


def rotate(values, positions, head_count, width):
    row_count = values.shape[0]
    shaped = values.reshape(row_count, head_count, width)
    half_width = width // 2
    frequency = jnp.exp(
        jnp.arange(half_width, dtype=jnp.float32) * (-2.0 * math.log(ROPE_BASE) / width)
    )
    angles = positions.astype(jnp.float32)[:, None] * frequency[None, :]
    cosine = jnp.cos(angles)[:, None, :]
    sine_part = jnp.sin(angles)[:, None, :]
    lower_half = shaped[:, :, :half_width]
    upper_half = shaped[:, :, half_width:]
    turned = jnp.concatenate(
        [
            lower_half * cosine - upper_half * sine_part,
            upper_half * cosine + lower_half * sine_part,
        ],
        axis=2,
    )
    return turned.reshape(row_count, head_count * width)


def split_keys(kv_sum, positions, kv_count, width):
    row_count = kv_sum.shape[0]
    shaped = kv_sum.reshape(row_count, kv_count, 2, width)
    key_part = rotate(
        shaped[:, :, 0, :].reshape(row_count, kv_count * width), positions, kv_count, width
    )
    key_part = key_part.reshape(row_count, kv_count, 1, width)
    return jnp.concatenate([key_part, shaped[:, :, 1:2, :]], axis=2).astype(jnp.bfloat16)


def merge_keys(
    state_in, query_tile, query_pos_tile, query_seg_tile, key_tile, key_pos_tile, key_seg_tile
):
    running_max, running_sum, weighted = state_in
    allowed = (key_pos_tile[None, :] <= query_pos_tile[:, None]) & (
        key_seg_tile[None, :] == query_seg_tile[:, None]
    )
    key_part = key_tile[:, :HD]
    value_part = key_tile[:, HD:]
    scores = lax.dot_general(
        query_tile, key_part, (((1,), (1,)), ((), ())), preferred_element_type=jnp.float32
    ) * HD ** (-0.5)
    masked = jnp.where(allowed, scores, NEG_FILL)
    new_max = jnp.maximum(running_max, jnp.max(masked, axis=1))
    weights = jnp.where(allowed, jnp.exp(masked - new_max[:, None]), 0.0)
    new_sum = jnp.sum(weights, axis=1)
    new_weighted = jnp.dot(
        weights.astype(jnp.bfloat16), value_part, preferred_element_type=jnp.float32
    )
    return (new_max, new_sum, new_weighted)


def on_device(hidden, w_query, w_keyvalue, w_output, segment_ids):
    fsdp_count = lax.axis_size("fsdp")
    seq_count = lax.axis_size("sp")
    fsdp_index = lax.axis_index("fsdp")
    seq_index = lax.axis_index("sp")
    tok_rows = hidden.shape[0]
    sub_rows = tok_rows // fsdp_count
    kv_count = seq_count // GROUP
    query_rows = seq_count * sub_rows
    offsets = jnp.arange(query_rows, dtype=jnp.int32)
    query_pos = offsets // sub_rows * tok_rows + fsdp_index * sub_rows + offsets % sub_rows
    own_positions = (
        seq_index * tok_rows + fsdp_index * sub_rows + jnp.arange(sub_rows, dtype=jnp.int32)
    )

    def project(weight_block):
        return jnp.dot(hidden, weight_block, preferred_element_type=jnp.float32)

    query_part = project(lax.all_gather(w_query, "sp", axis=1, tiled=True))
    kv_part = project(lax.all_gather(w_keyvalue, "sp", axis=1, tiled=True))
    query_sum, kv_sum = (
        lax.psum_scatter(query_part, "fsdp", scatter_dimension=0, tiled=True),
        lax.psum_scatter(kv_part, "fsdp", scatter_dimension=0, tiled=True),
    )
    query_local = rotate(query_sum, own_positions, seq_count, HD).astype(jnp.bfloat16)
    pairs = split_keys(kv_sum, own_positions, kv_count, HD)
    expanded = jnp.repeat(pairs, GROUP, axis=1).reshape(sub_rows, seq_count * 2 * HD)
    query_head, kv_head = (
        lax.all_to_all(query_local, "sp", split_axis=1, concat_axis=0, tiled=True),
        lax.all_to_all(expanded, "sp", split_axis=1, concat_axis=0, tiled=True),
    )
    segment_all = lax.all_gather(segment_ids, "sp", axis=0, tiled=True)
    query_seg = segment_all[query_pos]
    initial = (
        jnp.full((query_rows,), NEG_FILL, jnp.float32),
        jnp.zeros((query_rows,), jnp.float32),
        jnp.zeros((query_rows, HD), jnp.float32),
    )
    block_keys = lax.all_gather(kv_head, "fsdp", axis=0, tiled=True)
    piece_rows = block_keys.shape[0]
    row_ids = jnp.arange(piece_rows, dtype=jnp.int32)
    source_id = row_ids // query_rows
    within = row_ids % query_rows
    key_pos = within // sub_rows * tok_rows + source_id * sub_rows + within % sub_rows
    key_seg = segment_all[key_pos]
    final_max, final_sum, final_weighted = merge_keys(
        initial, query_head, query_pos, query_seg, block_keys, key_pos, key_seg
    )
    attention = (final_weighted / final_sum[:, None]).astype(jnp.bfloat16)
    back_rows = lax.all_to_all(attention, "sp", split_axis=0, concat_axis=1, tiled=True)
    mixed_rows = lax.all_gather(back_rows, "fsdp", axis=0, tiled=True)
    result = jnp.dot(
        mixed_rows,
        lax.all_gather(w_output, "sp", axis=0, tiled=True),
        preferred_element_type=jnp.float32,
    )
    return result.astype(jnp.bfloat16)


NEG_POS = -1
WO_CHUNKS = 4
MOVED = 4
END_CHUNKS = 2


def fused_kernel(
    nf, nz, nx, hid, wq, wkv, wo, seg, out,
    h_buf, wq_buf, wkv_buf, wo_buf, seg_buf,
    q_part, q_recv, kv_part, kv_recv, kv_piece, kv_all, mix_own, mix_buf, q_cos, q_sin,
    out_buf, out_away, h_end, e_part, e_recv, e_back, q_in,
    s_loc, s_hid, r_hid, s_seg, r_seg, s_wkv, r_wkv, s_wq, r_wq,
    s_q, r_q, s_kvp, r_kvp, s_kv, r_kv, s_wo, r_wo, s_wox, r_wox, s_mix, r_mix,
    s_out, r_out, s_res, s_he, r_he, s_hx, s_ep, r_ep, s_eb, r_eb,
):
    f = lax.axis_index("fsdp")
    s = lax.axis_index("sp")
    z, x = s // nx, s % nx
    tok, kdim = hid.shape
    rows = tok * nx
    sub = rows // nf
    kvw = wkv.shape[0]
    other = 1 - x
    moved = kdim * MOVED // 8
    block = tok // 2
    half_cols = wo.shape[1] // nx
    chunk = half_cols // WO_CHUNKS
    f32, bf16 = jnp.float32, jnp.bfloat16
    is_end = (z == 0) | (z == nz - 1)
    is_inner = jnp.logical_not(is_end)
    low = z < nz // 2
    e = jnp.where(low, 0, nz - 1)
    n = jnp.where(low, 1, nz - 2)
    m = nz - 1 - n
    e2 = nz - 1 - e

    def dev(ff, zz, xx):
        return (ff, zz * nx + xx)

    def remote(src, dst, ss, rs, target):
        return pltpu.make_async_remote_copy(
            src_ref=src, dst_ref=dst, send_sem=ss, recv_sem=rs,
            device_id=target, device_id_type=pl.DeviceIdType.MESH,
        )

    def tile(ref, count):
        return pl.ds(pl.multiple_of(ref * count, count), count)

    here = (f, s)
    pending = {"all": [], "end": [], "inner": []}

    def go(kind, make):
        make().start()
        pending[kind].append(make)

    def cols(c):
        return slice(c * chunk, (c + 1) * chunk)

    own_h = pltpu.make_async_copy(hid, h_buf.at[tile(x, tok)], s_loc.at[0])
    own_wq = pltpu.make_async_copy(wq, wq_buf.at[z], s_loc.at[1])
    own_wkv = pltpu.make_async_copy(wkv, wkv_buf.at[tile(z, kvw)], s_loc.at[2])
    own_wo = [
        pltpu.make_async_copy(
            wo.at[:, h * half_cols : (h + 1) * half_cols],
            wo_buf.at[h, tile(s, HD)], s_loc.at[3 + h],
        )
        for h in range(nx)
    ]
    own_seg = pltpu.make_async_copy(seg, seg_buf.at[1, x], s_loc.at[5])
    for copy in (own_wkv, own_wq, own_h, *own_wo, own_seg):
        copy.start()

    def hid_send():
        return remote(
            h_buf.at[tile(x, tok)], h_buf.at[tile(x, tok)], s_hid, r_hid, dev(f, z, other)
        )

    def hid_wait():
        remote(
            h_buf.at[tile(other, tok)], h_buf.at[tile(other, tok)], s_hid, r_hid, here
        ).wait_recv()

    def wkv_z(j, d, target):
        ref = wkv_buf.at[tile(j, kvw)]
        return remote(ref, ref, s_wkv.at[d, j], r_wkv.at[j], dev(f, target, x))

    def wkv_wait(j):
        wkv_z(j, 0, z).wait_recv()

    def wq_z(j, d, target):
        ref = wq_buf.at[j] if d else wq_buf.at[j, moved:, :]
        return remote(ref, ref, s_wq.at[d, j], r_wq.at[j], dev(f, target, x))

    def wq_wait(j, d=1):
        wq_z(j, d, z).wait_recv()

    def he_z(hf):
        rows_of = pl.ds(pl.multiple_of(x * tok + hf * block, block), block)
        return remote(
            h_buf.at[rows_of, 0:moved], h_end.at[x, hf], s_he.at[hf], r_he.at[x, hf], dev(f, n, x)
        )

    def he_x(hf):
        ref = h_end.at[x, hf]
        return remote(ref, ref, s_hx.at[hf], r_he.at[x, hf], dev(f, z, other))

    def he_wait(xx, hf):
        ref = h_end.at[xx, hf]
        remote(ref, ref, s_hx.at[hf], r_he.at[xx, hf], here).wait_recv()

    def wo_unit(h, j, xx, c):
        return wo_buf.at[h, tile(j * nx + xx, HD), cols(c)]

    def wo_z(j, xx, c, d, target):
        ref = wo_unit(x, j, xx, c)
        return remote(ref, ref, s_wo.at[d, j, xx, c], r_wo.at[j, xx, c], dev(f, target, x))

    def wo_pair(c):
        ref = wo_unit(other, z, x, c)
        return remote(ref, ref, s_wox.at[nz, x, c], r_wo.at[z, x, c], dev(f, z, other))

    def wo_wait(j, xx, c):
        ref = wo_unit(x, j, xx, c)
        remote(ref, ref, s_wox.at[0, 0, c], r_wo.at[j, xx, c], here).wait_recv()

    def wo_cross(j, xx, c):
        ref = wo_unit(x, j, xx, c)
        return remote(ref, ref, s_wox.at[j, xx, c], r_wox.at[j, xx, c], dev(f, z, other))

    def wox_wait(j, xx, c):
        ref = wo_unit(other, j, xx, c)
        remote(ref, ref, s_wox.at[0, 0, c], r_wox.at[j, xx, c], here).wait_recv()

    def seg_same():
        return remote(seg_buf.at[1, x], seg_buf.at[1, x], s_seg.at[0], r_seg.at[1, x], dev(f, z, other))

    def seg_next(xx):
        return remote(
            seg_buf.at[1, x], seg_buf.at[0, x], s_seg.at[1 + xx], r_seg.at[0, x], dev(f, z + 1, xx)
        )

    barrier = pltpu.get_barrier_semaphore()

    def greet(ff, zz, xx):
        pl.semaphore_signal(
            barrier, inc=1, device_id=dev(ff, zz, xx), device_id_type=pl.DeviceIdType.MESH
        )

    plane = nf * nx
    for step in (1, -1):
        @pl.when((z + step >= 0) & (z + step < nz))
        def _():
            for xx in range(nx):
                greet(f, z + step, xx)

    for d in range(1, plane):
        greet(lax.rem(f + d, nf), z, lax.rem(x + d // nf, nx))
    pl.semaphore_wait(barrier, plane - 1 + jnp.where(is_end, nx, 2 * nx))

    own_wkv.wait()
    own_wq.wait()

    @pl.when(is_end)
    def _():
        go("end", lambda: wkv_z(z, 1, n))
        go("end", lambda: wq_z(z, 1, n))

    @pl.when(is_inner)
    def _():
        for d, target in ((0, e), (1, m)):
            go("inner", lambda d=d, target=target: wkv_z(z, d, target))
            go("inner", lambda d=d, target=target: wq_z(z, d, target))

    own_h.wait()
    go("all", hid_send)
    own_seg.wait()
    go("all", seg_same)

    @pl.when(z < nz - 1)
    def _():
        for xx in range(nx):
            seg_next(xx).start()

    for copy in own_wo:
        copy.wait()

    @pl.when(is_end)
    def _():
        for hf in range(2):
            go("end", lambda hf=hf: he_z(hf))
        for c in range(WO_CHUNKS):
            go("end", lambda c=c: wo_pair(c))
        for c in range(END_CHUNKS):
            go("end", lambda c=c: wo_cross(z, x, c))

    @pl.when(is_inner)
    def _():
        for c in range(WO_CHUNKS):
            go("inner", lambda c=c: wo_z(z, x, c, 0, e))

    @pl.when(z == 0)
    def _():
        kv_all[0] = jnp.zeros(kv_all.shape[1:], bf16)
        seg_buf[0] = jnp.full(seg_buf.shape[1:], NEG_POS, jnp.int32)

    @pl.when(is_inner)
    def _():
        q_in[...] = jnp.zeros(q_in.shape, f32)

    def table(row_count, first, lane_index):
        position = (first + lax.broadcasted_iota(jnp.int32, (row_count, HD), 0)).astype(f32)
        frequency = jnp.exp(lane_index.astype(f32) * (-2.0 * math.log(ROPE_BASE) / HD))
        return position * frequency

    lane = lax.broadcasted_iota(jnp.int32, (1, HD), 1)
    half = HD // 2
    quarter = half // nx
    kv_angle = table(sub, z * rows + f * sub, x * quarter + lane % quarter)
    is_key = lane < half
    kv_cos = jnp.where(is_key, jnp.cos(kv_angle), 1.0)
    kv_sin = jnp.where(is_key, jnp.sin(kv_angle), 0.0)
    kv_sin = jnp.where(lane < quarter, -kv_sin, kv_sin)
    q_angle = table(rows, z * rows, lane % half)
    q_sine = jnp.sin(q_angle)
    q_cos[...] = jnp.cos(q_angle)
    q_sin[...] = jnp.where(lane < half, -q_sine, q_sine)

    def q_send(j):
        return remote(q_part.at[j], q_recv.at[f], s_q.at[j], r_q.at[f], (j, s))

    def q_spread(j):
        @pl.when(j != f)
        def _():
            q_send(j).start()

    def q_project(j):
        q_part[j] = jnp.dot(h_buf[...], wq_buf[j], preferred_element_type=f32)
        q_spread(j)

    def q_kept(j):
        q_part[j] = jnp.dot(
            h_buf[:, moved:], wq_buf[j, moved:, :], preferred_element_type=f32
        )
        q_spread(j)

    def e_send(j, xx, hf):
        return remote(
            e_part.at[j, xx, hf], e_recv.at[f, xx, hf], s_ep.at[j, xx, hf], r_ep.at[f, xx, hf], (j, s)
        )

    def e_project(xx, hf, blocks):
        for j in blocks:
            e_part[j, xx, hf] = jnp.dot(
                h_end[xx, hf], wq_buf[j, 0:moved, :], preferred_element_type=f32
            )

            @pl.when(j != f)
            def _():
                e_send(j, xx, hf).start()


    def e_return(xx, hf):
        return remote(
            e_back.at[xx, hf], q_in.at[xx, hf], s_eb.at[xx, hf], r_eb.at[xx, hf], dev(f, e, x)
        )

    def e_collect(xx, hf):
        part = e_part[f, xx, hf]
        for d in range(1, nf):
            ff = lax.rem(f + d, nf)
            remote(
                e_recv.at[ff, xx, hf], e_recv.at[ff, xx, hf],
                s_ep.at[0, xx, hf], r_ep.at[ff, xx, hf], here,
            ).wait_recv()
            part = part + e_recv[ff, xx, hf]
        e_back[xx, hf] = part
        go("inner", lambda: e_return(xx, hf))

    @pl.when(is_inner)
    def _():
        wkv_wait(e)
        go("inner", lambda: wkv_z(e, 1, m))
        wkv_wait(m)
        go("inner", lambda: wkv_z(m, 0, e))
        wq_wait(e)
        go("inner", lambda: wq_z(e, 1, m))
        wq_wait(m)
        go("inner", lambda: wq_z(m, 0, e))
        wkv_wait(e2)
        go("inner", lambda: wkv_z(e2, 0, e))
        he_wait(x, 0)
        go("inner", lambda: he_x(0))

    hid_wait()

    @pl.when(is_inner)
    def _():
        for j in (z, e, m):
            q_project(j)

    @pl.when(is_end)
    def _():
        q_kept(z)
        wq_wait(n, 0)
        q_kept(n)
        for j in (n, m, e2):
            wkv_wait(j)

    kv_part[...] = lax.dot_general(
        h_buf[...], wkv_buf[...], (((1,), (1,)), ((), ())), preferred_element_type=f32
    )

    def kvp_send(d):
        ff = lax.rem(f + d, nf)
        return remote(
            kv_part.at[tile(ff, sub)], kv_recv.at[f], s_kvp.at[d - 1], r_kvp.at[f], (ff, s)
        )

    def kvp_wait(d):
        ff = lax.rem(f + d, nf)
        remote(
            kv_part.at[tile(ff, sub)], kv_recv.at[ff], s_kvp.at[d - 1], r_kvp.at[ff], here
        ).wait_recv()

    for d in range(1, nf):
        go("all", lambda d=d: kvp_send(d))

    @pl.when(is_inner)
    def _():
        he_wait(x, 1)
        go("inner", lambda: he_x(1))
        for c in range(WO_CHUNKS):
            go("inner", lambda c=c: wo_pair(c))
        e_project(x, 0, (z, e, m))

    @pl.when(is_end)
    def _():
        wq_wait(m, 0)
        q_kept(m)

    total = kv_part[tile(f, sub), :]
    for d in range(1, nf):
        kvp_wait(d)
        total = total + kv_recv[lax.rem(f + d, nf)]
    partner = jnp.where(
        lane < quarter, pltpu.roll(total, HD - quarter, 1), pltpu.roll(total, quarter, 1)
    )
    kv_piece[...] = (total * kv_cos + partner * kv_sin).astype(bf16)
    piece_rows = tile(f, sub)
    own_piece = pltpu.make_async_copy(kv_piece, kv_all.at[1, x, piece_rows], s_loc.at[6])
    own_piece.start()

    def kv_send(plane, dx, d):
        ff, xx = lax.rem(f + d, nf), lax.rem(x + dx, nx)
        slot = kv_all.at[plane, x, piece_rows]
        return remote(
            kv_piece if plane else slot, slot,
            s_kv.at[plane, dx, d], r_kv.at[plane, x, f], dev(ff, z, xx),
        )

    def kv_next():
        return remote(
            kv_piece, kv_all.at[0, x, piece_rows],
            s_kv.at[0, 0, 0], r_kv.at[0, x, f], dev(f, z + 1, x),
        )

    def kv_wait(plane, dx, d):
        ff, xx = lax.rem(f + d, nf), lax.rem(x + dx, nx)
        remote(
            kv_piece, kv_all.at[plane, xx, tile(ff, sub)],
            s_kv.at[plane, dx, d], r_kv.at[plane, xx, ff], here,
        ).wait_recv()

    pairs = [(dx, d) for dx in range(nx) for d in range(nf)]
    for pair in pairs[1:]:
        go("all", lambda pair=pair: kv_send(1, *pair))

    @pl.when(z < nz - 1)
    def _():
        kv_next().start()

    @pl.when(is_end)
    def _():
        for c in range(WO_CHUNKS):
            go("end", lambda c=c: wo_z(z, x, c, 1, n))
        for c in range(WO_CHUNKS):
            wo_wait(z, other, c)
            go("end", lambda c=c: wo_z(z, other, c, 1, n))

    @pl.when(is_inner)
    def _():
        for c in range(WO_CHUNKS):
            go("inner", lambda c=c: wo_z(z, x, c, 1, m))
        wq_wait(e2)
        go("inner", lambda: wq_z(e2, 0, e))
        q_project(e2)
        e_project(x, 0, (e2,))
        he_wait(other, 0)
        e_project(other, 0, (z, e, m, e2))
        e_project(x, 1, (z, e, m, e2))
        e_collect(x, 0)

    @pl.when(z > 0)
    def _():
        kv_wait(0, 0, 0)
        for pair in pairs[1:]:
            kv_send(0, *pair).start()

    @pl.when(is_inner)
    def _():
        he_wait(other, 1)
        e_project(other, 1, (z, e, m, e2))
        for c in range(WO_CHUNKS):
            wo_wait(m, x, c)
            go("inner", lambda c=c: wo_z(m, x, c, 0, e))
        e_collect(other, 0)
        e_collect(x, 1)

    @pl.when(is_end)
    def _():
        wq_wait(e2, 0)
        q_kept(e2)
        for xx in range(nx):
            for hf in range(2):
                remote(
                    q_in.at[xx, hf], q_in.at[xx, hf], s_eb.at[xx, hf], r_eb.at[xx, hf], here
                ).wait_recv()

    q_total = q_part[f]
    for d in range(1, nf):
        ff = lax.rem(f + d, nf)
        remote(q_part.at[0], q_recv.at[ff], s_q.at[0], r_q.at[ff], here).wait_recv()
        q_total = q_total + q_recv[ff]
    returned = q_in[...].reshape(rows, HD)
    q_total = q_total + jnp.where(is_end, returned, 0.0)
    q_turned = q_total * q_cos[...] + pltpu.roll(q_total, half, 1) * q_sin[...]
    q_head = q_turned.astype(bf16).astype(f32)
    quarters = []
    for xx in range(nx):
        first = q_head if xx == 0 else pltpu.roll(q_head, HD - xx * quarter, 1)
        second = pltpu.roll(q_head, (HD - half - xx * quarter + quarter) % HD, 1)
        picked = jnp.where(lane < quarter, first, jnp.where(lane < half, second, 0.0))
        quarters.append(picked.astype(bf16))

    seg_wait = lambda plane, xx: remote(
        seg_buf.at[plane, xx], seg_buf.at[plane, xx], s_seg.at[0], r_seg.at[plane, xx], here
    ).wait_recv()
    seg_wait(1, other)
    own_piece.wait()
    for pair in pairs[1:]:
        kv_wait(1, *pair)

    @pl.when(z > 0)
    def _():
        for xx in range(nx):
            seg_wait(0, xx)
        for pair in pairs[1:]:
            kv_wait(0, *pair)

    key_seg = jnp.concatenate(
        [seg_buf[plane, xx] for plane in range(2) for xx in range(nx)], axis=1
    )
    own_seg_row = key_seg[:, rows:]
    seg_column = jnp.transpose(jnp.broadcast_to(own_seg_row, (HD, rows)))[:, :1]
    key_pos = lax.broadcasted_iota(jnp.int32, (1, 2 * rows), 1) - rows
    keys = [
        jnp.concatenate([kv_all[0, xx], kv_all[1, xx]], axis=0) for xx in range(nx)
    ]
    step_rows = rows // nf
    for b in range(nf):
        span = slice(b * step_rows, (b + 1) * step_rows)
        query_pos = b * step_rows + lax.broadcasted_iota(jnp.int32, (step_rows, 1), 0)
        score = None
        for xx in range(nx):
            term = lax.dot_general(
                quarters[xx][span], keys[xx], (((1,), (1,)), ((), ())),
                preferred_element_type=f32,
            )
            score = term if score is None else score + term
        allowed = (key_pos <= query_pos) & (key_seg == seg_column[span])
        masked = jnp.where(allowed, score * HD ** (-0.5), NEG_FILL)
        row_max = jnp.max(masked, axis=1, keepdims=True)
        weight = jnp.where(allowed, jnp.exp(masked - row_max), 0.0)
        row_total = jnp.sum(weight, axis=1, keepdims=True)
        rounded = weight.astype(bf16)
        product = [
            jnp.dot(rounded, keys[xx], preferred_element_type=f32) for xx in range(nx)
        ]
        mixed = None
        for xx in reversed(range(nx)):
            first = pltpu.roll(product[xx], (half + xx * quarter) % HD, 1)
            second = pltpu.roll(product[xx], (HD - (nx - 1 - xx) * quarter) % HD, 1)
            lane_block = lane // quarter
            value = jnp.where(lane_block < nx, first, second)
            mixed = value if mixed is None else jnp.where(lane_block % nx == xx, value, mixed)
        mix_own[span, :] = (mixed / row_total).astype(bf16)

    head = f * nx + x

    ahead = lax.rem(f + 2, nf)
    beside = f + 1 - 2 * lax.rem(f, 2)
    across = lax.rem(beside + 2, nf)

    def mix_of(ff, xx):
        return mix_buf.at[:, tile(ff * nx + xx, HD)]

    def mix_send(ff, xx, hop):
        target = (dev(f, z, other), dev(ahead, z, x), dev(beside, z, x))[hop]
        return remote(
            mix_of(ff, xx), mix_of(ff, xx), s_mix.at[hop, xx, ff], r_mix.at[xx, ff], target
        )

    def mix_wait(ff, xx):
        remote(
            mix_of(ff, xx), mix_of(ff, xx), s_mix.at[0, xx, ff], r_mix.at[xx, ff], here
        ).wait_recv()

    mix_buf[:, tile(head, HD)] = mix_own[...]
    for hop in range(3):
        go("all", lambda hop=hop: mix_send(f, x, hop))

    @pl.when(is_inner)
    def _():
        e_collect(other, 1)
        for c in range(WO_CHUNKS):
            wo_wait(z, other, c)
            go("inner", lambda c=c: wo_z(z, other, c, 1, m))
            go("inner", lambda c=c: wo_z(z, other, c, 0, e))

    @pl.when(is_end)
    def _():
        for xx in (x, other):
            for c in range(WO_CHUNKS):
                wo_wait(n, xx, c)
                if c < END_CHUNKS:
                    go("end", lambda xx=xx, c=c: wo_cross(n, xx, c))

    mix_wait(f, other)
    for hop in (1, 2):
        go("all", lambda hop=hop: mix_send(f, other, hop))
    mix_wait(ahead, x)
    go("all", lambda: mix_send(ahead, x, 2))

    @pl.when(is_inner)
    def _():
        for xx in (x, other):
            for c in range(WO_CHUNKS):
                wo_wait(e, xx, c)
                go("inner", lambda xx=xx, c=c: wo_z(e, xx, c, 1, m))

    mix_wait(ahead, other)
    go("all", lambda: mix_send(ahead, other, 2))

    def result(h, c):
        where = pl.ds(pl.multiple_of(h * half_cols + c * chunk, chunk), chunk)
        return pltpu.make_async_copy(out_buf.at[h, :, cols(c)], out.at[:, where], s_res.at[h, c])

    @pl.when(is_inner)
    def _():
        for c in range(WO_CHUNKS):
            wo_wait(m, other, c)
            go("inner", lambda c=c: wo_z(m, other, c, 0, e))
        for xx in (x, other):
            for c in range(WO_CHUNKS):
                wo_wait(e2, xx, c)
                go("inner", lambda xx=xx, c=c: wo_z(e2, xx, c, 0, e))

    for ff in (beside, across):
        for xx in (x, other):
            mix_wait(ff, xx)

    @pl.when(is_end)
    def _():
        for j in (m, e2):
            for xx in (x, other):
                for c in range(WO_CHUNKS):
                    wo_wait(j, xx, c)
                    if c < END_CHUNKS:
                        go("end", lambda j=j, xx=xx, c=c: wo_cross(j, xx, c))

    def product(h, c, row_tile):
        return jnp.dot(
            mix_buf[tile(row_tile, tok), :], wo_buf[h, :, cols(c)], preferred_element_type=f32
        ).astype(bf16)

    def away(c):
        return remote(
            out_away.at[c], out_buf.at[x, :, cols(c)], s_out.at[c], r_out.at[c], dev(f, z, other)
        )

    def away_stage(kind, c):
        out_away[c] = product(x, c, other)
        go(kind, lambda: away(c))

    def own_stage(h, c):
        out_buf[h, :, cols(c)] = product(h, c, x)
        result(h, c).start()

    def away_wait(c):
        ref = out_buf.at[other, :, cols(c)]
        remote(ref, ref, s_out.at[c], r_out.at[c], here).wait_recv()
        result(other, c).start()

    for c in range(END_CHUNKS, WO_CHUNKS):
        away_stage("all", c)

    @pl.when(is_inner)
    def _():
        for c in range(END_CHUNKS):
            away_stage("inner", c)

    for c in range(WO_CHUNKS):
        own_stage(x, c)

    @pl.when(is_end)
    def _():
        for c in range(END_CHUNKS):
            wox_wait(z, other, c)
            for j in (n, m, e2):
                for xx in range(nx):
                    wox_wait(j, xx, c)
            own_stage(other, c)

    for c in range(END_CHUNKS, WO_CHUNKS):
        away_wait(c)

    @pl.when(is_inner)
    def _():
        for c in range(END_CHUNKS):
            away_wait(c)

    for make in pending["all"]:
        make().wait_send()
    for kind, cond in (("end", is_end), ("inner", is_inner)):
        @pl.when(cond)
        def _():
            for make in pending[kind]:
                make().wait_send()

    for d in range(1, nf):
        q_send(lax.rem(f + d, nf)).wait_send()

    @pl.when(is_inner)
    def _():
        for d in range(1, nf):
            for xx in range(nx):
                for hf in range(2):
                    e_send(lax.rem(f + d, nf), xx, hf).wait_send()

    @pl.when(z < nz - 1)
    def _():
        for xx in range(nx):
            seg_next(xx).wait_send()
        kv_next().wait_send()

    @pl.when(z > 0)
    def _():
        for pair in pairs[1:]:
            kv_send(0, *pair).wait_send()

    for h in range(nx):
        for c in range(WO_CHUNKS):
            result(h, c).wait()


def fused_on_device(nf, nz, nx, hidden, w_query, w_keyvalue, w_output, segment_ids):
    tok, kdim = hidden.shape
    cols = w_output.shape[1]
    rows = tok * nx
    sub = rows // nf
    kvw = w_keyvalue.shape[1]
    heads = nz * nx
    part = cols // nx
    f32, bf16 = jnp.float32, jnp.bfloat16
    dma = pltpu.SemaphoreType.DMA
    vmem = pl.BlockSpec(memory_space=pltpu.VMEM)
    anywhere = pl.BlockSpec(memory_space=pl.ANY)
    scratch = [
        pltpu.VMEM((rows, kdim), bf16),
        pltpu.VMEM((nz, kdim, HD), bf16),
        pltpu.VMEM((nz * kvw, kdim), bf16),
        pltpu.VMEM((nx, heads * HD, part), bf16),
        pltpu.VMEM((2, nx, 1, tok), jnp.int32),
        pltpu.VMEM((nz, rows, HD), f32),
        pltpu.VMEM((nf, rows, HD), f32),
        pltpu.VMEM((rows, nz * kvw), f32),
        pltpu.VMEM((nf, sub, nz * kvw), f32),
        pltpu.VMEM((sub, HD), bf16),
        pltpu.VMEM((2, nx, rows, HD), bf16),
        pltpu.VMEM((rows, HD), bf16),
        pltpu.VMEM((rows, heads * HD), bf16),
        pltpu.VMEM((rows, HD), f32),
        pltpu.VMEM((rows, HD), f32),
        pltpu.VMEM((nx, tok, part), bf16),
        pltpu.VMEM((WO_CHUNKS, tok, part // WO_CHUNKS), bf16),
        pltpu.VMEM((nx, 2, tok // 2, kdim * MOVED // 8), bf16),
        pltpu.VMEM((nz, nx, 2, tok // 2, HD), f32),
        pltpu.VMEM((nf, nx, 2, tok // 2, HD), f32),
        pltpu.VMEM((nx, 2, tok // 2, HD), f32),
        pltpu.VMEM((nx, 2, tok // 2, HD), f32),
        dma((7,)), dma, dma, dma((1 + nx,)), dma((2, nx)),
        dma((2, nz)), dma((nz,)), dma((2, nz)), dma((nz,)),
        dma((nz,)), dma((nf,)), dma((nf,)), dma((nf,)),
        dma((2, nx, nf)), dma((2, nx, nf)),
        dma((2, nz, nx, WO_CHUNKS)), dma((nz, nx, WO_CHUNKS)),
        dma((nz + 1, nx, WO_CHUNKS)), dma((nz, nx, WO_CHUNKS)),
        dma((3, nx, nf)), dma((nx, nf)),
        dma((WO_CHUNKS,)), dma((WO_CHUNKS,)), dma((nx, WO_CHUNKS)),
        dma((2,)), dma((nx, 2)), dma((2,)), dma((nz, nx, 2)), dma((nf, nx, 2)),
        dma((nx, 2)), dma((nx, 2)),
    ]
    return pl.pallas_call(
        functools.partial(fused_kernel, nf, nz, nx),
        out_shape=jax.ShapeDtypeStruct((tok, cols), bf16),
        in_specs=[anywhere] * 4 + [vmem],
        out_specs=anywhere,
        scratch_shapes=scratch,
        name="fused_sublayer",
        compiler_params=pltpu.CompilerParams(
            collective_id=0, has_side_effects=True, vmem_limit_bytes=60 * 1024 * 1024
        ),
    )(hidden, w_query, w_keyvalue.T, w_output, segment_ids.reshape(1, tok))


def solution(mesh):
    in_specs = (P("sp", "fsdp"), P("fsdp", "sp"), P("fsdp", "sp"), P("sp", "fsdp"), P("sp"))
    out_specs = P("sp", "fsdp")
    nf, sp = mesh.shape["fsdp"], mesh.shape["sp"]
    if sp == GROUP and sp == 2 * nf:
        body = functools.partial(fused_on_device, nf, nf, sp // nf)
    else:
        body = on_device
    return jax.shard_map(
        body, mesh=mesh, in_specs=in_specs, out_specs=out_specs, check_vma=False
    )
```

```python
import functools
import math

import jax
import jax.numpy as jnp
from jax import lax
from jax.experimental import pallas as pl
from jax.experimental.pallas import tpu as pltpu
from jax.sharding import PartitionSpec as P

HD = 128
GROUP = 8


ROPE_BASE = 500000.0
NEG_FILL = -1e30


def rotate(values, positions, head_count, width):
    row_count = values.shape[0]
    shaped = values.reshape(row_count, head_count, width)
    half_width = width // 2
    frequency = jnp.exp(
        jnp.arange(half_width, dtype=jnp.float32) * (-2.0 * math.log(ROPE_BASE) / width)
    )
    angles = positions.astype(jnp.float32)[:, None] * frequency[None, :]
    cosine = jnp.cos(angles)[:, None, :]
    sine_part = jnp.sin(angles)[:, None, :]
    lower_half = shaped[:, :, :half_width]
    upper_half = shaped[:, :, half_width:]
    turned = jnp.concatenate(
        [
            lower_half * cosine - upper_half * sine_part,
            upper_half * cosine + lower_half * sine_part,
        ],
        axis=2,
    )
    return turned.reshape(row_count, head_count * width)


def split_keys(kv_sum, positions, kv_count, width):
    row_count = kv_sum.shape[0]
    shaped = kv_sum.reshape(row_count, kv_count, 2, width)
    key_part = rotate(
        shaped[:, :, 0, :].reshape(row_count, kv_count * width), positions, kv_count, width
    )
    key_part = key_part.reshape(row_count, kv_count, 1, width)
    return jnp.concatenate([key_part, shaped[:, :, 1:2, :]], axis=2).astype(jnp.bfloat16)


def merge_keys(
    state_in, query_tile, query_pos_tile, query_seg_tile, key_tile, key_pos_tile, key_seg_tile
):
    running_max, running_sum, weighted = state_in
    allowed = (key_pos_tile[None, :] <= query_pos_tile[:, None]) & (
        key_seg_tile[None, :] == query_seg_tile[:, None]
    )
    key_part = key_tile[:, :HD]
    value_part = key_tile[:, HD:]
    scores = lax.dot_general(
        query_tile, key_part, (((1,), (1,)), ((), ())), preferred_element_type=jnp.float32
    ) * HD ** (-0.5)
    masked = jnp.where(allowed, scores, NEG_FILL)
    new_max = jnp.maximum(running_max, jnp.max(masked, axis=1))
    weights = jnp.where(allowed, jnp.exp(masked - new_max[:, None]), 0.0)
    new_sum = jnp.sum(weights, axis=1)
    new_weighted = jnp.dot(
        weights.astype(jnp.bfloat16), value_part, preferred_element_type=jnp.float32
    )
    return (new_max, new_sum, new_weighted)


def on_device(hidden, w_query, w_keyvalue, w_output, segment_ids):
    fsdp_count = lax.axis_size("fsdp")
    seq_count = lax.axis_size("sp")
    fsdp_index = lax.axis_index("fsdp")
    seq_index = lax.axis_index("sp")
    tok_rows = hidden.shape[0]
    sub_rows = tok_rows // fsdp_count
    kv_count = seq_count // GROUP
    query_rows = seq_count * sub_rows
    offsets = jnp.arange(query_rows, dtype=jnp.int32)
    query_pos = offsets // sub_rows * tok_rows + fsdp_index * sub_rows + offsets % sub_rows
    own_positions = (
        seq_index * tok_rows + fsdp_index * sub_rows + jnp.arange(sub_rows, dtype=jnp.int32)
    )

    def project(weight_block):
        return jnp.dot(hidden, weight_block, preferred_element_type=jnp.float32)

    query_part = project(lax.all_gather(w_query, "sp", axis=1, tiled=True))
    kv_part = project(lax.all_gather(w_keyvalue, "sp", axis=1, tiled=True))
    query_sum, kv_sum = (
        lax.psum_scatter(query_part, "fsdp", scatter_dimension=0, tiled=True),
        lax.psum_scatter(kv_part, "fsdp", scatter_dimension=0, tiled=True),
    )
    query_local = rotate(query_sum, own_positions, seq_count, HD).astype(jnp.bfloat16)
    pairs = split_keys(kv_sum, own_positions, kv_count, HD)
    expanded = jnp.repeat(pairs, GROUP, axis=1).reshape(sub_rows, seq_count * 2 * HD)
    query_head, kv_head = (
        lax.all_to_all(query_local, "sp", split_axis=1, concat_axis=0, tiled=True),
        lax.all_to_all(expanded, "sp", split_axis=1, concat_axis=0, tiled=True),
    )
    segment_all = lax.all_gather(segment_ids, "sp", axis=0, tiled=True)
    query_seg = segment_all[query_pos]
    initial = (
        jnp.full((query_rows,), NEG_FILL, jnp.float32),
        jnp.zeros((query_rows,), jnp.float32),
        jnp.zeros((query_rows, HD), jnp.float32),
    )
    block_keys = lax.all_gather(kv_head, "fsdp", axis=0, tiled=True)
    piece_rows = block_keys.shape[0]
    row_ids = jnp.arange(piece_rows, dtype=jnp.int32)
    source_id = row_ids // query_rows
    within = row_ids % query_rows
    key_pos = within // sub_rows * tok_rows + source_id * sub_rows + within % sub_rows
    key_seg = segment_all[key_pos]
    final_max, final_sum, final_weighted = merge_keys(
        initial, query_head, query_pos, query_seg, block_keys, key_pos, key_seg
    )
    attention = (final_weighted / final_sum[:, None]).astype(jnp.bfloat16)
    back_rows = lax.all_to_all(attention, "sp", split_axis=0, concat_axis=1, tiled=True)
    mixed_rows = lax.all_gather(back_rows, "fsdp", axis=0, tiled=True)
    result = jnp.dot(
        mixed_rows,
        lax.all_gather(w_output, "sp", axis=0, tiled=True),
        preferred_element_type=jnp.float32,
    )
    return result.astype(jnp.bfloat16)


NEG_POS = -1
WO_CHUNKS = 4
MOVED = 4
END_CHUNKS = 2


def fused_kernel(
    nf, nz, nx, hid, wq, wkv, wo, seg, out,
    h_buf, wq_buf, wkv_buf, wo_buf, seg_buf,
    q_part, q_mate, q_sum, q_far, kv_part, kv_recv, kv_piece, kv_all, mix_own, mix_buf, q_cos, q_sin,
    out_buf, out_away, h_end, e_part, e_mate, e_sum, e_far, e_back, q_in,
    s_loc, s_hid, r_hid, s_seg, r_seg, s_wkv, r_wkv, s_wq, r_wq,
    s_q, r_q, s_qf, r_qf, s_kvp, r_kvp, s_kv, r_kv, s_wo, r_wo, s_wox, r_wox, s_mix, r_mix,
    s_out, r_out, s_res, s_he, r_he, s_hx, s_ep, r_ep, s_ef, r_ef, s_eb, r_eb,
):
    f = lax.axis_index("fsdp")
    s = lax.axis_index("sp")
    z, x = s // nx, s % nx
    tok, kdim = hid.shape
    rows = tok * nx
    sub = rows // nf
    kvw = wkv.shape[0]
    other = 1 - x
    moved = kdim * MOVED // 8
    block = tok // 2
    half_cols = wo.shape[1] // nx
    chunk = half_cols // WO_CHUNKS
    f32, bf16 = jnp.float32, jnp.bfloat16
    is_end = (z == 0) | (z == nz - 1)
    is_inner = jnp.logical_not(is_end)
    low = z < nz // 2
    e = jnp.where(low, 0, nz - 1)
    n = jnp.where(low, 1, nz - 2)
    m = nz - 1 - n
    e2 = nz - 1 - e
    beside = f + 1 - 2 * lax.rem(f, 2)
    ahead = lax.rem(f + 2, nf)
    across = lax.rem(beside + 2, nf)

    def block_of(ff):
        return lax.rem(ff, 2) * 2 + ff // 2

    core = lax.rem(f, 2)
    mine, theirs = block_of(f), block_of(ahead)
    near = core == z // 2

    def dev(ff, zz, xx):
        return (ff, zz * nx + xx)

    def remote(src, dst, ss, rs, target):
        return pltpu.make_async_remote_copy(
            src_ref=src, dst_ref=dst, send_sem=ss, recv_sem=rs,
            device_id=target, device_id_type=pl.DeviceIdType.MESH,
        )

    def tile(ref, count):
        return pl.ds(pl.multiple_of(ref * count, count), count)

    here = (f, s)
    pending = {"all": [], "end": [], "inner": []}

    def go(kind, make):
        make().start()
        pending[kind].append(make)

    def cols(c):
        return slice(c * chunk, (c + 1) * chunk)

    own_h = pltpu.make_async_copy(hid, h_buf.at[tile(x, tok)], s_loc.at[0])
    own_wq = pltpu.make_async_copy(
        wq, wq_buf.at[z // 2, :, tile(lax.rem(z, 2), HD)], s_loc.at[1]
    )
    own_wkv = pltpu.make_async_copy(wkv, wkv_buf.at[tile(z, kvw)], s_loc.at[2])
    own_wo = [
        pltpu.make_async_copy(
            wo.at[:, h * half_cols : (h + 1) * half_cols],
            wo_buf.at[h, tile(s, HD)], s_loc.at[3 + h],
        )
        for h in range(nx)
    ]
    own_seg = pltpu.make_async_copy(seg, seg_buf.at[1, x], s_loc.at[5])
    for copy in (own_wkv, own_wq, own_h, *own_wo, own_seg):
        copy.start()

    def hid_send():
        return remote(
            h_buf.at[tile(x, tok)], h_buf.at[tile(x, tok)], s_hid, r_hid, dev(f, z, other)
        )

    def hid_wait():
        remote(
            h_buf.at[tile(other, tok)], h_buf.at[tile(other, tok)], s_hid, r_hid, here
        ).wait_recv()

    def wkv_z(j, d, target):
        ref = wkv_buf.at[tile(j, kvw)]
        return remote(ref, ref, s_wkv.at[d, j], r_wkv.at[j], dev(f, target, x))

    def wkv_wait(j):
        wkv_z(j, 0, z).wait_recv()

    def wq_of(j, first):
        return wq_buf.at[j // 2, first:, tile(lax.rem(j, 2), HD)]

    def wq_z(j, d, target):
        ref = wq_of(j, 0) if d else wq_of(j, moved)
        return remote(ref, ref, s_wq.at[d, j], r_wq.at[j], dev(f, target, x))

    def wq_wait(j, d=1):
        wq_z(j, d, z).wait_recv()

    def he_z(hf):
        rows_of = pl.ds(pl.multiple_of(x * tok + hf * block, block), block)
        return remote(
            h_buf.at[rows_of, 0:moved], h_end.at[x, hf], s_he.at[hf], r_he.at[x, hf], dev(f, n, x)
        )

    def he_x(hf):
        ref = h_end.at[x, hf]
        return remote(ref, ref, s_hx.at[hf], r_he.at[x, hf], dev(f, z, other))

    def he_wait(xx, hf):
        ref = h_end.at[xx, hf]
        remote(ref, ref, s_hx.at[hf], r_he.at[xx, hf], here).wait_recv()

    def wo_unit(h, j, xx, c):
        return wo_buf.at[h, tile(j * nx + xx, HD), cols(c)]

    def wo_z(j, xx, c, d, target):
        ref = wo_unit(x, j, xx, c)
        return remote(ref, ref, s_wo.at[d, j, xx, c], r_wo.at[j, xx, c], dev(f, target, x))

    def wo_pair(c):
        ref = wo_unit(other, z, x, c)
        return remote(ref, ref, s_wox.at[nz, x, c], r_wo.at[z, x, c], dev(f, z, other))

    def wo_wait(j, xx, c):
        ref = wo_unit(x, j, xx, c)
        remote(ref, ref, s_wox.at[0, 0, c], r_wo.at[j, xx, c], here).wait_recv()

    def wo_cross(j, xx, c):
        ref = wo_unit(x, j, xx, c)
        return remote(ref, ref, s_wox.at[j, xx, c], r_wox.at[j, xx, c], dev(f, z, other))

    def wox_wait(j, xx, c):
        ref = wo_unit(other, j, xx, c)
        remote(ref, ref, s_wox.at[0, 0, c], r_wox.at[j, xx, c], here).wait_recv()

    def seg_same():
        return remote(seg_buf.at[1, x], seg_buf.at[1, x], s_seg.at[0], r_seg.at[1, x], dev(f, z, other))

    def seg_next(xx):
        return remote(
            seg_buf.at[1, x], seg_buf.at[0, x], s_seg.at[1 + xx], r_seg.at[0, x], dev(f, z + 1, xx)
        )

    barrier = pltpu.get_barrier_semaphore()

    def greet(ff, zz, xx):
        pl.semaphore_signal(
            barrier, inc=1, device_id=dev(ff, zz, xx), device_id_type=pl.DeviceIdType.MESH
        )

    plane = nf * nx
    for step in (1, -1):
        @pl.when((z + step >= 0) & (z + step < nz))
        def _():
            for xx in range(nx):
                greet(f, z + step, xx)

    for d in range(1, plane):
        greet(lax.rem(f + d, nf), z, lax.rem(x + d // nf, nx))
    pl.semaphore_wait(barrier, plane - 1 + jnp.where(is_end, nx, 2 * nx))

    own_wkv.wait()
    own_wq.wait()

    @pl.when(is_end)
    def _():
        go("end", lambda: wkv_z(z, 1, n))
        go("end", lambda: wq_z(z, 1, n))

    @pl.when(is_inner)
    def _():
        for d, target in ((0, e), (1, m)):
            go("inner", lambda d=d, target=target: wkv_z(z, d, target))
            go("inner", lambda d=d, target=target: wq_z(z, d, target))

    own_h.wait()
    go("all", hid_send)
    own_seg.wait()
    go("all", seg_same)

    @pl.when(z < nz - 1)
    def _():
        for xx in range(nx):
            seg_next(xx).start()

    for copy in own_wo:
        copy.wait()

    @pl.when(is_end)
    def _():
        for hf in range(2):
            go("end", lambda hf=hf: he_z(hf))
        for c in range(WO_CHUNKS):
            go("end", lambda c=c: wo_z(z, x, c, 1, n))
        for c in range(WO_CHUNKS):
            go("end", lambda c=c: wo_pair(c))
        for c in range(END_CHUNKS):
            go("end", lambda c=c: wo_cross(z, x, c))

    @pl.when(is_inner)
    def _():
        for c in range(WO_CHUNKS):
            go("inner", lambda c=c: wo_z(z, x, c, 0, e))

    @pl.when(z == 0)
    def _():
        kv_all[0] = jnp.zeros(kv_all.shape[1:], bf16)
        seg_buf[0] = jnp.full(seg_buf.shape[1:], NEG_POS, jnp.int32)

    @pl.when(is_inner)
    def _():
        q_in[...] = jnp.zeros(q_in.shape, f32)

    def table(row_count, first, lane_index):
        position = (first + lax.broadcasted_iota(jnp.int32, (row_count, HD), 0)).astype(f32)
        frequency = jnp.exp(lane_index.astype(f32) * (-2.0 * math.log(ROPE_BASE) / HD))
        return position * frequency

    lane = lax.broadcasted_iota(jnp.int32, (1, HD), 1)
    half = HD // 2
    quarter = half // nx
    kv_angle = table(sub, z * rows + f * sub, x * quarter + lane % quarter)
    is_key = lane < half
    kv_cos = jnp.where(is_key, jnp.cos(kv_angle), 1.0)
    kv_sin = jnp.where(is_key, jnp.sin(kv_angle), 0.0)
    kv_sin = jnp.where(lane < quarter, -kv_sin, kv_sin)
    q_angle = table(rows, z * rows, lane % half)
    q_sine = jnp.sin(q_angle)
    q_cos[...] = jnp.cos(q_angle)
    q_sin[...] = jnp.where(lane < half, -q_sine, q_sine)

    same_core = lambda j: j // 2 == core

    def q_send(j):
        return remote(
            q_part.at[j], q_mate.at[lax.rem(j, 2)], s_q.at[lax.rem(j, 2)], r_q.at[lax.rem(j, 2)], dev(beside, z, x)
        )

    def q_mate_wait(j):
        remote(
            q_mate.at[lax.rem(j, 2)], q_mate.at[lax.rem(j, 2)], s_q.at[0], r_q.at[lax.rem(j, 2)], here
        ).wait_recv()

    def q_far_copy():
        return remote(q_sum, q_far, s_qf, r_qf, dev(ahead, z, x))

    def q_project(j, first):
        both = jnp.dot(
            h_buf[:, first:], wq_buf[j // 2, first:, :], preferred_element_type=f32
        )
        for b in range(2):
            q_part[j // 2 * 2 + b] = both[:, b * HD : (b + 1) * HD]

        @pl.when(jnp.logical_not(same_core(j)))
        def _():
            for b in range(2):
                q_send(j // 2 * 2 + b).start()

    def q_relay(far):
        @pl.when(jnp.logical_not(near) if far else near)
        def _():
            q_mate_wait(theirs)
            q_sum[...] = q_part[theirs] + q_mate[lax.rem(theirs, 2)]
            q_far_copy().start()

    def e_send(j, xx, hf):
        return remote(
            e_part.at[j, xx, hf], e_mate.at[lax.rem(j, 2), xx, hf],
            s_ep.at[lax.rem(j, 2), xx, hf], r_ep.at[lax.rem(j, 2), xx, hf], dev(beside, z, x)
        )

    def e_mate_wait(j, xx, hf):
        ref = e_mate.at[lax.rem(j, 2), xx, hf]
        remote(ref, ref, s_ep.at[0, xx, hf], r_ep.at[lax.rem(j, 2), xx, hf], here).wait_recv()

    def e_far_copy(xx, hf):
        return remote(
            e_sum.at[xx, hf], e_far.at[xx, hf], s_ef.at[xx, hf], r_ef.at[xx, hf], dev(ahead, z, x)
        )

    def e_project(xx, hf, j):
        both = jnp.dot(
            h_end[xx, hf], wq_buf[j // 2, 0:moved, :], preferred_element_type=f32
        )
        for b in range(2):
            e_part[j // 2 * 2 + b, xx, hf] = both[:, b * HD : (b + 1) * HD]

        @pl.when(jnp.logical_not(same_core(j)))
        def _():
            for b in range(2):
                e_send(j // 2 * 2 + b, xx, hf).start()

    def e_relay(xx, hf):
        e_mate_wait(theirs, xx, hf)
        e_sum[xx, hf] = e_part[theirs, xx, hf] + e_mate[lax.rem(theirs, 2), xx, hf]
        e_far_copy(xx, hf).start()

    def e_return(xx, hf):
        return remote(
            e_back.at[xx, hf], q_in.at[xx, hf], s_eb.at[xx, hf], r_eb.at[xx, hf], dev(f, e, x)
        )

    def e_collect(xx, hf):
        e_mate_wait(mine, xx, hf)
        ref = e_far.at[xx, hf]
        remote(ref, ref, s_ef.at[xx, hf], r_ef.at[xx, hf], here).wait_recv()
        e_back[xx, hf] = (
            e_part[mine, xx, hf] + e_mate[lax.rem(mine, 2), xx, hf] + e_far[xx, hf]
        )
        go("inner", lambda: e_return(xx, hf))

    @pl.when(is_inner)
    def _():
        wkv_wait(e)
        go("inner", lambda: wkv_z(e, 1, m))
        wkv_wait(m)
        go("inner", lambda: wkv_z(m, 0, e))
        wq_wait(e)
        go("inner", lambda: wq_z(e, 1, m))
        for c in range(WO_CHUNKS):
            go("inner", lambda c=c: wo_z(z, x, c, 1, m))
        wq_wait(m)
        go("inner", lambda: wq_z(m, 0, e))
        wkv_wait(e2)
        go("inner", lambda: wkv_z(e2, 0, e))
        he_wait(x, 0)
        go("inner", lambda: he_x(0))

    hid_wait()

    @pl.when(is_end)
    def _():
        for j in (n, m, e2):
            wkv_wait(j)

    kv_part[...] = lax.dot_general(
        h_buf[...], wkv_buf[...], (((1,), (1,)), ((), ())), preferred_element_type=f32
    )

    def kvp_send(d):
        ff = lax.rem(f + d, nf)
        return remote(
            kv_part.at[tile(ff, sub)], kv_recv.at[f], s_kvp.at[d - 1], r_kvp.at[f], (ff, s)
        )

    def kvp_wait(d):
        ff = lax.rem(f + d, nf)
        remote(
            kv_part.at[tile(ff, sub)], kv_recv.at[ff], s_kvp.at[d - 1], r_kvp.at[ff], here
        ).wait_recv()

    for d in range(1, nf):
        go("all", lambda d=d: kvp_send(d))

    @pl.when(is_inner)
    def _():
        q_project(z, 0)
        he_wait(x, 1)
        go("inner", lambda: he_x(1))
        q_relay(False)
        e_project(x, 0, z)

        @pl.when(near)
        def _():
            e_relay(x, 0)


    @pl.when(is_end)
    def _():
        wq_wait(n, 0)
        q_project(z, moved)
        q_relay(False)

    total = kv_part[tile(f, sub), :]
    for d in range(1, nf):
        kvp_wait(d)
        total = total + kv_recv[lax.rem(f + d, nf)]
    partner = jnp.where(
        lane < quarter, pltpu.roll(total, HD - quarter, 1), pltpu.roll(total, quarter, 1)
    )
    kv_piece[...] = (total * kv_cos + partner * kv_sin).astype(bf16)
    piece_rows = tile(f, sub)
    own_piece = pltpu.make_async_copy(kv_piece, kv_all.at[1, x, piece_rows], s_loc.at[6])
    own_piece.start()

    def kv_send(plane, dx, d):
        ff, xx = lax.rem(f + d, nf), lax.rem(x + dx, nx)
        slot = kv_all.at[plane, x, piece_rows]
        return remote(
            kv_piece if plane else slot, slot,
            s_kv.at[plane, dx, d], r_kv.at[plane, x, f], dev(ff, z, xx),
        )

    def kv_next():
        return remote(
            kv_piece, kv_all.at[0, x, piece_rows],
            s_kv.at[0, 0, 0], r_kv.at[0, x, f], dev(f, z + 1, x),
        )

    def kv_wait(plane, dx, d):
        ff, xx = lax.rem(f + d, nf), lax.rem(x + dx, nx)
        remote(
            kv_piece, kv_all.at[plane, xx, tile(ff, sub)],
            s_kv.at[plane, dx, d], r_kv.at[plane, xx, ff], here,
        ).wait_recv()

    pairs = [(dx, d) for dx in range(nx) for d in range(nf)]
    for pair in pairs[1:]:
        go("all", lambda pair=pair: kv_send(1, *pair))

    @pl.when(z < nz - 1)
    def _():
        kv_next().start()

    @pl.when(is_end)
    def _():
        for c in range(WO_CHUNKS):
            wo_wait(z, other, c)
            go("end", lambda c=c: wo_z(z, other, c, 1, n))

    @pl.when(is_inner)
    def _():
        wq_wait(e2)
        go("inner", lambda: wq_z(e2, 0, e))
        q_project(e2, 0)
        e_project(x, 0, e2)
        e_project(x, 1, z)
        e_project(x, 1, e2)

        @pl.when(jnp.logical_not(near))
        def _():
            e_relay(x, 0)

        e_relay(x, 1)
        q_relay(True)
        he_wait(other, 0)
        e_project(other, 0, z)
        e_project(other, 0, e2)
        e_relay(other, 0)

    @pl.when(z > 0)
    def _():
        kv_wait(0, 0, 0)
        for pair in pairs[1:]:
            kv_send(0, *pair).start()

    @pl.when(is_inner)
    def _():
        for c in range(WO_CHUNKS):
            go("inner", lambda c=c: wo_pair(c))
        for c in range(WO_CHUNKS):
            wo_wait(e, x, c)
            go("inner", lambda c=c: wo_z(e, x, c, 1, m))
        e_collect(x, 0)
        he_wait(other, 1)
        e_project(other, 1, z)
        e_project(other, 1, e2)
        for c in range(WO_CHUNKS):
            wo_wait(m, x, c)
            go("inner", lambda c=c: wo_z(m, x, c, 0, e))
        e_collect(other, 0)
        e_relay(other, 1)
        e_collect(x, 1)
        for c in range(WO_CHUNKS):
            wo_wait(e, other, c)
            go("inner", lambda c=c: wo_z(e, other, c, 1, m))
        e_collect(other, 1)

    def cross(j, xx):
        for c in range(WO_CHUNKS):
            wo_wait(j, xx, c)
            if c < END_CHUNKS:
                go("end", lambda c=c: wo_cross(j, xx, c))

    @pl.when(is_end)
    def _():
        cross(n, x)
        wq_wait(m, 0)
        wq_wait(e2, 0)
        q_project(e2, moved)
        q_relay(True)
        cross(m, x)
        for xx in range(nx):
            for hf in range(2):
                remote(
                    q_in.at[xx, hf], q_in.at[xx, hf], s_eb.at[xx, hf], r_eb.at[xx, hf], here
                ).wait_recv()

    q_mate_wait(mine)
    remote(q_far, q_far, s_qf, r_qf, here).wait_recv()
    q_total = q_part[mine] + q_mate[lax.rem(mine, 2)] + q_far[...]
    returned = q_in[...].reshape(rows, HD)
    q_total = q_total + jnp.where(is_end, returned, 0.0)
    q_turned = q_total * q_cos[...] + pltpu.roll(q_total, half, 1) * q_sin[...]
    q_head = q_turned.astype(bf16).astype(f32)
    quarters = []
    for xx in range(nx):
        first = q_head if xx == 0 else pltpu.roll(q_head, HD - xx * quarter, 1)
        second = pltpu.roll(q_head, (HD - half - xx * quarter + quarter) % HD, 1)
        picked = jnp.where(lane < quarter, first, jnp.where(lane < half, second, 0.0))
        quarters.append(picked.astype(bf16))

    seg_wait = lambda plane, xx: remote(
        seg_buf.at[plane, xx], seg_buf.at[plane, xx], s_seg.at[0], r_seg.at[plane, xx], here
    ).wait_recv()
    seg_wait(1, other)
    own_piece.wait()
    for pair in pairs[1:]:
        kv_wait(1, *pair)

    @pl.when(z > 0)
    def _():
        for xx in range(nx):
            seg_wait(0, xx)
        for pair in pairs[1:]:
            kv_wait(0, *pair)

    key_seg = jnp.concatenate(
        [seg_buf[plane, xx] for plane in range(2) for xx in range(nx)], axis=1
    )
    own_seg_row = key_seg[:, rows:]
    seg_column = jnp.transpose(jnp.broadcast_to(own_seg_row, (HD, rows)))[:, :1]
    key_pos = lax.broadcasted_iota(jnp.int32, (1, 2 * rows), 1) - rows
    keys = [
        jnp.concatenate([kv_all[0, xx], kv_all[1, xx]], axis=0) for xx in range(nx)
    ]
    step_rows = rows // nf
    for b in range(nf):
        span = slice(b * step_rows, (b + 1) * step_rows)
        query_pos = b * step_rows + lax.broadcasted_iota(jnp.int32, (step_rows, 1), 0)
        score = None
        for xx in range(nx):
            term = lax.dot_general(
                quarters[xx][span], keys[xx], (((1,), (1,)), ((), ())),
                preferred_element_type=f32,
            )
            score = term if score is None else score + term
        allowed = (key_pos <= query_pos) & (key_seg == seg_column[span])
        masked = jnp.where(allowed, score * HD ** (-0.5), NEG_FILL)
        row_max = jnp.max(masked, axis=1, keepdims=True)
        weight = jnp.where(allowed, jnp.exp(masked - row_max), 0.0)
        row_total = jnp.sum(weight, axis=1, keepdims=True)
        rounded = weight.astype(bf16)
        product = [
            jnp.dot(rounded, keys[xx], preferred_element_type=f32) for xx in range(nx)
        ]
        mixed = None
        for xx in reversed(range(nx)):
            first = pltpu.roll(product[xx], (half + xx * quarter) % HD, 1)
            second = pltpu.roll(product[xx], (HD - (nx - 1 - xx) * quarter) % HD, 1)
            lane_block = lane // quarter
            value = jnp.where(lane_block < nx, first, second)
            mixed = value if mixed is None else jnp.where(lane_block % nx == xx, value, mixed)
        mix_own[span, :] = (mixed / row_total).astype(bf16)

    head = mine * nx + x

    def mix_of(ff, xx):
        return mix_buf.at[:, tile(block_of(ff) * nx + xx, HD)]

    def mix_send(ff, xx, hop):
        target = (dev(f, z, other), dev(ahead, z, x), dev(beside, z, x))[hop]
        return remote(
            mix_of(ff, xx), mix_of(ff, xx), s_mix.at[hop, xx, ff], r_mix.at[xx, ff], target
        )

    def mix_wait(ff, xx):
        remote(
            mix_of(ff, xx), mix_of(ff, xx), s_mix.at[0, xx, ff], r_mix.at[xx, ff], here
        ).wait_recv()

    mix_buf[:, tile(head, HD)] = mix_own[...]
    for hop in range(3):
        go("all", lambda hop=hop: mix_send(f, x, hop))

    @pl.when(is_inner)
    def _():
        for c in range(WO_CHUNKS):
            wo_wait(e2, x, c)
            go("inner", lambda c=c: wo_z(e2, x, c, 0, e))
        for c in range(WO_CHUNKS):
            wo_wait(z, other, c)
            go("inner", lambda c=c: wo_z(z, other, c, 0, e))
            go("inner", lambda c=c: wo_z(z, other, c, 1, m))

    @pl.when(is_end)
    def _():
        cross(e2, x)

    mix_wait(f, other)
    for hop in (1, 2):
        go("all", lambda hop=hop: mix_send(f, other, hop))
    mix_wait(ahead, x)
    go("all", lambda: mix_send(ahead, x, 2))

    @pl.when(is_inner)
    def _():
        for c in range(WO_CHUNKS):
            wo_wait(e2, other, c)
            go("inner", lambda c=c: wo_z(e2, other, c, 0, e))

    mix_wait(ahead, other)
    go("all", lambda: mix_send(ahead, other, 2))

    def result(h, c):
        where = pl.ds(pl.multiple_of(h * half_cols + c * chunk, chunk), chunk)
        return pltpu.make_async_copy(out_buf.at[h, :, cols(c)], out.at[:, where], s_res.at[h, c])

    @pl.when(is_end)
    def _():
        cross(n, other)

    for ff in (beside, across):
        for xx in (x, other):
            mix_wait(ff, xx)

    @pl.when(is_end)
    def _():
        cross(e2, other)

    def product(h, c, row_tile):
        return jnp.dot(
            mix_buf[tile(row_tile, tok), :], wo_buf[h, :, cols(c)], preferred_element_type=f32
        ).astype(bf16)

    def away(c):
        return remote(
            out_away.at[c], out_buf.at[x, :, cols(c)], s_out.at[c], r_out.at[c], dev(f, z, other)
        )

    def away_stage(c):
        out_away[c] = product(x, c, other)
        away(c).start()

    def own_stage(h, c):
        out_buf[h, :, cols(c)] = product(h, c, x)
        result(h, c).start()

    def away_wait(c):
        ref = out_buf.at[other, :, cols(c)]
        remote(ref, ref, s_out.at[c], r_out.at[c], here).wait_recv()
        result(other, c).start()

    def settle(kind):
        for make in pending["all"] + pending[kind]:
            make().wait_send()
        q_far_copy().wait_send()
        for b in range(2):
            q_send(b).wait_send()
        if kind == "inner":
            for xx in range(nx):
                for hf in range(2):
                    e_far_copy(xx, hf).wait_send()
                    for b in range(2):
                        e_send(b, xx, hf).wait_send()

        @pl.when(z < nz - 1)
        def _():
            for xx in range(nx):
                seg_next(xx).wait_send()
            kv_next().wait_send()

        @pl.when(z > 0)
        def _():
            for pair in pairs[1:]:
                kv_send(0, *pair).wait_send()

    order = [*range(END_CHUNKS, WO_CHUNKS), *range(END_CHUNKS)]

    @pl.when(is_inner)
    def _():
        for c in order:
            wo_wait(m, other, c)
            go("inner", lambda c=c: wo_z(m, other, c, 0, e))
            away_stage(c)
        for c in order:
            own_stage(x, c)
        for c in order:
            away_wait(c)
        settle("inner")
        for c in order:
            away(c).wait_send()

    @pl.when(is_end)
    def _():
        for c in order:
            wo_wait(m, other, c)
            if c < END_CHUNKS:
                go("end", lambda c=c: wo_cross(m, other, c))
            if c >= END_CHUNKS:
                away_stage(c)
        for c in order:
            own_stage(x, c)
        for c in range(END_CHUNKS):
            wox_wait(z, other, c)
            for j in (n, m, e2):
                for xx in range(nx):
                    wox_wait(j, xx, c)
            own_stage(other, c)
        for c in range(END_CHUNKS, WO_CHUNKS):
            away_wait(c)
        settle("end")
        for c in range(END_CHUNKS, WO_CHUNKS):
            away(c).wait_send()

    for h in range(nx):
        for c in range(WO_CHUNKS):
            result(h, c).wait()


def fused_on_device(nf, nz, nx, hidden, w_query, w_keyvalue, w_output, segment_ids):
    tok, kdim = hidden.shape
    cols = w_output.shape[1]
    rows = tok * nx
    sub = rows // nf
    kvw = w_keyvalue.shape[1]
    heads = nz * nx
    part = cols // nx
    f32, bf16 = jnp.float32, jnp.bfloat16
    dma = pltpu.SemaphoreType.DMA
    vmem = pl.BlockSpec(memory_space=pltpu.VMEM)
    anywhere = pl.BlockSpec(memory_space=pl.ANY)
    scratch = [
        pltpu.VMEM((rows, kdim), bf16),
        pltpu.VMEM((nz // 2, kdim, 2 * HD), bf16),
        pltpu.VMEM((nz * kvw, kdim), bf16),
        pltpu.VMEM((nx, heads * HD, part), bf16),
        pltpu.VMEM((2, nx, 1, tok), jnp.int32),
        pltpu.VMEM((nz, rows, HD), f32),
        pltpu.VMEM((nf // 2, rows, HD), f32),
        pltpu.VMEM((rows, HD), f32),
        pltpu.VMEM((rows, HD), f32),
        pltpu.VMEM((rows, nz * kvw), f32),
        pltpu.VMEM((nf, sub, nz * kvw), f32),
        pltpu.VMEM((sub, HD), bf16),
        pltpu.VMEM((2, nx, rows, HD), bf16),
        pltpu.VMEM((rows, HD), bf16),
        pltpu.VMEM((rows, heads * HD), bf16),
        pltpu.VMEM((rows, HD), f32),
        pltpu.VMEM((rows, HD), f32),
        pltpu.VMEM((nx, tok, part), bf16),
        pltpu.VMEM((WO_CHUNKS, tok, part // WO_CHUNKS), bf16),
        pltpu.VMEM((nx, 2, tok // 2, kdim * MOVED // 8), bf16),
        pltpu.VMEM((nz, nx, 2, tok // 2, HD), f32),
        pltpu.VMEM((nf // 2, nx, 2, tok // 2, HD), f32),
        pltpu.VMEM((nx, 2, tok // 2, HD), f32),
        pltpu.VMEM((nx, 2, tok // 2, HD), f32),
        pltpu.VMEM((nx, 2, tok // 2, HD), f32),
        pltpu.VMEM((nx, 2, tok // 2, HD), f32),
        dma((7,)), dma, dma, dma((1 + nx,)), dma((2, nx)),
        dma((2, nz)), dma((nz,)), dma((2, nz)), dma((nz,)),
        dma((nf // 2,)), dma((nf // 2,)), dma, dma, dma((nf,)), dma((nf,)),
        dma((2, nx, nf)), dma((2, nx, nf)),
        dma((2, nz, nx, WO_CHUNKS)), dma((nz, nx, WO_CHUNKS)),
        dma((nz + 1, nx, WO_CHUNKS)), dma((nz, nx, WO_CHUNKS)),
        dma((3, nx, nf)), dma((nx, nf)),
        dma((WO_CHUNKS,)), dma((WO_CHUNKS,)), dma((nx, WO_CHUNKS)),
        dma((2,)), dma((nx, 2)), dma((2,)), dma((nf // 2, nx, 2)), dma((nf // 2, nx, 2)),
        dma((nx, 2)), dma((nx, 2)),
        dma((nx, 2)), dma((nx, 2)),
    ]
    return pl.pallas_call(
        functools.partial(fused_kernel, nf, nz, nx),
        out_shape=jax.ShapeDtypeStruct((tok, cols), bf16),
        in_specs=[anywhere] * 4 + [vmem],
        out_specs=anywhere,
        scratch_shapes=scratch,
        name="fused_sublayer",
        compiler_params=pltpu.CompilerParams(
            collective_id=0, has_side_effects=True, vmem_limit_bytes=60 * 1024 * 1024
        ),
    )(hidden, w_query, w_keyvalue.T, w_output, segment_ids.reshape(1, tok))


def solution(mesh):
    in_specs = (P("sp", "fsdp"), P("fsdp", "sp"), P("fsdp", "sp"), P("sp", "fsdp"), P("sp"))
    out_specs = P("sp", "fsdp")
    nf, sp = mesh.shape["fsdp"], mesh.shape["sp"]
    if sp == GROUP and sp == 2 * nf:
        body = functools.partial(fused_on_device, nf, nf, sp // nf)
    else:
        body = on_device
    return jax.shard_map(
        body, mesh=mesh, in_specs=in_specs, out_specs=out_specs, check_vma=False
    )
```

```python
import functools
import math

import jax
import jax.numpy as jnp
from jax import lax
from jax.experimental import pallas as pl
from jax.experimental.pallas import tpu as pltpu
from jax.sharding import PartitionSpec as P

HD = 128
GROUP = 8


ROPE_BASE = 500000.0
NEG_FILL = -1e30


def rotate(values, positions, head_count, width):
    row_count = values.shape[0]
    shaped = values.reshape(row_count, head_count, width)
    half_width = width // 2
    frequency = jnp.exp(
        jnp.arange(half_width, dtype=jnp.float32) * (-2.0 * math.log(ROPE_BASE) / width)
    )
    angles = positions.astype(jnp.float32)[:, None] * frequency[None, :]
    cosine = jnp.cos(angles)[:, None, :]
    sine_part = jnp.sin(angles)[:, None, :]
    lower_half = shaped[:, :, :half_width]
    upper_half = shaped[:, :, half_width:]
    turned = jnp.concatenate(
        [
            lower_half * cosine - upper_half * sine_part,
            upper_half * cosine + lower_half * sine_part,
        ],
        axis=2,
    )
    return turned.reshape(row_count, head_count * width)


def split_keys(kv_sum, positions, kv_count, width):
    row_count = kv_sum.shape[0]
    shaped = kv_sum.reshape(row_count, kv_count, 2, width)
    key_part = rotate(
        shaped[:, :, 0, :].reshape(row_count, kv_count * width), positions, kv_count, width
    )
    key_part = key_part.reshape(row_count, kv_count, 1, width)
    return jnp.concatenate([key_part, shaped[:, :, 1:2, :]], axis=2).astype(jnp.bfloat16)


def merge_keys(
    state_in, query_tile, query_pos_tile, query_seg_tile, key_tile, key_pos_tile, key_seg_tile
):
    running_max, running_sum, weighted = state_in
    allowed = (key_pos_tile[None, :] <= query_pos_tile[:, None]) & (
        key_seg_tile[None, :] == query_seg_tile[:, None]
    )
    key_part = key_tile[:, :HD]
    value_part = key_tile[:, HD:]
    scores = lax.dot_general(
        query_tile, key_part, (((1,), (1,)), ((), ())), preferred_element_type=jnp.float32
    ) * HD ** (-0.5)
    masked = jnp.where(allowed, scores, NEG_FILL)
    new_max = jnp.maximum(running_max, jnp.max(masked, axis=1))
    weights = jnp.where(allowed, jnp.exp(masked - new_max[:, None]), 0.0)
    new_sum = jnp.sum(weights, axis=1)
    new_weighted = jnp.dot(
        weights.astype(jnp.bfloat16), value_part, preferred_element_type=jnp.float32
    )
    return (new_max, new_sum, new_weighted)


def on_device(hidden, w_query, w_keyvalue, w_output, segment_ids):
    fsdp_count = lax.axis_size("fsdp")
    seq_count = lax.axis_size("sp")
    fsdp_index = lax.axis_index("fsdp")
    seq_index = lax.axis_index("sp")
    tok_rows = hidden.shape[0]
    sub_rows = tok_rows // fsdp_count
    kv_count = seq_count // GROUP
    query_rows = seq_count * sub_rows
    offsets = jnp.arange(query_rows, dtype=jnp.int32)
    query_pos = offsets // sub_rows * tok_rows + fsdp_index * sub_rows + offsets % sub_rows
    own_positions = (
        seq_index * tok_rows + fsdp_index * sub_rows + jnp.arange(sub_rows, dtype=jnp.int32)
    )

    def project(weight_block):
        return jnp.dot(hidden, weight_block, preferred_element_type=jnp.float32)

    query_part = project(lax.all_gather(w_query, "sp", axis=1, tiled=True))
    kv_part = project(lax.all_gather(w_keyvalue, "sp", axis=1, tiled=True))
    query_sum, kv_sum = (
        lax.psum_scatter(query_part, "fsdp", scatter_dimension=0, tiled=True),
        lax.psum_scatter(kv_part, "fsdp", scatter_dimension=0, tiled=True),
    )
    query_local = rotate(query_sum, own_positions, seq_count, HD).astype(jnp.bfloat16)
    pairs = split_keys(kv_sum, own_positions, kv_count, HD)
    expanded = jnp.repeat(pairs, GROUP, axis=1).reshape(sub_rows, seq_count * 2 * HD)
    query_head, kv_head = (
        lax.all_to_all(query_local, "sp", split_axis=1, concat_axis=0, tiled=True),
        lax.all_to_all(expanded, "sp", split_axis=1, concat_axis=0, tiled=True),
    )
    segment_all = lax.all_gather(segment_ids, "sp", axis=0, tiled=True)
    query_seg = segment_all[query_pos]
    initial = (
        jnp.full((query_rows,), NEG_FILL, jnp.float32),
        jnp.zeros((query_rows,), jnp.float32),
        jnp.zeros((query_rows, HD), jnp.float32),
    )
    block_keys = lax.all_gather(kv_head, "fsdp", axis=0, tiled=True)
    piece_rows = block_keys.shape[0]
    row_ids = jnp.arange(piece_rows, dtype=jnp.int32)
    source_id = row_ids // query_rows
    within = row_ids % query_rows
    key_pos = within // sub_rows * tok_rows + source_id * sub_rows + within % sub_rows
    key_seg = segment_all[key_pos]
    final_max, final_sum, final_weighted = merge_keys(
        initial, query_head, query_pos, query_seg, block_keys, key_pos, key_seg
    )
    attention = (final_weighted / final_sum[:, None]).astype(jnp.bfloat16)
    back_rows = lax.all_to_all(attention, "sp", split_axis=0, concat_axis=1, tiled=True)
    mixed_rows = lax.all_gather(back_rows, "fsdp", axis=0, tiled=True)
    result = jnp.dot(
        mixed_rows,
        lax.all_gather(w_output, "sp", axis=0, tiled=True),
        preferred_element_type=jnp.float32,
    )
    return result.astype(jnp.bfloat16)


NEG_POS = -1
WO_CHUNKS = 4
MOVED = 4
END_CHUNKS = 3


def fused_kernel(
    nf, nz, nx, hid, wq, wkv, wo, seg, out,
    h_buf, wq_buf, wkv_buf, wo_buf, seg_buf,
    q_part, q_mate, q_sum, q_far, kv_part, kv_recv, kv_piece, kv_all, mix_own, mix_buf, q_cos, q_sin,
    out_buf, out_away, h_end, e_part, e_mate, e_sum, e_far, e_back, q_in,
    s_loc, s_hid, r_hid, s_seg, r_seg, s_wkv, r_wkv, s_wq, r_wq,
    s_q, r_q, s_qf, r_qf, s_kvp, r_kvp, s_kv, r_kv, s_kn, s_wo, r_wo, s_wox, r_wox, s_mix, r_mix,
    s_out, r_out, s_res, s_he, r_he, s_hx, s_ep, r_ep, s_ef, r_ef, s_eb, r_eb,
):
    f = lax.axis_index("fsdp")
    s = lax.axis_index("sp")
    z, x = s // nx, s % nx
    tok, kdim = hid.shape
    rows = tok * nx
    sub = rows // nf
    kvw = wkv.shape[0]
    other = 1 - x
    moved = kdim * MOVED // 8
    block = tok // 2
    half_cols = wo.shape[1] // nx
    chunk = half_cols // WO_CHUNKS
    f32, bf16 = jnp.float32, jnp.bfloat16
    is_end = (z == 0) | (z == nz - 1)
    is_inner = jnp.logical_not(is_end)
    low = z < nz // 2
    e = jnp.where(low, 0, nz - 1)
    n = jnp.where(low, 1, nz - 2)
    m = nz - 1 - n
    e2 = nz - 1 - e
    beside = f + 1 - 2 * lax.rem(f, 2)
    ahead = lax.rem(f + 2, nf)
    across = lax.rem(beside + 2, nf)

    def block_of(ff):
        return lax.rem(ff, 2) * 2 + ff // 2

    core = lax.rem(f, 2)
    mine, theirs = block_of(f), block_of(ahead)
    near = core == z // 2

    def dev(ff, zz, xx):
        return (ff, zz * nx + xx)

    def remote(src, dst, ss, rs, target):
        return pltpu.make_async_remote_copy(
            src_ref=src, dst_ref=dst, send_sem=ss, recv_sem=rs,
            device_id=target, device_id_type=pl.DeviceIdType.MESH,
        )

    def tile(ref, count):
        return pl.ds(pl.multiple_of(ref * count, count), count)

    here = (f, s)
    def cols(c):
        return slice(c * chunk, (c + 1) * chunk)

    own_h = pltpu.make_async_copy(hid, h_buf.at[tile(x, tok)], s_loc.at[0])
    own_wq = pltpu.make_async_copy(
        wq, wq_buf.at[z // 2, :, tile(lax.rem(z, 2), HD)], s_loc.at[1]
    )
    own_wkv = pltpu.make_async_copy(wkv, wkv_buf.at[tile(z, kvw)], s_loc.at[2])
    own_wo = [
        pltpu.make_async_copy(
            wo.at[:, h * half_cols : (h + 1) * half_cols],
            wo_buf.at[h, tile(s, HD)], s_loc.at[3 + h],
        )
        for h in range(nx)
    ]
    own_seg = pltpu.make_async_copy(seg, seg_buf.at[1, x], s_loc.at[5])
    for copy in (own_wkv, own_wq, own_h, *own_wo, own_seg):
        copy.start()

    def hid_send():
        return remote(
            h_buf.at[tile(x, tok)], h_buf.at[tile(x, tok)], s_hid, r_hid, dev(f, z, other)
        )

    def hid_wait():
        remote(
            h_buf.at[tile(other, tok)], h_buf.at[tile(other, tok)], s_hid, r_hid, here
        ).wait_recv()

    def wkv_z(j, d, target):
        ref = wkv_buf.at[tile(j, kvw)]
        return remote(ref, ref, s_wkv.at[d], r_wkv.at[j], dev(f, target, x))

    def wkv_wait(j):
        wkv_z(j, 0, z).wait_recv()

    def wq_of(j, first):
        return wq_buf.at[j // 2, first:, tile(lax.rem(j, 2), HD)]

    def wq_z(j, d, target):
        ref = wq_of(j, 0) if d else wq_of(j, moved)
        return remote(ref, ref, s_wq.at[d], r_wq.at[j], dev(f, target, x))

    def wq_wait(j, d=1):
        wq_z(j, d, z).wait_recv()

    def he_z(hf):
        rows_of = pl.ds(pl.multiple_of(x * tok + hf * block, block), block)
        return remote(
            h_buf.at[rows_of, 0:moved], h_end.at[x, hf], s_he, r_he.at[x, hf], dev(f, n, x)
        )

    def he_x(hf):
        ref = h_end.at[x, hf]
        return remote(ref, ref, s_hx, r_he.at[x, hf], dev(f, z, other))

    def he_wait(xx, hf):
        ref = h_end.at[xx, hf]
        remote(ref, ref, s_hx, r_he.at[xx, hf], here).wait_recv()

    def wo_unit(h, j, xx, c):
        return wo_buf.at[h, tile(j * nx + xx, HD), cols(c)]

    def wo_z(j, xx, c, d, target):
        ref = wo_unit(x, j, xx, c)
        return remote(ref, ref, s_wo.at[d], r_wo.at[j, xx, c], dev(f, target, x))

    def wo_pair(c):
        ref = wo_unit(other, z, x, c)
        return remote(ref, ref, s_wox, r_wo.at[z, x, c], dev(f, z, other))

    def wo_wait(j, xx, c):
        ref = wo_unit(x, j, xx, c)
        remote(ref, ref, s_wox, r_wo.at[j, xx, c], here).wait_recv()

    def wo_cross(j, xx, c):
        ref = wo_unit(x, j, xx, c)
        return remote(ref, ref, s_wox, r_wox.at[c], dev(f, z, other))

    def wox_wait(c):
        ref = wo_buf.at[other, HD:, cols(c)]
        remote(ref, ref, s_wox, r_wox.at[c], here).wait_recv()

    def seg_same():
        return remote(seg_buf.at[1, x], seg_buf.at[1, x], s_seg.at[0], r_seg.at[1], dev(f, z, other))

    def seg_next(xx):
        return remote(
            seg_buf.at[1, x], seg_buf.at[0, x], s_seg.at[1], r_seg.at[0], dev(f, z + 1, xx)
        )

    barrier = pltpu.get_barrier_semaphore()

    def greet(ff, zz, xx):
        pl.semaphore_signal(
            barrier, inc=1, device_id=dev(ff, zz, xx), device_id_type=pl.DeviceIdType.MESH
        )

    plane = nf * nx
    for step in (1, -1):
        @pl.when((z + step >= 0) & (z + step < nz))
        def _():
            for xx in range(nx):
                greet(f, z + step, xx)

    for d in range(1, plane):
        greet(lax.rem(f + d, nf), z, lax.rem(x + d // nf, nx))
    pl.semaphore_wait(barrier, plane - 1 + jnp.where(is_end, nx, 2 * nx))

    own_wkv.wait()
    own_wq.wait()

    @pl.when(is_end)
    def _():
        wkv_z(z, 1, n).start()
        wq_z(z, 1, n).start()

    @pl.when(is_inner)
    def _():
        for d, target in ((0, e), (1, m)):
            wkv_z(z, d, target).start()
            wq_z(z, d, target).start()

    own_h.wait()
    hid_send().start()
    own_seg.wait()
    seg_same().start()

    @pl.when(z < nz - 1)
    def _():
        for xx in range(nx):
            seg_next(xx).start()

    for copy in own_wo:
        copy.wait()

    @pl.when(is_end)
    def _():
        for hf in range(2):
            he_z(hf).start()
        for c in range(WO_CHUNKS):
            wo_z(z, x, c, 1, n).start()
        for c in range(WO_CHUNKS):
            wo_pair(c).start()
        for c in range(END_CHUNKS):
            wo_cross(z, x, c).start()

    @pl.when(is_inner)
    def _():
        for c in range(WO_CHUNKS):
            wo_z(z, x, c, 0, e).start()

    @pl.when(z == 0)
    def _():
        kv_all[0] = jnp.zeros(kv_all.shape[1:], bf16)
        seg_buf[0] = jnp.full(seg_buf.shape[1:], NEG_POS, jnp.int32)

    @pl.when(is_inner)
    def _():
        q_in[...] = jnp.zeros(q_in.shape, f32)

    def table(row_count, first, lane_index):
        position = (first + lax.broadcasted_iota(jnp.int32, (row_count, HD), 0)).astype(f32)
        frequency = jnp.exp(lane_index.astype(f32) * (-2.0 * math.log(ROPE_BASE) / HD))
        return position * frequency

    lane = lax.broadcasted_iota(jnp.int32, (1, HD), 1)
    half = HD // 2
    quarter = half // nx
    kv_angle = table(sub, z * rows + f * sub, x * quarter + lane % quarter)
    is_key = lane < half
    kv_cos = jnp.where(is_key, jnp.cos(kv_angle), 1.0)
    kv_sin = jnp.where(is_key, jnp.sin(kv_angle), 0.0)
    kv_sin = jnp.where(lane < quarter, -kv_sin, kv_sin)
    q_angle = table(rows, z * rows, lane % half)
    q_sine = jnp.sin(q_angle)
    q_cos[...] = jnp.cos(q_angle)
    q_sin[...] = jnp.where(lane < half, -q_sine, q_sine)

    same_core = lambda j: j // 2 == core

    def q_send(j):
        return remote(
            q_part.at[j], q_mate.at[lax.rem(j, 2)], s_q, r_q, dev(beside, z, x)
        )

    def q_far_copy():
        return remote(q_sum, q_far, s_qf, r_qf, dev(ahead, z, x))

    def q_project(j, first):
        both = jnp.dot(
            h_buf[:, first:], wq_buf[j // 2, first:, :], preferred_element_type=f32
        )
        for b in range(2):
            q_part[j // 2 * 2 + b] = both[:, b * HD : (b + 1) * HD]

        @pl.when(jnp.logical_not(same_core(j)))
        def _():
            for b in range(2):
                q_send(j // 2 * 2 + b).start()

    def q_relay(far):
        @pl.when(jnp.logical_not(near) if far else near)
        def _():
            remote(q_mate, q_mate, s_q, r_q, here).wait_recv()
            q_sum[...] = q_part[theirs] + q_mate[lax.rem(theirs, 2)]
            q_far_copy().start()

    def e_send(j, xx, hf):
        return remote(
            e_part.at[j, xx, hf], e_mate.at[lax.rem(j, 2), xx, hf],
            s_ep, r_ep.at[xx, hf], dev(beside, z, x)
        )

    def e_far_copy(xx, hf):
        return remote(
            e_sum.at[xx, hf], e_far.at[xx, hf], s_ef, r_ef.at[xx, hf], dev(ahead, z, x)
        )

    def e_project(xx, hf, j):
        both = jnp.dot(
            h_end[xx, hf], wq_buf[j // 2, 0:moved, :], preferred_element_type=f32
        )
        for b in range(2):
            e_part[j // 2 * 2 + b, xx, hf] = both[:, b * HD : (b + 1) * HD]

        @pl.when(jnp.logical_not(same_core(j)))
        def _():
            for b in range(2):
                e_send(j // 2 * 2 + b, xx, hf).start()

    def e_relay(xx, hf):
        ref = e_mate.at[:, xx, hf]
        remote(ref, ref, s_ep, r_ep.at[xx, hf], here).wait_recv()
        e_sum[xx, hf] = e_part[theirs, xx, hf] + e_mate[lax.rem(theirs, 2), xx, hf]
        e_far_copy(xx, hf).start()

    def e_return(xx, hf):
        return remote(
            e_back.at[xx, hf], q_in.at[xx, hf], s_eb, r_eb, dev(f, e, x)
        )

    def e_collect(xx, hf):
        ref = e_far.at[xx, hf]
        remote(ref, ref, s_ef, r_ef.at[xx, hf], here).wait_recv()
        e_back[xx, hf] = (
            e_part[mine, xx, hf] + e_mate[lax.rem(mine, 2), xx, hf] + e_far[xx, hf]
        )
        e_return(xx, hf).start()

    @pl.when(is_inner)
    def _():
        wkv_wait(e)
        wkv_z(e, 1, m).start()
        wkv_wait(m)
        wkv_z(m, 0, e).start()
        wq_wait(e)
        wq_z(e, 1, m).start()
        for c in range(WO_CHUNKS):
            wo_z(z, x, c, 1, m).start()
        wq_wait(m)
        wq_z(m, 0, e).start()
        wkv_wait(e2)
        wkv_z(e2, 0, e).start()
        he_wait(x, 0)
        he_x(0).start()

    hid_wait()

    @pl.when(is_end)
    def _():
        for j in (n, m, e2):
            wkv_wait(j)

    kv_part[...] = lax.dot_general(
        h_buf[...], wkv_buf[...], (((1,), (1,)), ((), ())), preferred_element_type=f32
    )

    def kvp_send(d):
        ff = lax.rem(f + d, nf)
        return remote(
            kv_part.at[tile(ff, sub)], kv_recv.at[f], s_kvp, r_kvp, (ff, s)
        )

    for d in range(1, nf):
        kvp_send(d).start()

    @pl.when(is_inner)
    def _():
        q_project(z, 0)
        he_wait(x, 1)
        he_x(1).start()
        q_relay(False)
        e_project(x, 0, z)

        @pl.when(near)
        def _():
            e_relay(x, 0)


    @pl.when(is_end)
    def _():
        wq_wait(n, 0)
        q_project(z, moved)
        q_relay(False)

    total = kv_part[tile(f, sub), :]
    arrived = kv_recv.at[1:nf]
    remote(arrived, arrived, s_kvp, r_kvp, here).wait_recv()
    for d in range(1, nf):
        total = total + kv_recv[lax.rem(f + d, nf)]
    partner = jnp.where(
        lane < quarter, pltpu.roll(total, HD - quarter, 1), pltpu.roll(total, quarter, 1)
    )
    kv_piece[...] = (total * kv_cos + partner * kv_sin).astype(bf16)
    piece_rows = tile(f, sub)
    kv_all[1, x, piece_rows] = kv_piece[...]

    def kv_of(plane, ff, xx):
        return kv_all.at[plane, xx, tile(ff, sub)]

    def kv_hop(plane, ff, xx, hop):
        target = (dev(f, z, other), dev(ahead, z, x), dev(beside, z, x))[hop]
        ref = kv_of(plane, ff, xx)
        slot = hop + (hop == 2 or xx is other)
        return remote(ref, ref, s_kv.at[plane], r_kv.at[plane, slot], target)

    def kv_first(plane):
        for hop in range(3):
            kv_hop(plane, f, x, hop).start()

    def kv_second(plane):
        kv_wait(plane, f, other, 0)
        for hop in (1, 2):
            kv_hop(plane, f, other, hop).start()
        kv_wait(plane, ahead, x, 1)
        kv_hop(plane, ahead, x, 2).start()

    def kv_third(plane):
        kv_wait(plane, ahead, other, 2)
        kv_hop(plane, ahead, other, 2).start()

    def kv_last(plane):
        ref = kv_all.at[plane, x]
        remote(ref, ref, s_kn, r_kv.at[plane, 3], here).wait_recv()

    def kv_next():
        return remote(
            kv_piece, kv_all.at[0, x, piece_rows],
            s_kn, r_kv.at[0, 4], dev(f, z + 1, x),
        )

    def kv_wait(plane, ff, xx, slot):
        ref = kv_of(plane, ff, xx)
        remote(ref, ref, s_kn, r_kv.at[plane, slot], here).wait_recv()

    kv_first(1)

    @pl.when(z < nz - 1)
    def _():
        kv_next().start()

    @pl.when(is_end)
    def _():
        for c in range(WO_CHUNKS):
            wo_wait(z, other, c)
            wo_z(z, other, c, 1, n).start()

    @pl.when(is_inner)
    def _():
        wq_wait(e2)
        wq_z(e2, 0, e).start()
        q_project(e2, 0)
        e_project(x, 0, e2)
        e_project(x, 1, z)
        e_project(x, 1, e2)

        @pl.when(jnp.logical_not(near))
        def _():
            e_relay(x, 0)

        e_relay(x, 1)
        he_wait(other, 0)
        e_project(other, 0, z)
        e_project(other, 0, e2)
        e_relay(other, 0)

    @pl.when(z > 0)
    def _():
        kv_wait(0, f, x, 4)
        kv_first(0)

    kv_second(1)

    @pl.when(is_inner)
    def _():
        for c in range(WO_CHUNKS):
            wo_pair(c).start()
        for c in range(WO_CHUNKS):
            wo_wait(e, x, c)
            wo_z(e, x, c, 1, m).start()
        e_collect(x, 0)
        he_wait(other, 1)
        e_project(other, 1, z)
        e_project(other, 1, e2)
        e_relay(other, 1)
        q_relay(True)
        for c in range(WO_CHUNKS):
            wo_wait(m, x, c)
            wo_z(m, x, c, 0, e).start()
        kv_third(1)

        @pl.when(z > 0)
        def _():
            kv_second(0)

        e_collect(other, 0)
        e_collect(x, 1)
        for c in range(WO_CHUNKS):
            wo_wait(e, other, c)
            wo_z(e, other, c, 1, m).start()

        @pl.when(z > 0)
        def _():
            kv_third(0)

        e_collect(other, 1)

    def cross(j, xx):
        for c in range(WO_CHUNKS):
            wo_wait(j, xx, c)
            if c < END_CHUNKS:
                wo_cross(j, xx, c).start()

    @pl.when(is_end)
    def _():
        cross(n, x)
        kv_third(1)

        @pl.when(z > 0)
        def _():
            kv_second(0)

        wq_wait(m, 0)
        wq_wait(e2, 0)
        q_project(e2, moved)
        q_relay(True)

        @pl.when(z > 0)
        def _():
            kv_third(0)

        cross(m, x)
        remote(q_in, q_in, s_eb, r_eb, here).wait_recv()

    remote(q_far, q_far, s_qf, r_qf, here).wait_recv()
    q_total = q_part[mine] + q_mate[lax.rem(mine, 2)] + q_far[...]
    returned = q_in[...].reshape(rows, HD)
    q_total = q_total + jnp.where(is_end, returned, 0.0)
    q_turned = q_total * q_cos[...] + pltpu.roll(q_total, half, 1) * q_sin[...]
    q_head = q_turned.astype(bf16).astype(f32)
    quarters = []
    for xx in range(nx):
        first = q_head if xx == 0 else pltpu.roll(q_head, HD - xx * quarter, 1)
        second = pltpu.roll(q_head, (HD - half - xx * quarter + quarter) % HD, 1)
        picked = jnp.where(lane < quarter, first, jnp.where(lane < half, second, 0.0))
        quarters.append(picked.astype(bf16))

    seg_ref = seg_buf.at[1, other]
    remote(seg_ref, seg_ref, s_seg.at[0], r_seg.at[1], here).wait_recv()
    kv_last(1)

    @pl.when(z > 0)
    def _():
        before = seg_buf.at[0]
        remote(before, before, s_seg.at[1], r_seg.at[0], here).wait_recv()
        kv_last(0)

    key_seg = jnp.concatenate(
        [seg_buf[plane, xx] for plane in range(2) for xx in range(nx)], axis=1
    )
    own_seg_row = key_seg[:, rows:]
    seg_column = jnp.transpose(jnp.broadcast_to(own_seg_row, (HD, rows)))[:, :1]
    key_pos = lax.broadcasted_iota(jnp.int32, (1, 2 * rows), 1) - rows
    keys = [
        jnp.concatenate([kv_all[0, xx], kv_all[1, xx]], axis=0) for xx in range(nx)
    ]
    step_rows = rows // nf
    for b in range(nf):
        span = slice(b * step_rows, (b + 1) * step_rows)
        query_pos = b * step_rows + lax.broadcasted_iota(jnp.int32, (step_rows, 1), 0)
        score = None
        for xx in range(nx):
            term = lax.dot_general(
                quarters[xx][span], keys[xx], (((1,), (1,)), ((), ())),
                preferred_element_type=f32,
            )
            score = term if score is None else score + term
        allowed = (key_pos <= query_pos) & (key_seg == seg_column[span])
        masked = jnp.where(allowed, score * HD ** (-0.5), NEG_FILL)
        row_max = jnp.max(masked, axis=1, keepdims=True)
        weight = jnp.where(allowed, jnp.exp(masked - row_max), 0.0)
        row_total = jnp.sum(weight, axis=1, keepdims=True)
        rounded = weight.astype(bf16)
        product = [
            jnp.dot(rounded, keys[xx], preferred_element_type=f32) for xx in range(nx)
        ]
        mixed = None
        for xx in reversed(range(nx)):
            first = pltpu.roll(product[xx], (half + xx * quarter) % HD, 1)
            second = pltpu.roll(product[xx], (HD - (nx - 1 - xx) * quarter) % HD, 1)
            lane_block = lane // quarter
            value = jnp.where(lane_block < nx, first, second)
            mixed = value if mixed is None else jnp.where(lane_block % nx == xx, value, mixed)
        mix_own[span, :] = (mixed / row_total).astype(bf16)

    head = mine * nx + x

    def mix_of(ff, xx):
        return mix_buf.at[:, tile(block_of(ff) * nx + xx, HD)]

    def mix_send(ff, xx, hop):
        target = (dev(f, z, other), dev(ahead, z, x), dev(beside, z, x))[hop]
        return remote(
            mix_of(ff, xx), mix_of(ff, xx), s_mix,
            r_mix.at[hop + (hop == 2 or xx is other)], target,
        )

    def mix_wait(ref, slot):
        remote(ref, ref, s_mix, r_mix.at[slot], here).wait_recv()

    mix_buf[:, tile(head, HD)] = mix_own[...]
    for hop in range(3):
        mix_send(f, x, hop).start()

    @pl.when(is_inner)
    def _():
        for c in range(WO_CHUNKS):
            wo_wait(e2, x, c)
            wo_z(e2, x, c, 0, e).start()
        for c in range(WO_CHUNKS):
            wo_wait(z, other, c)
            wo_z(z, other, c, 0, e).start()
            wo_z(z, other, c, 1, m).start()

    @pl.when(is_end)
    def _():
        cross(e2, x)

    mix_wait(mix_of(f, other), 0)
    for hop in (1, 2):
        mix_send(f, other, hop).start()
    mix_wait(mix_of(ahead, x), 1)
    mix_send(ahead, x, 2).start()

    @pl.when(is_inner)
    def _():
        for c in range(WO_CHUNKS):
            wo_wait(e2, other, c)
            wo_z(e2, other, c, 0, e).start()

    mix_wait(mix_of(ahead, other), 2)
    mix_send(ahead, other, 2).start()

    def result(h, c):
        where = pl.ds(pl.multiple_of(h * half_cols + c * chunk, chunk), chunk)
        return pltpu.make_async_copy(out_buf.at[h, :, cols(c)], out.at[:, where], s_res)

    @pl.when(is_end)
    def _():
        cross(n, other)

    mix_wait(mix_buf.at[:, 0 : 4 * HD], 3)

    @pl.when(is_end)
    def _():
        cross(e2, other)

    def product(h, c, row_tile):
        return jnp.dot(
            mix_buf[tile(row_tile, tok), :], wo_buf[h, :, cols(c)], preferred_element_type=f32
        ).astype(bf16)

    def away(c):
        return remote(
            out_away.at[c], out_buf.at[x, :, cols(c)], s_out, r_out.at[c], dev(f, z, other)
        )

    def away_stage(c):
        out_away[c] = product(x, c, other)
        away(c).start()

    def own_stage(h, c):
        out_buf[h, :, cols(c)] = product(h, c, x)
        result(h, c).start()

    def away_wait(c):
        ref = out_buf.at[other, :, cols(c)]
        remote(ref, ref, s_out, r_out.at[c], here).wait_recv()
        result(other, c).start()

    def drained(sem, size):
        ruler = wo_buf.at[0, 0 : size // (half_cols * 2), :]
        remote(ruler, ruler, sem, r_hid, here).wait_send()

    def settle(kind):
        inner = kind == "inner"
        unit = HD * chunk * 2
        drained(s_hid, tok * kdim * 2)
        drained(s_wkv.at[1], (2 if inner else 1) * kvw * kdim * 2)
        drained(s_wq.at[1], (2 if inner else 1) * kdim * HD * 2)
        drained(s_wo.at[1], (2 if inner else 1) * nx * WO_CHUNKS * unit)
        crossed = 0 if inner else (nz * nx - 1) * END_CHUNKS
        drained(s_wox, (WO_CHUNKS + crossed) * unit)
        drained(s_hx if inner else s_he, 2 * block * moved * 2)
        drained(s_q, 2 * rows * HD * 4)
        drained(s_qf, rows * HD * 4)
        drained(s_kvp, (nf - 1) * sub * nz * kvw * 4)
        drained(s_kv.at[1], (nf * nx - 1) * sub * HD * 2)
        drained(s_mix, (nf * nx - 1) * rows * HD * 2)
        drained(s_out, (WO_CHUNKS if inner else WO_CHUNKS - END_CHUNKS) * tok * chunk * 2)
        if inner:
            drained(s_wkv.at[0], 3 * kvw * kdim * 2)
            drained(s_wq.at[0], 3 * (kdim - moved) * HD * 2)
            drained(s_wo.at[0], 3 * nx * WO_CHUNKS * unit)
            drained(s_ep, 2 * rows * HD * 4)
            drained(s_ef, rows * HD * 4)
            drained(s_eb, rows * HD * 4)
        seg_same().wait_send()

        @pl.when(z < nz - 1)
        def _():
            before = seg_buf.at[0]
            remote(before, before, s_seg.at[1], r_seg.at[0], here).wait_send()
            kv_next().wait_send()

        @pl.when(z > 0)
        def _():
            drained(s_kv.at[0], (nf * nx - 1) * sub * HD * 2)

    order = [*range(END_CHUNKS, WO_CHUNKS), *range(END_CHUNKS)]

    @pl.when(is_inner)
    def _():
        for c in order:
            wo_wait(m, other, c)
            wo_z(m, other, c, 0, e).start()
            away_stage(c)
        for c in order:
            own_stage(x, c)
        for c in order:
            away_wait(c)
        settle("inner")

    @pl.when(is_end)
    def _():
        for c in order:
            wo_wait(m, other, c)
            if c < END_CHUNKS:
                wo_cross(m, other, c).start()
            if c >= END_CHUNKS:
                away_stage(c)
        for c in order:
            own_stage(x, c)
        for c in range(END_CHUNKS):
            wox_wait(c)
            own_stage(other, c)
        for c in range(END_CHUNKS, WO_CHUNKS):
            away_wait(c)
        settle("end")

    ruler = wo_buf.at[0, 0 : tok * nx, :]
    pltpu.make_async_copy(ruler, ruler, s_res).wait()


def fused_on_device(nf, nz, nx, hidden, w_query, w_keyvalue, w_output, segment_ids):
    tok, kdim = hidden.shape
    cols = w_output.shape[1]
    rows = tok * nx
    sub = rows // nf
    kvw = w_keyvalue.shape[1]
    heads = nz * nx
    part = cols // nx
    f32, bf16 = jnp.float32, jnp.bfloat16
    dma = pltpu.SemaphoreType.DMA
    vmem = pl.BlockSpec(memory_space=pltpu.VMEM)
    anywhere = pl.BlockSpec(memory_space=pl.ANY)
    scratch = [
        pltpu.VMEM((rows, kdim), bf16),
        pltpu.VMEM((nz // 2, kdim, 2 * HD), bf16),
        pltpu.VMEM((nz * kvw, kdim), bf16),
        pltpu.VMEM((nx, heads * HD, part), bf16),
        pltpu.VMEM((2, nx, 1, tok), jnp.int32),
        pltpu.VMEM((nz, rows, HD), f32),
        pltpu.VMEM((nf // 2, rows, HD), f32),
        pltpu.VMEM((rows, HD), f32),
        pltpu.VMEM((rows, HD), f32),
        pltpu.VMEM((rows, nz * kvw), f32),
        pltpu.VMEM((nf, sub, nz * kvw), f32),
        pltpu.VMEM((sub, HD), bf16),
        pltpu.VMEM((2, nx, rows, HD), bf16),
        pltpu.VMEM((rows, HD), bf16),
        pltpu.VMEM((rows, heads * HD), bf16),
        pltpu.VMEM((rows, HD), f32),
        pltpu.VMEM((rows, HD), f32),
        pltpu.VMEM((nx, tok, part), bf16),
        pltpu.VMEM((WO_CHUNKS, tok, part // WO_CHUNKS), bf16),
        pltpu.VMEM((nx, 2, tok // 2, kdim * MOVED // 8), bf16),
        pltpu.VMEM((nz, nx, 2, tok // 2, HD), f32),
        pltpu.VMEM((nf // 2, nx, 2, tok // 2, HD), f32),
        pltpu.VMEM((nx, 2, tok // 2, HD), f32),
        pltpu.VMEM((nx, 2, tok // 2, HD), f32),
        pltpu.VMEM((nx, 2, tok // 2, HD), f32),
        pltpu.VMEM((nx, 2, tok // 2, HD), f32),
        dma((6,)), dma, dma, dma((2,)), dma((2,)), dma((2,)), dma((nz,)), dma((2,)), dma((nz,)),
        dma, dma, dma, dma, dma, dma, dma((2,)), dma((2, 5)), dma,
        dma((2,)), dma((nz, nx, WO_CHUNKS)), dma, dma((WO_CHUNKS,)), dma, dma((4,)),
        dma, dma((WO_CHUNKS,)), dma, dma, dma((nx, 2)), dma,
        dma, dma((nx, 2)), dma, dma((nx, 2)), dma, dma,
    ]
    return pl.pallas_call(
        functools.partial(fused_kernel, nf, nz, nx),
        out_shape=jax.ShapeDtypeStruct((tok, cols), bf16),
        in_specs=[anywhere] * 4 + [vmem],
        out_specs=anywhere,
        scratch_shapes=scratch,
        name="fused_sublayer",
        compiler_params=pltpu.CompilerParams(
            collective_id=0, has_side_effects=True, vmem_limit_bytes=60 * 1024 * 1024
        ),
    )(hidden, w_query, w_keyvalue.T, w_output, segment_ids.reshape(1, tok))


def solution(mesh):
    in_specs = (P("sp", "fsdp"), P("fsdp", "sp"), P("fsdp", "sp"), P("sp", "fsdp"), P("sp"))
    out_specs = P("sp", "fsdp")
    nf, sp = mesh.shape["fsdp"], mesh.shape["sp"]
    if sp == GROUP and sp == 2 * nf:
        body = functools.partial(fused_on_device, nf, nf, sp // nf)
    else:
        body = on_device
    return jax.shard_map(
        body, mesh=mesh, in_specs=in_specs, out_specs=out_specs, check_vma=False
    )
```

```python
import functools
import math

import jax
import jax.numpy as jnp
from jax import lax
from jax.experimental import pallas as pl
from jax.experimental.pallas import tpu as pltpu
from jax.sharding import PartitionSpec as P

HD = 128
GROUP = 8


ROPE_BASE = 500000.0
NEG_FILL = -1e30


def rotate(values, positions, head_count, width):
    row_count = values.shape[0]
    shaped = values.reshape(row_count, head_count, width)
    half_width = width // 2
    frequency = jnp.exp(
        jnp.arange(half_width, dtype=jnp.float32) * (-2.0 * math.log(ROPE_BASE) / width)
    )
    angles = positions.astype(jnp.float32)[:, None] * frequency[None, :]
    cosine = jnp.cos(angles)[:, None, :]
    sine_part = jnp.sin(angles)[:, None, :]
    lower_half = shaped[:, :, :half_width]
    upper_half = shaped[:, :, half_width:]
    turned = jnp.concatenate(
        [
            lower_half * cosine - upper_half * sine_part,
            upper_half * cosine + lower_half * sine_part,
        ],
        axis=2,
    )
    return turned.reshape(row_count, head_count * width)


def split_keys(kv_sum, positions, kv_count, width):
    row_count = kv_sum.shape[0]
    shaped = kv_sum.reshape(row_count, kv_count, 2, width)
    key_part = rotate(
        shaped[:, :, 0, :].reshape(row_count, kv_count * width), positions, kv_count, width
    )
    key_part = key_part.reshape(row_count, kv_count, 1, width)
    return jnp.concatenate([key_part, shaped[:, :, 1:2, :]], axis=2).astype(jnp.bfloat16)


def merge_keys(
    state_in, query_tile, query_pos_tile, query_seg_tile, key_tile, key_pos_tile, key_seg_tile
):
    running_max, running_sum, weighted = state_in
    allowed = (key_pos_tile[None, :] <= query_pos_tile[:, None]) & (
        key_seg_tile[None, :] == query_seg_tile[:, None]
    )
    key_part = key_tile[:, :HD]
    value_part = key_tile[:, HD:]
    scores = lax.dot_general(
        query_tile, key_part, (((1,), (1,)), ((), ())), preferred_element_type=jnp.float32
    ) * HD ** (-0.5)
    masked = jnp.where(allowed, scores, NEG_FILL)
    new_max = jnp.maximum(running_max, jnp.max(masked, axis=1))
    weights = jnp.where(allowed, jnp.exp(masked - new_max[:, None]), 0.0)
    new_sum = jnp.sum(weights, axis=1)
    new_weighted = jnp.dot(
        weights.astype(jnp.bfloat16), value_part, preferred_element_type=jnp.float32
    )
    return (new_max, new_sum, new_weighted)


def on_device(hidden, w_query, w_keyvalue, w_output, segment_ids):
    fsdp_count = lax.axis_size("fsdp")
    seq_count = lax.axis_size("sp")
    fsdp_index = lax.axis_index("fsdp")
    seq_index = lax.axis_index("sp")
    tok_rows = hidden.shape[0]
    sub_rows = tok_rows // fsdp_count
    kv_count = seq_count // GROUP
    query_rows = seq_count * sub_rows
    offsets = jnp.arange(query_rows, dtype=jnp.int32)
    query_pos = offsets // sub_rows * tok_rows + fsdp_index * sub_rows + offsets % sub_rows
    own_positions = (
        seq_index * tok_rows + fsdp_index * sub_rows + jnp.arange(sub_rows, dtype=jnp.int32)
    )

    def project(weight_block):
        return jnp.dot(hidden, weight_block, preferred_element_type=jnp.float32)

    query_part = project(lax.all_gather(w_query, "sp", axis=1, tiled=True))
    kv_part = project(lax.all_gather(w_keyvalue, "sp", axis=1, tiled=True))
    query_sum, kv_sum = (
        lax.psum_scatter(query_part, "fsdp", scatter_dimension=0, tiled=True),
        lax.psum_scatter(kv_part, "fsdp", scatter_dimension=0, tiled=True),
    )
    query_local = rotate(query_sum, own_positions, seq_count, HD).astype(jnp.bfloat16)
    pairs = split_keys(kv_sum, own_positions, kv_count, HD)
    expanded = jnp.repeat(pairs, GROUP, axis=1).reshape(sub_rows, seq_count * 2 * HD)
    query_head, kv_head = (
        lax.all_to_all(query_local, "sp", split_axis=1, concat_axis=0, tiled=True),
        lax.all_to_all(expanded, "sp", split_axis=1, concat_axis=0, tiled=True),
    )
    segment_all = lax.all_gather(segment_ids, "sp", axis=0, tiled=True)
    query_seg = segment_all[query_pos]
    initial = (
        jnp.full((query_rows,), NEG_FILL, jnp.float32),
        jnp.zeros((query_rows,), jnp.float32),
        jnp.zeros((query_rows, HD), jnp.float32),
    )
    block_keys = lax.all_gather(kv_head, "fsdp", axis=0, tiled=True)
    piece_rows = block_keys.shape[0]
    row_ids = jnp.arange(piece_rows, dtype=jnp.int32)
    source_id = row_ids // query_rows
    within = row_ids % query_rows
    key_pos = within // sub_rows * tok_rows + source_id * sub_rows + within % sub_rows
    key_seg = segment_all[key_pos]
    final_max, final_sum, final_weighted = merge_keys(
        initial, query_head, query_pos, query_seg, block_keys, key_pos, key_seg
    )
    attention = (final_weighted / final_sum[:, None]).astype(jnp.bfloat16)
    back_rows = lax.all_to_all(attention, "sp", split_axis=0, concat_axis=1, tiled=True)
    mixed_rows = lax.all_gather(back_rows, "fsdp", axis=0, tiled=True)
    result = jnp.dot(
        mixed_rows,
        lax.all_gather(w_output, "sp", axis=0, tiled=True),
        preferred_element_type=jnp.float32,
    )
    return result.astype(jnp.bfloat16)


NEG_POS = -1
WO_CHUNKS = 4
MOVED = 4
END_CHUNKS = 3


def fused_kernel(
    nf, nz, nx, hid, wq, wkv, wo, seg, out,
    h_buf, wq_buf, wkv_buf, wo_buf, seg_buf,
    q_part, q_mate, q_sum, q_far, kv_part, kv_recv, kv_piece, kv_all, mix_own, mix_buf, q_cos, q_sin,
    out_buf, out_away, h_end, e_part, e_mate, e_sum, e_far, e_back, q_in,
    s_loc, s_hid, r_hid, s_seg, r_seg, s_wkv, r_wkv, s_wq, r_wq,
    s_q, r_q, s_qf, r_qf, s_kvp, r_kvp, s_kv, r_kv, s_kn, s_wo, r_wo, r_rest, s_wox, r_wox, s_mix, r_mix,
    s_out, r_out, s_res, s_he, r_he, s_hx, s_ep, r_ep, s_ef, r_ef, s_eb, r_eb,
):
    f = lax.axis_index("fsdp")
    s = lax.axis_index("sp")
    z, x = s // nx, s % nx
    tok, kdim = hid.shape
    rows = tok * nx
    sub = rows // nf
    kvw = wkv.shape[0]
    other = 1 - x
    moved = kdim * MOVED // 8
    block = tok // 2
    half_cols = wo.shape[1] // nx
    chunk = half_cols // WO_CHUNKS
    f32, bf16 = jnp.float32, jnp.bfloat16
    is_end = (z == 0) | (z == nz - 1)
    is_inner = jnp.logical_not(is_end)
    low = z < nz // 2
    e = jnp.where(low, 0, nz - 1)
    n = jnp.where(low, 1, nz - 2)
    m = nz - 1 - n
    e2 = nz - 1 - e
    beside = f + 1 - 2 * lax.rem(f, 2)
    ahead = lax.rem(f + 2, nf)
    across = lax.rem(beside + 2, nf)

    def block_of(ff):
        return lax.rem(ff, 2) * 2 + ff // 2

    core = lax.rem(f, 2)
    mine, theirs = block_of(f), block_of(ahead)
    near = core == z // 2

    def dev(ff, zz, xx):
        return (ff, zz * nx + xx)

    def remote(src, dst, ss, rs, target):
        return pltpu.make_async_remote_copy(
            src_ref=src, dst_ref=dst, send_sem=ss, recv_sem=rs,
            device_id=target, device_id_type=pl.DeviceIdType.MESH,
        )

    def tile(ref, count):
        return pl.ds(pl.multiple_of(ref * count, count), count)

    here = (f, s)
    def cols(c):
        return slice(c * chunk, (c + 1) * chunk)

    own_h = pltpu.make_async_copy(hid, h_buf.at[tile(x, tok)], s_loc.at[0])
    own_wq = pltpu.make_async_copy(
        wq, wq_buf.at[z // 2, :, tile(lax.rem(z, 2), HD)], s_loc.at[1]
    )
    own_wkv = pltpu.make_async_copy(wkv, wkv_buf.at[tile(z, kvw)], s_loc.at[2])
    own_wo = [
        pltpu.make_async_copy(
            wo.at[:, h * half_cols : (h + 1) * half_cols],
            wo_buf.at[h, tile(s, HD)], s_loc.at[3 + h],
        )
        for h in range(nx)
    ]
    own_seg = pltpu.make_async_copy(seg, seg_buf.at[1, x], s_loc.at[5])
    for copy in (own_wkv, own_wq, own_h, *own_wo, own_seg):
        copy.start()

    def hid_send():
        return remote(
            h_buf.at[tile(x, tok)], h_buf.at[tile(x, tok)], s_hid, r_hid, dev(f, z, other)
        )

    def hid_wait():
        remote(
            h_buf.at[tile(other, tok)], h_buf.at[tile(other, tok)], s_hid, r_hid, here
        ).wait_recv()

    def wkv_z(j, d, target):
        ref = wkv_buf.at[tile(j, kvw)]
        return remote(ref, ref, s_wkv.at[d], r_wkv.at[j], dev(f, target, x))

    def wkv_wait(j):
        wkv_z(j, 0, z).wait_recv()

    def wq_z(j, part, d, target):
        features = slice(moved, kdim) if part == 0 else slice(0, moved)
        ref = wq_buf.at[j // 2, features, tile(lax.rem(j, 2), HD)]
        return remote(ref, ref, s_wq.at[d], r_wq.at[j, part], dev(f, target, x))

    def wq_wait(j, part):
        wq_z(j, part, 1, z).wait_recv()

    def he_z(hf):
        rows_of = pl.ds(pl.multiple_of(x * tok + hf * block, block), block)
        return remote(
            h_buf.at[rows_of, 0:moved], h_end.at[x, hf], s_he, r_he.at[x, hf], dev(f, n, x)
        )

    def he_x(hf):
        ref = h_end.at[x, hf]
        return remote(ref, ref, s_hx, r_he.at[x, hf], dev(f, z, other))

    def he_wait(xx, hf):
        ref = h_end.at[xx, hf]
        remote(ref, ref, s_hx, r_he.at[xx, hf], here).wait_recv()

    def wo_unit(h, j, xx, c):
        return wo_buf.at[h, tile(j * nx + xx, HD), cols(c)]

    def wo_z(j, xx, c, d, target):
        ref = wo_unit(x, j, xx, c)
        return remote(ref, ref, s_wo.at[d], r_wo.at[j, xx, c], dev(f, target, x))

    def wo_pair(c):
        ref = wo_unit(other, z, x, c)
        return remote(ref, ref, s_wox, r_wo.at[z, x, c], dev(f, z, other))

    def wo_wait(j, xx, c):
        ref = wo_unit(x, j, xx, c)
        remote(ref, ref, s_wox, r_wo.at[j, xx, c], here).wait_recv()

    def wo_cross(j, xx, c):
        ref = wo_unit(x, j, xx, c)
        return remote(ref, ref, s_wox, r_wox.at[c], dev(f, z, other))

    def wo_rest(c):
        ref = wo_unit(other, n, x, c)
        return remote(ref, ref, s_wo.at[0], r_rest.at[c], dev(f, e, x))

    def wo_swap(c):
        ref = wo_unit(other, n, x, c)
        remote(ref, ref, s_wox, r_rest.at[c], here).wait_recv()
        return remote(ref, ref, s_wox, r_wo.at[n, x, c], dev(f, z, other))

    def wox_wait(c):
        ref = wo_buf.at[other, 2 * HD :, cols(c)]
        remote(ref, ref, s_wox, r_wox.at[c], here).wait_recv()

    def seg_same():
        return remote(seg_buf.at[1, x], seg_buf.at[1, x], s_seg.at[0], r_seg.at[1], dev(f, z, other))

    def seg_next(xx):
        return remote(
            seg_buf.at[1, x], seg_buf.at[0, x], s_seg.at[1], r_seg.at[0], dev(f, z + 1, xx)
        )

    barrier = pltpu.get_barrier_semaphore()

    def greet(ff, zz, xx):
        pl.semaphore_signal(
            barrier, inc=1, device_id=dev(ff, zz, xx), device_id_type=pl.DeviceIdType.MESH
        )

    plane = nf * nx
    for step in (1, -1):
        @pl.when((z + step >= 0) & (z + step < nz))
        def _():
            for xx in range(nx):
                greet(f, z + step, xx)

    for d in range(1, plane):
        greet(lax.rem(f + d, nf), z, lax.rem(x + d // nf, nx))
    pl.semaphore_wait(barrier, plane - 1 + jnp.where(is_end, nx, 2 * nx))

    own_wkv.wait()
    own_wq.wait()

    @pl.when(is_end)
    def _():
        wkv_z(z, 1, n).start()
        wq_z(z, 0, 1, n).start()
        wq_z(z, 1, 1, n).start()

    @pl.when(is_inner)
    def _():
        for d, target in ((0, e), (1, m)):
            wkv_z(z, d, target).start()
            wq_z(z, 0, d, target).start()
        wq_z(z, 1, 1, m).start()

    own_h.wait()
    hid_send().start()
    own_seg.wait()
    seg_same().start()

    @pl.when(z < nz - 1)
    def _():
        for xx in range(nx):
            seg_next(xx).start()

    for copy in own_wo:
        copy.wait()

    @pl.when(is_end)
    def _():
        for hf in range(2):
            he_z(hf).start()
        for c in range(WO_CHUNKS):
            wo_z(z, x, c, 1, n).start()
        for c in range(WO_CHUNKS):
            wo_pair(c).start()
        for c in range(END_CHUNKS):
            wo_cross(z, x, c).start()

    @pl.when(is_inner)
    def _():
        for c in range(WO_CHUNKS):
            wo_z(z, x, c, 0, e).start()

    @pl.when(z == 0)
    def _():
        kv_all[0] = jnp.zeros(kv_all.shape[1:], bf16)
        seg_buf[0] = jnp.full(seg_buf.shape[1:], NEG_POS, jnp.int32)

    @pl.when(is_inner)
    def _():
        q_in[...] = jnp.zeros(q_in.shape, f32)

    def table(row_count, first, lane_index):
        position = (first + lax.broadcasted_iota(jnp.int32, (row_count, HD), 0)).astype(f32)
        frequency = jnp.exp(lane_index.astype(f32) * (-2.0 * math.log(ROPE_BASE) / HD))
        return position * frequency

    lane = lax.broadcasted_iota(jnp.int32, (1, HD), 1)
    half = HD // 2
    quarter = half // nx
    kv_angle = table(sub, z * rows + f * sub, x * quarter + lane % quarter)
    is_key = lane < half
    kv_cos = jnp.where(is_key, jnp.cos(kv_angle), 1.0)
    kv_sin = jnp.where(is_key, jnp.sin(kv_angle), 0.0)
    kv_sin = jnp.where(lane < quarter, -kv_sin, kv_sin)
    q_angle = table(rows, z * rows, lane % half)
    q_sine = jnp.sin(q_angle)
    q_cos[...] = jnp.cos(q_angle)
    q_sin[...] = jnp.where(lane < half, -q_sine, q_sine)

    same_core = lambda j: j // 2 == core

    def q_send(j):
        return remote(
            q_part.at[j], q_mate.at[lax.rem(j, 2)], s_q, r_q, dev(beside, z, x)
        )

    def q_far_copy():
        return remote(q_sum, q_far, s_qf, r_qf, dev(ahead, z, x))

    def q_project(j, first):
        both = jnp.dot(
            h_buf[:, first:], wq_buf[j // 2, first:, :], preferred_element_type=f32
        )
        for b in range(2):
            q_part[j // 2 * 2 + b] = both[:, b * HD : (b + 1) * HD]

        @pl.when(jnp.logical_not(same_core(j)))
        def _():
            for b in range(2):
                q_send(j // 2 * 2 + b).start()

    def q_relay(far):
        @pl.when(jnp.logical_not(near) if far else near)
        def _():
            remote(q_mate, q_mate, s_q, r_q, here).wait_recv()
            q_sum[...] = q_part[theirs] + q_mate[lax.rem(theirs, 2)]
            q_far_copy().start()

    def e_send(j, xx, hf):
        return remote(
            e_part.at[j, xx, hf], e_mate.at[lax.rem(j, 2), xx, hf],
            s_ep, r_ep.at[xx, hf], dev(beside, z, x)
        )

    def e_far_copy(xx, hf):
        return remote(
            e_sum.at[xx, hf], e_far.at[xx, hf], s_ef, r_ef.at[xx, hf], dev(ahead, z, x)
        )

    def e_project(xx, hf, j):
        both = jnp.dot(
            h_end[xx, hf], wq_buf[j // 2, 0:moved, :], preferred_element_type=f32
        )
        for b in range(2):
            e_part[j // 2 * 2 + b, xx, hf] = both[:, b * HD : (b + 1) * HD]

        @pl.when(jnp.logical_not(same_core(j)))
        def _():
            for b in range(2):
                e_send(j // 2 * 2 + b, xx, hf).start()

    def e_relay(xx, hf):
        ref = e_mate.at[:, xx, hf]
        remote(ref, ref, s_ep, r_ep.at[xx, hf], here).wait_recv()
        e_sum[xx, hf] = e_part[theirs, xx, hf] + e_mate[lax.rem(theirs, 2), xx, hf]
        e_far_copy(xx, hf).start()

    def e_return(xx, hf):
        return remote(
            e_back.at[xx, hf], q_in.at[xx, hf], s_eb, r_eb, dev(f, e, x)
        )

    def e_collect(xx, hf):
        ref = e_far.at[xx, hf]
        remote(ref, ref, s_ef, r_ef.at[xx, hf], here).wait_recv()
        e_back[xx, hf] = (
            e_part[mine, xx, hf] + e_mate[lax.rem(mine, 2), xx, hf] + e_far[xx, hf]
        )
        e_return(xx, hf).start()

    @pl.when(is_inner)
    def _():
        wkv_wait(e)
        wkv_z(e, 1, m).start()
        wkv_wait(m)
        wkv_z(m, 0, e).start()
        wq_wait(e, 0)
        wq_z(e, 0, 1, m).start()
        wq_wait(m, 0)
        wq_z(m, 0, 0, e).start()
        wq_wait(e, 1)
        wq_z(e, 1, 1, m).start()
        wkv_wait(e2)
        wkv_z(e2, 0, e).start()
        he_wait(x, 0)
        he_x(0).start()
        wq_wait(e2, 0)
        wq_z(e2, 0, 0, e).start()
        for c in range(WO_CHUNKS):
            wo_rest(c).start()

    hid_wait()

    @pl.when(is_end)
    def _():
        for j in (n, m, e2):
            wkv_wait(j)

    kv_part[...] = lax.dot_general(
        h_buf[...], wkv_buf[...], (((1,), (1,)), ((), ())), preferred_element_type=f32
    )

    def kvp_send(d):
        ff = lax.rem(f + d, nf)
        return remote(
            kv_part.at[tile(ff, sub)], kv_recv.at[f], s_kvp, r_kvp, (ff, s)
        )

    for d in range(1, nf):
        kvp_send(d).start()

    @pl.when(is_inner)
    def _():
        q_project(z, 0)
        he_wait(x, 1)
        he_x(1).start()
        q_relay(False)
        e_project(x, 0, z)

        @pl.when(near)
        def _():
            e_relay(x, 0)


    @pl.when(is_end)
    def _():
        wq_wait(n, 0)
        q_project(z, moved)
        q_relay(False)

    total = kv_part[tile(f, sub), :]
    arrived = kv_recv.at[1:nf]
    remote(arrived, arrived, s_kvp, r_kvp, here).wait_recv()
    for d in range(1, nf):
        total = total + kv_recv[lax.rem(f + d, nf)]
    partner = jnp.where(
        lane < quarter, pltpu.roll(total, HD - quarter, 1), pltpu.roll(total, quarter, 1)
    )
    kv_piece[...] = (total * kv_cos + partner * kv_sin).astype(bf16)
    piece_rows = tile(f, sub)
    kv_all[1, x, piece_rows] = kv_piece[...]

    def kv_of(plane, ff, xx):
        return kv_all.at[plane, xx, tile(ff, sub)]

    def kv_hop(plane, ff, xx, hop):
        target = (dev(f, z, other), dev(ahead, z, x), dev(beside, z, x))[hop]
        ref = kv_of(plane, ff, xx)
        slot = hop + (hop == 2 or xx is other)
        return remote(ref, ref, s_kv.at[plane], r_kv.at[plane, slot], target)

    def kv_first(plane):
        for hop in range(3):
            kv_hop(plane, f, x, hop).start()

    def kv_second(plane):
        kv_wait(plane, f, other, 0)
        for hop in (1, 2):
            kv_hop(plane, f, other, hop).start()
        kv_wait(plane, ahead, x, 1)
        kv_hop(plane, ahead, x, 2).start()

    def kv_third(plane):
        kv_wait(plane, ahead, other, 2)
        kv_hop(plane, ahead, other, 2).start()

    def kv_last(plane):
        ref = kv_all.at[plane, x]
        remote(ref, ref, s_kn, r_kv.at[plane, 3], here).wait_recv()

    def kv_next():
        return remote(
            kv_piece, kv_all.at[0, x, piece_rows],
            s_kn, r_kv.at[0, 4], dev(f, z + 1, x),
        )

    def kv_wait(plane, ff, xx, slot):
        ref = kv_of(plane, ff, xx)
        remote(ref, ref, s_kn, r_kv.at[plane, slot], here).wait_recv()

    kv_first(1)

    @pl.when(z < nz - 1)
    def _():
        kv_next().start()

    @pl.when(is_end)
    def _():
        for c in range(WO_CHUNKS):
            wo_wait(z, other, c)
            wo_z(z, other, c, 1, n).start()

    @pl.when(is_inner)
    def _():
        for c in range(WO_CHUNKS):
            wo_z(z, x, c, 1, m).start()
        wq_wait(m, 1)
        wq_wait(e2, 1)
        q_project(e2, 0)
        e_project(x, 0, e2)
        e_project(x, 1, z)
        e_project(x, 1, e2)

        @pl.when(jnp.logical_not(near))
        def _():
            e_relay(x, 0)

        e_relay(x, 1)
        he_wait(other, 0)
        e_project(other, 0, z)
        e_project(other, 0, e2)
        e_relay(other, 0)

    @pl.when(z > 0)
    def _():
        kv_wait(0, f, x, 4)
        kv_first(0)

    kv_second(1)

    @pl.when(is_inner)
    def _():
        for c in range(WO_CHUNKS):
            wo_pair(c).start()
        for c in range(WO_CHUNKS):
            wo_wait(e, x, c)
            wo_z(e, x, c, 1, m).start()
        e_collect(x, 0)
        he_wait(other, 1)
        e_project(other, 1, z)
        e_project(other, 1, e2)
        e_relay(other, 1)
        q_relay(True)
        for c in range(WO_CHUNKS):
            wo_wait(m, x, c)
            wo_z(m, x, c, 0, e).start()
        kv_third(1)

        @pl.when(z > 0)
        def _():
            kv_second(0)

        e_collect(other, 0)
        e_collect(x, 1)
        e_collect(other, 1)
        for c in range(WO_CHUNKS):
            wo_wait(e, other, c)
            wo_z(e, other, c, 1, m).start()

        @pl.when(z > 0)
        def _():
            kv_third(0)

        for c in range(WO_CHUNKS):
            wo_wait(e2, x, c)
            wo_z(e2, x, c, 0, e).start()

    def cross(j, xx):
        for c in range(WO_CHUNKS):
            wo_wait(j, xx, c)
            if c < END_CHUNKS:
                wo_cross(j, xx, c).start()

    @pl.when(is_end)
    def _():
        cross(n, x)
        kv_third(1)

        @pl.when(z > 0)
        def _():
            kv_second(0)

        wq_wait(m, 0)
        wq_wait(e2, 0)
        q_project(e2, moved)
        q_relay(True)

        @pl.when(z > 0)
        def _():
            kv_third(0)

        for c in range(WO_CHUNKS):
            wo_swap(c).start()
        cross(m, x)
        remote(q_in, q_in, s_eb, r_eb, here).wait_recv()

    remote(q_far, q_far, s_qf, r_qf, here).wait_recv()
    q_total = q_part[mine] + q_mate[lax.rem(mine, 2)] + q_far[...]
    returned = q_in[...].reshape(rows, HD)
    q_total = q_total + jnp.where(is_end, returned, 0.0)
    q_turned = q_total * q_cos[...] + pltpu.roll(q_total, half, 1) * q_sin[...]
    q_head = q_turned.astype(bf16).astype(f32)
    quarters = []
    for xx in range(nx):
        first = q_head if xx == 0 else pltpu.roll(q_head, HD - xx * quarter, 1)
        second = pltpu.roll(q_head, (HD - half - xx * quarter + quarter) % HD, 1)
        picked = jnp.where(lane < quarter, first, jnp.where(lane < half, second, 0.0))
        quarters.append(picked.astype(bf16))

    seg_ref = seg_buf.at[1, other]
    remote(seg_ref, seg_ref, s_seg.at[0], r_seg.at[1], here).wait_recv()
    kv_last(1)

    @pl.when(z > 0)
    def _():
        before = seg_buf.at[0]
        remote(before, before, s_seg.at[1], r_seg.at[0], here).wait_recv()
        kv_last(0)

    key_seg = jnp.concatenate(
        [seg_buf[plane, xx] for plane in range(2) for xx in range(nx)], axis=1
    )
    own_seg_row = key_seg[:, rows:]
    seg_column = jnp.transpose(jnp.broadcast_to(own_seg_row, (HD, rows)))[:, :1]
    key_pos = lax.broadcasted_iota(jnp.int32, (1, 2 * rows), 1) - rows
    keys = [
        jnp.concatenate([kv_all[0, xx], kv_all[1, xx]], axis=0) for xx in range(nx)
    ]
    step_rows = rows // nf
    for b in range(nf):
        span = slice(b * step_rows, (b + 1) * step_rows)
        query_pos = b * step_rows + lax.broadcasted_iota(jnp.int32, (step_rows, 1), 0)
        score = None
        for xx in range(nx):
            term = lax.dot_general(
                quarters[xx][span], keys[xx], (((1,), (1,)), ((), ())),
                preferred_element_type=f32,
            )
            score = term if score is None else score + term
        allowed = (key_pos <= query_pos) & (key_seg == seg_column[span])
        masked = jnp.where(allowed, score * HD ** (-0.5), NEG_FILL)
        row_max = jnp.max(masked, axis=1, keepdims=True)
        weight = jnp.where(allowed, jnp.exp(masked - row_max), 0.0)
        row_total = jnp.sum(weight, axis=1, keepdims=True)
        rounded = weight.astype(bf16)
        product = [
            jnp.dot(rounded, keys[xx], preferred_element_type=f32) for xx in range(nx)
        ]
        mixed = None
        for xx in reversed(range(nx)):
            first = pltpu.roll(product[xx], (half + xx * quarter) % HD, 1)
            second = pltpu.roll(product[xx], (HD - (nx - 1 - xx) * quarter) % HD, 1)
            lane_block = lane // quarter
            value = jnp.where(lane_block < nx, first, second)
            mixed = value if mixed is None else jnp.where(lane_block % nx == xx, value, mixed)
        mix_own[span, :] = (mixed / row_total).astype(bf16)

    head = mine * nx + x

    def mix_of(ff, xx):
        return mix_buf.at[:, tile(block_of(ff) * nx + xx, HD)]

    def mix_send(ff, xx, hop):
        target = (dev(f, z, other), dev(ahead, z, x), dev(beside, z, x))[hop]
        return remote(
            mix_of(ff, xx), mix_of(ff, xx), s_mix,
            r_mix.at[hop + (hop == 2 or xx is other)], target,
        )

    def mix_wait(ref, slot):
        remote(ref, ref, s_mix, r_mix.at[slot], here).wait_recv()

    mix_buf[:, tile(head, HD)] = mix_own[...]
    for hop in range(3):
        mix_send(f, x, hop).start()

    @pl.when(is_inner)
    def _():
        for c in range(WO_CHUNKS):
            wo_wait(z, other, c)
            wo_z(z, other, c, 1, m).start()

    @pl.when(is_end)
    def _():
        cross(e2, x)

    mix_wait(mix_of(f, other), 0)
    for hop in (1, 2):
        mix_send(f, other, hop).start()
    mix_wait(mix_of(ahead, x), 1)
    mix_send(ahead, x, 2).start()

    @pl.when(is_inner)
    def _():
        for c in range(WO_CHUNKS):
            wo_wait(e2, other, c)
            wo_z(e2, other, c, 0, e).start()

    @pl.when(is_end)
    def _():
        for c in range(WO_CHUNKS):
            wo_wait(n, other, c)
        cross(e2, other)

    mix_wait(mix_of(ahead, other), 2)
    mix_send(ahead, other, 2).start()

    def result(h, c):
        where = pl.ds(pl.multiple_of(h * half_cols + c * chunk, chunk), chunk)
        return pltpu.make_async_copy(out_buf.at[h, :, cols(c)], out.at[:, where], s_res)

    mix_wait(mix_buf.at[:, 0 : 4 * HD], 3)

    def product(h, c, row_tile):
        return jnp.dot(
            mix_buf[tile(row_tile, tok), :], wo_buf[h, :, cols(c)], preferred_element_type=f32
        ).astype(bf16)

    def away(c):
        return remote(
            out_away.at[c], out_buf.at[x, :, cols(c)], s_out, r_out.at[c], dev(f, z, other)
        )

    def away_stage(c):
        out_away[c] = product(x, c, other)
        away(c).start()

    def own_stage(h, c):
        out_buf[h, :, cols(c)] = product(h, c, x)
        result(h, c).start()

    def away_wait(c):
        ref = out_buf.at[other, :, cols(c)]
        remote(ref, ref, s_out, r_out.at[c], here).wait_recv()
        result(other, c).start()

    def drained(sem, size):
        ruler = wo_buf.at[0, 0 : size // (half_cols * 2), :]
        remote(ruler, ruler, sem, r_hid, here).wait_send()

    def settle(kind):
        inner = kind == "inner"
        unit = HD * chunk * 2
        drained(s_hid, tok * kdim * 2)
        drained(s_wkv.at[1], (2 if inner else 1) * kvw * kdim * 2)
        drained(s_wq.at[1], (2 if inner else 1) * kdim * HD * 2)
        drained(s_wo.at[1], (2 if inner else 1) * nx * WO_CHUNKS * unit)
        crossed = 0 if inner else (nz * nx - 2) * END_CHUNKS + WO_CHUNKS
        drained(s_wox, (WO_CHUNKS + crossed) * unit)
        drained(s_hx if inner else s_he, 2 * block * moved * 2)
        drained(s_q, 2 * rows * HD * 4)
        drained(s_qf, rows * HD * 4)
        drained(s_kvp, (nf - 1) * sub * nz * kvw * 4)
        drained(s_kv.at[1], (nf * nx - 1) * sub * HD * 2)
        drained(s_mix, (nf * nx - 1) * rows * HD * 2)
        drained(s_out, (WO_CHUNKS if inner else WO_CHUNKS - END_CHUNKS) * tok * chunk * 2)
        if inner:
            drained(s_wkv.at[0], 3 * kvw * kdim * 2)
            drained(s_wq.at[0], 3 * (kdim - moved) * HD * 2)
            drained(s_wo.at[0], 3 * nx * WO_CHUNKS * unit)
            drained(s_ep, 2 * rows * HD * 4)
            drained(s_ef, rows * HD * 4)
            drained(s_eb, rows * HD * 4)
        seg_same().wait_send()

        @pl.when(z < nz - 1)
        def _():
            before = seg_buf.at[0]
            remote(before, before, s_seg.at[1], r_seg.at[0], here).wait_send()
            kv_next().wait_send()

        @pl.when(z > 0)
        def _():
            drained(s_kv.at[0], (nf * nx - 1) * sub * HD * 2)

    order = [*range(END_CHUNKS, WO_CHUNKS), *range(END_CHUNKS)]

    @pl.when(is_inner)
    def _():
        for c in order:
            wo_wait(m, other, c)
            wo_z(m, other, c, 0, e).start()
            away_stage(c)
        for c in order:
            own_stage(x, c)
        for c in order:
            away_wait(c)
        settle("inner")

    @pl.when(is_end)
    def _():
        for c in order:
            wo_wait(m, other, c)
            if c < END_CHUNKS:
                wo_cross(m, other, c).start()
            if c >= END_CHUNKS:
                away_stage(c)
        for c in order:
            own_stage(x, c)
        for c in range(END_CHUNKS):
            wox_wait(c)
            own_stage(other, c)
        for c in range(END_CHUNKS, WO_CHUNKS):
            away_wait(c)
        settle("end")

    ruler = wo_buf.at[0, 0 : tok * nx, :]
    pltpu.make_async_copy(ruler, ruler, s_res).wait()


def fused_on_device(nf, nz, nx, hidden, w_query, w_keyvalue, w_output, segment_ids):
    tok, kdim = hidden.shape
    cols = w_output.shape[1]
    rows = tok * nx
    sub = rows // nf
    kvw = w_keyvalue.shape[1]
    heads = nz * nx
    part = cols // nx
    f32, bf16 = jnp.float32, jnp.bfloat16
    dma = pltpu.SemaphoreType.DMA
    vmem = pl.BlockSpec(memory_space=pltpu.VMEM)
    anywhere = pl.BlockSpec(memory_space=pl.ANY)
    scratch = [
        pltpu.VMEM((rows, kdim), bf16),
        pltpu.VMEM((nz // 2, kdim, 2 * HD), bf16),
        pltpu.VMEM((nz * kvw, kdim), bf16),
        pltpu.VMEM((nx, heads * HD, part), bf16),
        pltpu.VMEM((2, nx, 1, tok), jnp.int32),
        pltpu.VMEM((nz, rows, HD), f32),
        pltpu.VMEM((nf // 2, rows, HD), f32),
        pltpu.VMEM((rows, HD), f32),
        pltpu.VMEM((rows, HD), f32),
        pltpu.VMEM((rows, nz * kvw), f32),
        pltpu.VMEM((nf, sub, nz * kvw), f32),
        pltpu.VMEM((sub, HD), bf16),
        pltpu.VMEM((2, nx, rows, HD), bf16),
        pltpu.VMEM((rows, HD), bf16),
        pltpu.VMEM((rows, heads * HD), bf16),
        pltpu.VMEM((rows, HD), f32),
        pltpu.VMEM((rows, HD), f32),
        pltpu.VMEM((nx, tok, part), bf16),
        pltpu.VMEM((WO_CHUNKS, tok, part // WO_CHUNKS), bf16),
        pltpu.VMEM((nx, 2, tok // 2, kdim * MOVED // 8), bf16),
        pltpu.VMEM((nz, nx, 2, tok // 2, HD), f32),
        pltpu.VMEM((nf // 2, nx, 2, tok // 2, HD), f32),
        pltpu.VMEM((nx, 2, tok // 2, HD), f32),
        pltpu.VMEM((nx, 2, tok // 2, HD), f32),
        pltpu.VMEM((nx, 2, tok // 2, HD), f32),
        pltpu.VMEM((nx, 2, tok // 2, HD), f32),
        dma((6,)), dma, dma, dma((2,)), dma((2,)), dma((2,)), dma((nz,)), dma((2,)), dma((nz, 2)),
        dma, dma, dma, dma, dma, dma, dma((2,)), dma((2, 5)), dma,
        dma((2,)), dma((nz, nx, WO_CHUNKS)), dma((WO_CHUNKS,)), dma, dma((WO_CHUNKS,)), dma,
        dma((4,)),
        dma, dma((WO_CHUNKS,)), dma, dma, dma((nx, 2)), dma,
        dma, dma((nx, 2)), dma, dma((nx, 2)), dma, dma,
    ]
    return pl.pallas_call(
        functools.partial(fused_kernel, nf, nz, nx),
        out_shape=jax.ShapeDtypeStruct((tok, cols), bf16),
        in_specs=[anywhere] * 4 + [vmem],
        out_specs=anywhere,
        scratch_shapes=scratch,
        name="fused_sublayer",
        compiler_params=pltpu.CompilerParams(
            collective_id=0, has_side_effects=True, vmem_limit_bytes=60 * 1024 * 1024
        ),
    )(hidden, w_query, w_keyvalue.T, w_output, segment_ids.reshape(1, tok))


def solution(mesh):
    in_specs = (P("sp", "fsdp"), P("fsdp", "sp"), P("fsdp", "sp"), P("sp", "fsdp"), P("sp"))
    out_specs = P("sp", "fsdp")
    nf, sp = mesh.shape["fsdp"], mesh.shape["sp"]
    if sp == GROUP and sp == 2 * nf:
        body = functools.partial(fused_on_device, nf, nf, sp // nf)
    else:
        body = on_device
    return jax.shard_map(
        body, mesh=mesh, in_specs=in_specs, out_specs=out_specs, check_vma=False
    )
```

```python
import functools
import math

import jax
import jax.numpy as jnp
from jax import lax
from jax.experimental import pallas as pl
from jax.experimental.pallas import tpu as pltpu
from jax.sharding import PartitionSpec as P

HD = 128
GROUP = 8


ROPE_BASE = 500000.0
NEG_FILL = -1e30


def rotate(values, positions, head_count, width):
    row_count = values.shape[0]
    shaped = values.reshape(row_count, head_count, width)
    half_width = width // 2
    frequency = jnp.exp(
        jnp.arange(half_width, dtype=jnp.float32) * (-2.0 * math.log(ROPE_BASE) / width)
    )
    angles = positions.astype(jnp.float32)[:, None] * frequency[None, :]
    cosine = jnp.cos(angles)[:, None, :]
    sine_part = jnp.sin(angles)[:, None, :]
    lower_half = shaped[:, :, :half_width]
    upper_half = shaped[:, :, half_width:]
    turned = jnp.concatenate(
        [
            lower_half * cosine - upper_half * sine_part,
            upper_half * cosine + lower_half * sine_part,
        ],
        axis=2,
    )
    return turned.reshape(row_count, head_count * width)


def split_keys(kv_sum, positions, kv_count, width):
    row_count = kv_sum.shape[0]
    shaped = kv_sum.reshape(row_count, kv_count, 2, width)
    key_part = rotate(
        shaped[:, :, 0, :].reshape(row_count, kv_count * width), positions, kv_count, width
    )
    key_part = key_part.reshape(row_count, kv_count, 1, width)
    return jnp.concatenate([key_part, shaped[:, :, 1:2, :]], axis=2).astype(jnp.bfloat16)


def merge_keys(
    state_in, query_tile, query_pos_tile, query_seg_tile, key_tile, key_pos_tile, key_seg_tile
):
    running_max, running_sum, weighted = state_in
    allowed = (key_pos_tile[None, :] <= query_pos_tile[:, None]) & (
        key_seg_tile[None, :] == query_seg_tile[:, None]
    )
    key_part = key_tile[:, :HD]
    value_part = key_tile[:, HD:]
    scores = lax.dot_general(
        query_tile, key_part, (((1,), (1,)), ((), ())), preferred_element_type=jnp.float32
    ) * HD ** (-0.5)
    masked = jnp.where(allowed, scores, NEG_FILL)
    new_max = jnp.maximum(running_max, jnp.max(masked, axis=1))
    weights = jnp.where(allowed, jnp.exp(masked - new_max[:, None]), 0.0)
    new_sum = jnp.sum(weights, axis=1)
    new_weighted = jnp.dot(
        weights.astype(jnp.bfloat16), value_part, preferred_element_type=jnp.float32
    )
    return (new_max, new_sum, new_weighted)


def on_device(hidden, w_query, w_keyvalue, w_output, segment_ids):
    fsdp_count = lax.axis_size("fsdp")
    seq_count = lax.axis_size("sp")
    fsdp_index = lax.axis_index("fsdp")
    seq_index = lax.axis_index("sp")
    tok_rows = hidden.shape[0]
    sub_rows = tok_rows // fsdp_count
    kv_count = seq_count // GROUP
    query_rows = seq_count * sub_rows
    offsets = jnp.arange(query_rows, dtype=jnp.int32)
    query_pos = offsets // sub_rows * tok_rows + fsdp_index * sub_rows + offsets % sub_rows
    own_positions = (
        seq_index * tok_rows + fsdp_index * sub_rows + jnp.arange(sub_rows, dtype=jnp.int32)
    )

    def project(weight_block):
        return jnp.dot(hidden, weight_block, preferred_element_type=jnp.float32)

    query_part = project(lax.all_gather(w_query, "sp", axis=1, tiled=True))
    kv_part = project(lax.all_gather(w_keyvalue, "sp", axis=1, tiled=True))
    query_sum, kv_sum = (
        lax.psum_scatter(query_part, "fsdp", scatter_dimension=0, tiled=True),
        lax.psum_scatter(kv_part, "fsdp", scatter_dimension=0, tiled=True),
    )
    query_local = rotate(query_sum, own_positions, seq_count, HD).astype(jnp.bfloat16)
    pairs = split_keys(kv_sum, own_positions, kv_count, HD)
    expanded = jnp.repeat(pairs, GROUP, axis=1).reshape(sub_rows, seq_count * 2 * HD)
    query_head, kv_head = (
        lax.all_to_all(query_local, "sp", split_axis=1, concat_axis=0, tiled=True),
        lax.all_to_all(expanded, "sp", split_axis=1, concat_axis=0, tiled=True),
    )
    segment_all = lax.all_gather(segment_ids, "sp", axis=0, tiled=True)
    query_seg = segment_all[query_pos]
    initial = (
        jnp.full((query_rows,), NEG_FILL, jnp.float32),
        jnp.zeros((query_rows,), jnp.float32),
        jnp.zeros((query_rows, HD), jnp.float32),
    )
    block_keys = lax.all_gather(kv_head, "fsdp", axis=0, tiled=True)
    piece_rows = block_keys.shape[0]
    row_ids = jnp.arange(piece_rows, dtype=jnp.int32)
    source_id = row_ids // query_rows
    within = row_ids % query_rows
    key_pos = within // sub_rows * tok_rows + source_id * sub_rows + within % sub_rows
    key_seg = segment_all[key_pos]
    final_max, final_sum, final_weighted = merge_keys(
        initial, query_head, query_pos, query_seg, block_keys, key_pos, key_seg
    )
    attention = (final_weighted / final_sum[:, None]).astype(jnp.bfloat16)
    back_rows = lax.all_to_all(attention, "sp", split_axis=0, concat_axis=1, tiled=True)
    mixed_rows = lax.all_gather(back_rows, "fsdp", axis=0, tiled=True)
    result = jnp.dot(
        mixed_rows,
        lax.all_gather(w_output, "sp", axis=0, tiled=True),
        preferred_element_type=jnp.float32,
    )
    return result.astype(jnp.bfloat16)


NEG_POS = -1
WO_CHUNKS = 4
MOVED = 4
END_CHUNKS = 3
INNER_CHUNKS = 1


def fused_kernel(
    nf, nz, nx, hid, wq, wkv, wo, seg, out,
    h_buf, wq_buf, wkv_buf, wo_buf, seg_buf,
    q_part, q_mate, q_sum, q_far, kv_part, kv_recv, kv_piece, kv_all, mix_buf, q_cos, q_sin,
    out_buf, out_away, h_end, e_part, e_mate, e_sum, e_far, e_back, q_in,
    s_loc, s_hid, r_hid, s_seg, r_seg, s_wkv, r_wkv, s_wq, r_wq,
    s_q, r_q, s_qf, r_qf, s_kvp, r_kvp, s_kv, r_kv, s_kn, s_wo, r_wo, r_rest, s_wox, r_wox, s_mix, r_mix,
    s_out, r_out, s_res, s_he, r_he, s_hx, s_ep, r_ep, s_ef, r_ef, s_eb, r_eb,
):
    f = lax.axis_index("fsdp")
    s = lax.axis_index("sp")
    z, x = s // nx, s % nx
    tok, kdim = hid.shape
    rows = tok * nx
    sub = rows // nf
    kvw = wkv.shape[0]
    other = 1 - x
    moved = kdim * MOVED // 8
    block = tok // 2
    half_cols = wo.shape[1] // nx
    chunk = half_cols // WO_CHUNKS
    f32, bf16 = jnp.float32, jnp.bfloat16
    is_end = (z == 0) | (z == nz - 1)
    is_inner = jnp.logical_not(is_end)
    low = z < nz // 2
    e = jnp.where(low, 0, nz - 1)
    n = jnp.where(low, 1, nz - 2)
    m = nz - 1 - n
    e2 = nz - 1 - e
    beside = f + 1 - 2 * lax.rem(f, 2)
    ahead = lax.rem(f + 2, nf)
    across = lax.rem(beside + 2, nf)

    def block_of(ff):
        return lax.rem(ff, 2) * 2 + ff // 2

    core = lax.rem(f, 2)
    mine, theirs = block_of(f), block_of(ahead)
    near = core == z // 2

    def dev(ff, zz, xx):
        return (ff, zz * nx + xx)

    def remote(src, dst, ss, rs, target):
        return pltpu.make_async_remote_copy(
            src_ref=src, dst_ref=dst, send_sem=ss, recv_sem=rs,
            device_id=target, device_id_type=pl.DeviceIdType.MESH,
        )

    def tile(ref, count):
        return pl.ds(pl.multiple_of(ref * count, count), count)

    here = (f, s)
    def cols(c):
        return slice(c * chunk, (c + 1) * chunk)

    own_h = pltpu.make_async_copy(hid, h_buf.at[tile(x, tok)], s_loc.at[0])
    own_wq = pltpu.make_async_copy(
        wq, wq_buf.at[z // 2, :, tile(lax.rem(z, 2), HD)], s_loc.at[1]
    )
    own_wkv = pltpu.make_async_copy(wkv, wkv_buf.at[tile(z, kvw)], s_loc.at[2])
    own_wo = [
        pltpu.make_async_copy(
            wo.at[:, h * half_cols : (h + 1) * half_cols],
            wo_buf.at[h, tile(s, HD)], s_loc.at[3 + h],
        )
        for h in range(nx)
    ]
    own_seg = pltpu.make_async_copy(seg, seg_buf.at[1, x], s_loc.at[5])
    for copy in (own_wkv, own_wq, own_h, *own_wo, own_seg):
        copy.start()

    def hid_send():
        return remote(
            h_buf.at[tile(x, tok)], h_buf.at[tile(x, tok)], s_hid, r_hid, dev(f, z, other)
        )

    def hid_wait():
        remote(
            h_buf.at[tile(other, tok)], h_buf.at[tile(other, tok)], s_hid, r_hid, here
        ).wait_recv()

    def wkv_z(j, d, target):
        ref = wkv_buf.at[tile(j, kvw)]
        return remote(ref, ref, s_wkv.at[d], r_wkv.at[j], dev(f, target, x))

    def wkv_wait(j):
        wkv_z(j, 0, z).wait_recv()

    def wq_z(j, part, d, target):
        features = slice(moved, kdim) if part == 0 else slice(0, moved)
        ref = wq_buf.at[j // 2, features, tile(lax.rem(j, 2), HD)]
        return remote(ref, ref, s_wq.at[d], r_wq.at[j, part], dev(f, target, x))

    def wq_wait(j, part):
        wq_z(j, part, 1, z).wait_recv()

    def he_z(hf):
        rows_of = pl.ds(pl.multiple_of(x * tok + hf * block, block), block)
        return remote(
            h_buf.at[rows_of, 0:moved], h_end.at[x, hf], s_he, r_he.at[x, hf], dev(f, n, x)
        )

    def he_x(hf):
        ref = h_end.at[x, hf]
        return remote(ref, ref, s_hx, r_he.at[x, hf], dev(f, z, other))

    def he_wait(xx, hf):
        ref = h_end.at[xx, hf]
        remote(ref, ref, s_hx, r_he.at[xx, hf], here).wait_recv()

    def wo_unit(h, j, xx, c):
        return wo_buf.at[h, tile(j * nx + xx, HD), cols(c)]

    def wo_z(j, xx, c, d, target):
        ref = wo_unit(x, j, xx, c)
        return remote(ref, ref, s_wo.at[d], r_wo.at[j, xx, c], dev(f, target, x))

    def wo_pair(c):
        ref = wo_unit(other, z, x, c)
        return remote(ref, ref, s_wox, r_wo.at[z, x, c], dev(f, z, other))

    def wo_wait(j, xx, c):
        ref = wo_unit(x, j, xx, c)
        remote(ref, ref, s_wox, r_wo.at[j, xx, c], here).wait_recv()

    def wo_cross(j, xx, c):
        ref = wo_unit(x, j, xx, c)
        return remote(ref, ref, s_wox, r_wox.at[c], dev(f, z, other))

    def wo_rest(c):
        ref = wo_unit(other, n, x, c)
        return remote(ref, ref, s_wo.at[0], r_rest.at[c], dev(f, e, x))

    def wo_swap(c):
        ref = wo_unit(other, n, x, c)
        remote(ref, ref, s_wox, r_rest.at[c], here).wait_recv()
        return remote(ref, ref, s_wox, r_wo.at[n, x, c], dev(f, z, other))

    def wox_wait(c, held):
        ref = wo_buf.at[other, held * HD :, cols(c)]
        remote(ref, ref, s_wox, r_wox.at[c], here).wait_recv()

    def seg_same():
        return remote(seg_buf.at[1, x], seg_buf.at[1, x], s_seg.at[0], r_seg.at[1], dev(f, z, other))

    def seg_next(xx):
        return remote(
            seg_buf.at[1, x], seg_buf.at[0, x], s_seg.at[1], r_seg.at[0], dev(f, z + 1, xx)
        )

    barrier = pltpu.get_barrier_semaphore()

    def greet(ff, zz, xx):
        pl.semaphore_signal(
            barrier, inc=1, device_id=dev(ff, zz, xx), device_id_type=pl.DeviceIdType.MESH
        )

    plane = nf * nx
    for step in (1, -1):
        @pl.when((z + step >= 0) & (z + step < nz))
        def _():
            for xx in range(nx):
                greet(f, z + step, xx)

    for d in range(1, plane):
        greet(lax.rem(f + d, nf), z, lax.rem(x + d // nf, nx))
    pl.semaphore_wait(barrier, plane - 1 + jnp.where(is_end, nx, 2 * nx))

    own_wkv.wait()
    own_wq.wait()

    @pl.when(is_end)
    def _():
        wkv_z(z, 1, n).start()
        wq_z(z, 0, 1, n).start()
        wq_z(z, 1, 1, n).start()

    @pl.when(is_inner)
    def _():
        for d, target in ((0, e), (1, m)):
            wkv_z(z, d, target).start()
            wq_z(z, 0, d, target).start()
        wq_z(z, 1, 1, m).start()

    own_h.wait()
    hid_send().start()
    own_seg.wait()
    seg_same().start()

    @pl.when(z < nz - 1)
    def _():
        for xx in range(nx):
            seg_next(xx).start()

    for copy in own_wo:
        copy.wait()

    @pl.when(is_end)
    def _():
        for hf in range(2):
            he_z(hf).start()
        for c in range(WO_CHUNKS):
            wo_z(z, x, c, 1, n).start()
        for c in range(WO_CHUNKS):
            wo_pair(c).start()
        for c in range(END_CHUNKS):
            wo_cross(z, x, c).start()

    @pl.when(is_inner)
    def _():
        for c in range(WO_CHUNKS):
            wo_z(z, x, c, 0, e).start()

    @pl.when(z == 0)
    def _():
        kv_all[0] = jnp.zeros(kv_all.shape[1:], bf16)
        seg_buf[0] = jnp.full(seg_buf.shape[1:], NEG_POS, jnp.int32)

    @pl.when(is_inner)
    def _():
        q_in[...] = jnp.zeros(q_in.shape, f32)

    def table(row_count, first, lane_index):
        position = (first + lax.broadcasted_iota(jnp.int32, (row_count, HD), 0)).astype(f32)
        frequency = jnp.exp(lane_index.astype(f32) * (-2.0 * math.log(ROPE_BASE) / HD))
        return position * frequency

    lane = lax.broadcasted_iota(jnp.int32, (1, HD), 1)
    half = HD // 2
    quarter = half // nx
    kv_angle = table(sub, z * rows + f * sub, x * quarter + lane % quarter)
    is_key = lane < half
    kv_cos = jnp.where(is_key, jnp.cos(kv_angle), 1.0)
    kv_sin = jnp.where(is_key, jnp.sin(kv_angle), 0.0)
    kv_sin = jnp.where(lane < quarter, -kv_sin, kv_sin)
    q_angle = table(rows, z * rows, lane % half)
    q_sine = jnp.sin(q_angle)
    q_cos[...] = jnp.cos(q_angle)
    q_sin[...] = jnp.where(lane < half, -q_sine, q_sine)

    same_core = lambda j: j // 2 == core

    def q_send(j):
        return remote(
            q_part.at[j], q_mate.at[lax.rem(j, 2)], s_q, r_q, dev(beside, z, x)
        )

    def q_far_copy():
        return remote(q_sum, q_far, s_qf, r_qf, dev(ahead, z, x))

    def q_project(j, first):
        both = jnp.dot(
            h_buf[:, first:], wq_buf[j // 2, first:, :], preferred_element_type=f32
        )
        for b in range(2):
            q_part[j // 2 * 2 + b] = both[:, b * HD : (b + 1) * HD]

        @pl.when(jnp.logical_not(same_core(j)))
        def _():
            for b in range(2):
                q_send(j // 2 * 2 + b).start()

    def q_relay(far):
        @pl.when(jnp.logical_not(near) if far else near)
        def _():
            remote(q_mate, q_mate, s_q, r_q, here).wait_recv()
            q_sum[...] = q_part[theirs] + q_mate[lax.rem(theirs, 2)]
            q_far_copy().start()

    def e_send(j, xx, hf):
        return remote(
            e_part.at[j, xx, hf], e_mate.at[lax.rem(j, 2), xx, hf],
            s_ep, r_ep.at[xx, hf], dev(beside, z, x)
        )

    def e_far_copy(xx, hf):
        return remote(
            e_sum.at[xx, hf], e_far.at[xx, hf], s_ef, r_ef.at[xx, hf], dev(ahead, z, x)
        )

    def e_project(xx, hf, j):
        both = jnp.dot(
            h_end[xx, hf], wq_buf[j // 2, 0:moved, :], preferred_element_type=f32
        )
        for b in range(2):
            e_part[j // 2 * 2 + b, xx, hf] = both[:, b * HD : (b + 1) * HD]

        @pl.when(jnp.logical_not(same_core(j)))
        def _():
            for b in range(2):
                e_send(j // 2 * 2 + b, xx, hf).start()

    def e_relay(xx, hf):
        ref = e_mate.at[:, xx, hf]
        remote(ref, ref, s_ep, r_ep.at[xx, hf], here).wait_recv()
        e_sum[xx, hf] = e_part[theirs, xx, hf] + e_mate[lax.rem(theirs, 2), xx, hf]
        e_far_copy(xx, hf).start()

    def e_return(xx, hf):
        return remote(
            e_back.at[xx, hf], q_in.at[xx, hf], s_eb, r_eb, dev(f, e, x)
        )

    def e_collect(xx, hf):
        ref = e_far.at[xx, hf]
        remote(ref, ref, s_ef, r_ef.at[xx, hf], here).wait_recv()
        e_back[xx, hf] = (
            e_part[mine, xx, hf] + e_mate[lax.rem(mine, 2), xx, hf] + e_far[xx, hf]
        )
        e_return(xx, hf).start()

    @pl.when(is_inner)
    def _():
        wkv_wait(e)
        wkv_z(e, 1, m).start()
        wkv_wait(m)
        wkv_z(m, 0, e).start()
        wq_wait(e, 0)
        wq_z(e, 0, 1, m).start()
        wq_wait(m, 0)
        wq_z(m, 0, 0, e).start()
        wq_wait(e, 1)
        wq_z(e, 1, 1, m).start()
        wkv_wait(e2)
        wkv_z(e2, 0, e).start()
        he_wait(x, 0)
        he_x(0).start()
        wq_wait(e2, 0)
        wq_z(e2, 0, 0, e).start()
        for c in range(WO_CHUNKS):
            wo_rest(c).start()

    hid_wait()

    @pl.when(is_end)
    def _():
        for j in (n, m, e2):
            wkv_wait(j)

    kv_part[...] = lax.dot_general(
        h_buf[...], wkv_buf[...], (((1,), (1,)), ((), ())), preferred_element_type=f32
    )

    def kvp_send(d):
        ff = lax.rem(f + d, nf)
        return remote(
            kv_part.at[tile(ff, sub)], kv_recv.at[f], s_kvp, r_kvp, (ff, s)
        )

    for d in range(1, nf):
        kvp_send(d).start()

    @pl.when(is_inner)
    def _():
        q_project(z, 0)
        he_wait(x, 1)
        he_x(1).start()
        q_relay(False)
        e_project(x, 0, z)

        @pl.when(near)
        def _():
            e_relay(x, 0)


    @pl.when(is_end)
    def _():
        wq_wait(n, 0)
        q_project(z, moved)
        q_relay(False)

    total = kv_part[tile(f, sub), :]
    arrived = kv_recv.at[1:nf]
    remote(arrived, arrived, s_kvp, r_kvp, here).wait_recv()
    for d in range(1, nf):
        total = total + kv_recv[lax.rem(f + d, nf)]
    partner = jnp.where(
        lane < quarter, pltpu.roll(total, HD - quarter, 1), pltpu.roll(total, quarter, 1)
    )
    kv_piece[...] = (total * kv_cos + partner * kv_sin).astype(bf16)
    piece_rows = tile(f, sub)
    kv_all[1, x, piece_rows] = kv_piece[...]

    def kv_of(plane, ff, xx):
        return kv_all.at[plane, xx, tile(ff, sub)]

    def kv_hop(plane, ff, xx, hop):
        target = (dev(f, z, other), dev(ahead, z, x), dev(beside, z, x))[hop]
        ref = kv_of(plane, ff, xx)
        slot = hop + (hop == 2 or xx is other)
        return remote(ref, ref, s_kv.at[plane], r_kv.at[plane, slot], target)

    def kv_first(plane):
        for hop in range(3):
            kv_hop(plane, f, x, hop).start()

    def kv_second(plane):
        kv_wait(plane, f, other, 0)
        for hop in (1, 2):
            kv_hop(plane, f, other, hop).start()
        kv_wait(plane, ahead, x, 1)
        kv_hop(plane, ahead, x, 2).start()

    def kv_third(plane):
        kv_wait(plane, ahead, other, 2)
        kv_hop(plane, ahead, other, 2).start()

    def kv_last(plane):
        ref = kv_all.at[plane, x]
        remote(ref, ref, s_kn, r_kv.at[plane, 3], here).wait_recv()

    def kv_next():
        return remote(
            kv_piece, kv_all.at[0, x, piece_rows],
            s_kn, r_kv.at[0, 4], dev(f, z + 1, x),
        )

    def kv_wait(plane, ff, xx, slot):
        ref = kv_of(plane, ff, xx)
        remote(ref, ref, s_kn, r_kv.at[plane, slot], here).wait_recv()

    kv_first(1)

    @pl.when(z < nz - 1)
    def _():
        kv_next().start()

    @pl.when(is_end)
    def _():
        for c in range(WO_CHUNKS):
            wo_wait(z, other, c)
            wo_z(z, other, c, 1, n).start()

    @pl.when(is_inner)
    def _():
        for c in range(WO_CHUNKS):
            wo_z(z, x, c, 1, m).start()
        wq_wait(m, 1)
        wq_wait(e2, 1)
        q_project(e2, 0)
        e_project(x, 0, e2)
        e_project(x, 1, z)
        e_project(x, 1, e2)

        @pl.when(jnp.logical_not(near))
        def _():
            e_relay(x, 0)

        e_relay(x, 1)
        he_wait(other, 0)
        e_project(other, 0, z)
        e_project(other, 0, e2)
        e_relay(other, 0)

    @pl.when(z > 0)
    def _():
        kv_wait(0, f, x, 4)
        kv_first(0)

    kv_second(1)

    @pl.when(is_inner)
    def _():
        for c in range(WO_CHUNKS):
            wo_pair(c).start()
        for c in range(INNER_CHUNKS):
            wo_cross(z, x, c).start()
        for c in range(WO_CHUNKS):
            wo_wait(e, x, c)
            wo_z(e, x, c, 1, m).start()
            if c < INNER_CHUNKS:
                wo_cross(e, x, c).start()
        e_collect(x, 0)
        he_wait(other, 1)
        e_project(other, 1, z)
        e_project(other, 1, e2)
        e_relay(other, 1)
        q_relay(True)
        for c in range(WO_CHUNKS):
            wo_wait(m, x, c)
            wo_z(m, x, c, 0, e).start()
            if c < INNER_CHUNKS:
                wo_cross(m, x, c).start()
        kv_third(1)

        @pl.when(z > 0)
        def _():
            kv_second(0)

        e_collect(other, 0)
        e_collect(x, 1)
        e_collect(other, 1)
        for c in range(WO_CHUNKS):
            wo_wait(e, other, c)
            wo_z(e, other, c, 1, m).start()
            if c < INNER_CHUNKS:
                wo_cross(e, other, c).start()

        @pl.when(z > 0)
        def _():
            kv_third(0)

        for c in range(WO_CHUNKS):
            wo_wait(e2, x, c)
            wo_z(e2, x, c, 0, e).start()
            if c < INNER_CHUNKS:
                wo_cross(e2, x, c).start()

    def cross(j, xx):
        for c in range(WO_CHUNKS):
            wo_wait(j, xx, c)
            if c < END_CHUNKS:
                wo_cross(j, xx, c).start()

    @pl.when(is_end)
    def _():
        cross(n, x)
        kv_third(1)

        @pl.when(z > 0)
        def _():
            kv_second(0)

        wq_wait(m, 0)
        wq_wait(e2, 0)
        q_project(e2, moved)
        q_relay(True)

        @pl.when(z > 0)
        def _():
            kv_third(0)

        for c in range(WO_CHUNKS):
            wo_swap(c).start()
        cross(m, x)
        remote(q_in, q_in, s_eb, r_eb, here).wait_recv()

    remote(q_far, q_far, s_qf, r_qf, here).wait_recv()
    q_total = q_part[mine] + q_mate[lax.rem(mine, 2)] + q_far[...]
    returned = q_in[...].reshape(rows, HD)
    q_total = q_total + jnp.where(is_end, returned, 0.0)
    q_turned = q_total * q_cos[...] + pltpu.roll(q_total, half, 1) * q_sin[...]
    q_head = q_turned.astype(bf16).astype(f32)
    quarters = []
    for xx in range(nx):
        first = q_head if xx == 0 else pltpu.roll(q_head, HD - xx * quarter, 1)
        second = pltpu.roll(q_head, (HD - half - xx * quarter + quarter) % HD, 1)
        picked = jnp.where(lane < quarter, first, jnp.where(lane < half, second, 0.0))
        quarters.append(picked.astype(bf16))

    seg_ref = seg_buf.at[1, other]
    remote(seg_ref, seg_ref, s_seg.at[0], r_seg.at[1], here).wait_recv()
    kv_last(1)

    @pl.when(z > 0)
    def _():
        before = seg_buf.at[0]
        remote(before, before, s_seg.at[1], r_seg.at[0], here).wait_recv()
        kv_last(0)

    key_seg = jnp.concatenate(
        [seg_buf[plane, xx] for plane in range(2) for xx in range(nx)], axis=1
    )
    own_seg_row = key_seg[:, rows:]
    seg_column = jnp.transpose(jnp.broadcast_to(own_seg_row, (HD, rows)))[:, :1]
    key_pos = lax.broadcasted_iota(jnp.int32, (1, 2 * rows), 1) - rows
    keys = [
        jnp.concatenate([kv_all[0, xx], kv_all[1, xx]], axis=0) for xx in range(nx)
    ]
    head = mine * nx + x
    half_rows = rows // 2

    def mix_of(ff, xx, hf):
        return mix_buf.at[
            hf * half_rows : (hf + 1) * half_rows, tile(block_of(ff) * nx + xx, HD)
        ]

    def mix_send(ff, xx, hop, hf):
        target = (dev(f, z, other), dev(ahead, z, x), dev(beside, z, x))[hop]
        ref = mix_of(ff, xx, hf)
        return remote(
            ref, ref, s_mix, r_mix.at[hf, hop + (hop == 2 or xx is other)], target
        )

    def mix_wait(ref, slot, hf):
        remote(ref, ref, s_mix, r_mix.at[hf, slot], here).wait_recv()

    step_rows = rows // nf
    for b in range(nf):
        span = slice(b * step_rows, (b + 1) * step_rows)
        query_pos = b * step_rows + lax.broadcasted_iota(jnp.int32, (step_rows, 1), 0)
        score = None
        for xx in range(nx):
            term = lax.dot_general(
                quarters[xx][span], keys[xx], (((1,), (1,)), ((), ())),
                preferred_element_type=f32,
            )
            score = term if score is None else score + term
        allowed = (key_pos <= query_pos) & (key_seg == seg_column[span])
        masked = jnp.where(allowed, score * HD ** (-0.5), NEG_FILL)
        row_max = jnp.max(masked, axis=1, keepdims=True)
        weight = jnp.where(allowed, jnp.exp(masked - row_max), 0.0)
        row_total = jnp.sum(weight, axis=1, keepdims=True)
        rounded = weight.astype(bf16)
        product = [
            jnp.dot(rounded, keys[xx], preferred_element_type=f32) for xx in range(nx)
        ]
        mixed = None
        for xx in reversed(range(nx)):
            first = pltpu.roll(product[xx], (half + xx * quarter) % HD, 1)
            second = pltpu.roll(product[xx], (HD - (nx - 1 - xx) * quarter) % HD, 1)
            lane_block = lane // quarter
            value = jnp.where(lane_block < nx, first, second)
            mixed = value if mixed is None else jnp.where(lane_block % nx == xx, value, mixed)
        mix_buf[span, tile(head, HD)] = (mixed / row_total).astype(bf16)
        if b % 2 == 1:
            for hop in range(3):
                mix_send(f, x, hop, b // 2).start()

    @pl.when(is_inner)
    def _():
        for c in range(WO_CHUNKS):
            wo_wait(z, other, c)
            wo_z(z, other, c, 1, m).start()

    def mix_relay(hf):
        mix_wait(mix_of(f, other, hf), 0, hf)
        for hop in (1, 2):
            mix_send(f, other, hop, hf).start()
        mix_wait(mix_of(ahead, x, hf), 1, hf)
        mix_send(ahead, x, 2, hf).start()

    @pl.when(is_end)
    def _():
        cross(e2, x)

    mix_relay(0)
    mix_relay(1)

    @pl.when(is_inner)
    def _():
        for c in range(WO_CHUNKS):
            wo_wait(e2, other, c)
            wo_z(e2, other, c, 0, e).start()
            if c < INNER_CHUNKS:
                wo_cross(e2, other, c).start()

    @pl.when(is_end)
    def _():
        for c in range(WO_CHUNKS):
            wo_wait(n, other, c)
        cross(e2, other)

    for hf in range(2):
        mix_wait(mix_of(ahead, other, hf), 2, hf)
        mix_send(ahead, other, 2, hf).start()

    def result(h, c):
        where = pl.ds(pl.multiple_of(h * half_cols + c * chunk, chunk), chunk)
        return pltpu.make_async_copy(out_buf.at[h, :, cols(c)], out.at[:, where], s_res)

    for hf in range(2):
        mix_wait(mix_buf.at[0:half_rows, 0 : 4 * HD], 3, hf)

    def product(h, c, row_tile):
        return jnp.dot(
            mix_buf[tile(row_tile, tok), :], wo_buf[h, :, cols(c)], preferred_element_type=f32
        ).astype(bf16)

    def away(c):
        return remote(
            out_away.at[c], out_buf.at[x, :, cols(c)], s_out, r_out.at[c], dev(f, z, other)
        )

    def away_stage(c):
        out_away[c] = product(x, c, other)
        away(c).start()

    def own_stage(h, c):
        out_buf[h, :, cols(c)] = product(h, c, x)
        result(h, c).start()

    def away_wait(c):
        ref = out_buf.at[other, :, cols(c)]
        remote(ref, ref, s_out, r_out.at[c], here).wait_recv()
        result(other, c).start()

    def drained(sem, size):
        ruler = wo_buf.at[0, 0 : size // (half_cols * 2), :]
        remote(ruler, ruler, sem, r_hid, here).wait_send()

    def settle(kind):
        inner = kind == "inner"
        unit = HD * chunk * 2
        drained(s_hid, tok * kdim * 2)
        drained(s_wkv.at[1], (2 if inner else 1) * kvw * kdim * 2)
        drained(s_wq.at[1], (2 if inner else 1) * kdim * HD * 2)
        drained(s_wo.at[1], (2 if inner else 1) * nx * WO_CHUNKS * unit)
        drained(s_hx if inner else s_he, 2 * block * moved * 2)
        drained(s_q, 2 * rows * HD * 4)
        drained(s_qf, rows * HD * 4)
        drained(s_kvp, (nf - 1) * sub * nz * kvw * 4)
        drained(s_kv.at[1], (nf * nx - 1) * sub * HD * 2)
        drained(s_mix, (nf * nx - 1) * rows * HD * 2)
        if inner:
            drained(s_wkv.at[0], 3 * kvw * kdim * 2)
            drained(s_wq.at[0], 3 * (kdim - moved) * HD * 2)
            drained(s_wo.at[0], 3 * nx * WO_CHUNKS * unit)
            drained(s_ep, 2 * rows * HD * 4)
            drained(s_ef, rows * HD * 4)
            drained(s_eb, rows * HD * 4)
        seg_same().wait_send()

        @pl.when(z < nz - 1)
        def _():
            before = seg_buf.at[0]
            remote(before, before, s_seg.at[1], r_seg.at[0], here).wait_send()
            kv_next().wait_send()

        @pl.when(z > 0)
        def _():
            drained(s_kv.at[0], (nf * nx - 1) * sub * HD * 2)

    def settle_last(kind):
        inner = kind == "inner"
        unit = HD * chunk * 2
        if inner:
            crossed = (nz * nx - 1) * INNER_CHUNKS
        else:
            crossed = (nz * nx - 2) * END_CHUNKS + WO_CHUNKS
        drained(s_wox, (WO_CHUNKS + crossed) * unit)
        drained(s_out, (WO_CHUNKS - (INNER_CHUNKS if inner else END_CHUNKS)) * tok * chunk * 2)

    order = [*range(END_CHUNKS, WO_CHUNKS), *range(END_CHUNKS)]

    @pl.when(is_inner)
    def _():
        for c in order:
            wo_wait(m, other, c)
            wo_z(m, other, c, 0, e).start()
            if c < INNER_CHUNKS:
                wo_cross(m, other, c).start()
            else:
                away_stage(c)
        for c in order:
            own_stage(x, c)
        settle("inner")
        for c in range(INNER_CHUNKS):
            wox_wait(c, 1)
            own_stage(other, c)
        for c in range(INNER_CHUNKS, WO_CHUNKS):
            away_wait(c)
        settle_last("inner")

    @pl.when(is_end)
    def _():
        for c in order:
            wo_wait(m, other, c)
            if c < END_CHUNKS:
                wo_cross(m, other, c).start()
            if c >= END_CHUNKS:
                away_stage(c)
        for c in order:
            own_stage(x, c)
        settle("end")
        for c in range(END_CHUNKS):
            wox_wait(c, 2)
            own_stage(other, c)
        for c in range(END_CHUNKS, WO_CHUNKS):
            away_wait(c)
        settle_last("end")

    ruler = wo_buf.at[0, 0 : tok * nx, :]
    pltpu.make_async_copy(ruler, ruler, s_res).wait()


def fused_on_device(nf, nz, nx, hidden, w_query, w_keyvalue, w_output, segment_ids):
    tok, kdim = hidden.shape
    cols = w_output.shape[1]
    rows = tok * nx
    sub = rows // nf
    kvw = w_keyvalue.shape[1]
    heads = nz * nx
    part = cols // nx
    f32, bf16 = jnp.float32, jnp.bfloat16
    dma = pltpu.SemaphoreType.DMA
    vmem = pl.BlockSpec(memory_space=pltpu.VMEM)
    anywhere = pl.BlockSpec(memory_space=pl.ANY)
    scratch = [
        pltpu.VMEM((rows, kdim), bf16),
        pltpu.VMEM((nz // 2, kdim, 2 * HD), bf16),
        pltpu.VMEM((nz * kvw, kdim), bf16),
        pltpu.VMEM((nx, heads * HD, part), bf16),
        pltpu.VMEM((2, nx, 1, tok), jnp.int32),
        pltpu.VMEM((nz, rows, HD), f32),
        pltpu.VMEM((nf // 2, rows, HD), f32),
        pltpu.VMEM((rows, HD), f32),
        pltpu.VMEM((rows, HD), f32),
        pltpu.VMEM((rows, nz * kvw), f32),
        pltpu.VMEM((nf, sub, nz * kvw), f32),
        pltpu.VMEM((sub, HD), bf16),
        pltpu.VMEM((2, nx, rows, HD), bf16),
        pltpu.VMEM((rows, heads * HD), bf16),
        pltpu.VMEM((rows, HD), f32),
        pltpu.VMEM((rows, HD), f32),
        pltpu.VMEM((nx, tok, part), bf16),
        pltpu.VMEM((WO_CHUNKS, tok, part // WO_CHUNKS), bf16),
        pltpu.VMEM((nx, 2, tok // 2, kdim * MOVED // 8), bf16),
        pltpu.VMEM((nz, nx, 2, tok // 2, HD), f32),
        pltpu.VMEM((nf // 2, nx, 2, tok // 2, HD), f32),
        pltpu.VMEM((nx, 2, tok // 2, HD), f32),
        pltpu.VMEM((nx, 2, tok // 2, HD), f32),
        pltpu.VMEM((nx, 2, tok // 2, HD), f32),
        pltpu.VMEM((nx, 2, tok // 2, HD), f32),
        dma((6,)), dma, dma, dma((2,)), dma((2,)), dma((2,)), dma((nz,)), dma((2,)), dma((nz, 2)),
        dma, dma, dma, dma, dma, dma, dma((2,)), dma((2, 5)), dma,
        dma((2,)), dma((nz, nx, WO_CHUNKS)), dma((WO_CHUNKS,)), dma, dma((WO_CHUNKS,)), dma,
        dma((2, 4)),
        dma, dma((WO_CHUNKS,)), dma, dma, dma((nx, 2)), dma,
        dma, dma((nx, 2)), dma, dma((nx, 2)), dma, dma,
    ]
    return pl.pallas_call(
        functools.partial(fused_kernel, nf, nz, nx),
        out_shape=jax.ShapeDtypeStruct((tok, cols), bf16),
        in_specs=[anywhere] * 4 + [vmem],
        out_specs=anywhere,
        scratch_shapes=scratch,
        name="fused_sublayer",
        compiler_params=pltpu.CompilerParams(
            collective_id=0, has_side_effects=True, vmem_limit_bytes=60 * 1024 * 1024
        ),
    )(hidden, w_query, w_keyvalue.T, w_output, segment_ids.reshape(1, tok))


def solution(mesh):
    in_specs = (P("sp", "fsdp"), P("fsdp", "sp"), P("fsdp", "sp"), P("sp", "fsdp"), P("sp"))
    out_specs = P("sp", "fsdp")
    nf, sp = mesh.shape["fsdp"], mesh.shape["sp"]
    if sp == GROUP and sp == 2 * nf:
        body = functools.partial(fused_on_device, nf, nf, sp // nf)
    else:
        body = on_device
    return jax.shard_map(
        body, mesh=mesh, in_specs=in_specs, out_specs=out_specs, check_vma=False
    )
```

```python
import functools
import math

import jax
import jax.numpy as jnp
from jax import lax
from jax.experimental import pallas as pl
from jax.experimental.pallas import tpu as pltpu
from jax.sharding import PartitionSpec as P

HD = 128
GROUP = 8


ROPE_BASE = 500000.0
NEG_FILL = -1e30


def rotate(values, positions, head_count, width):
    row_count = values.shape[0]
    shaped = values.reshape(row_count, head_count, width)
    half_width = width // 2
    frequency = jnp.exp(
        jnp.arange(half_width, dtype=jnp.float32) * (-2.0 * math.log(ROPE_BASE) / width)
    )
    angles = positions.astype(jnp.float32)[:, None] * frequency[None, :]
    cosine = jnp.cos(angles)[:, None, :]
    sine_part = jnp.sin(angles)[:, None, :]
    lower_half = shaped[:, :, :half_width]
    upper_half = shaped[:, :, half_width:]
    turned = jnp.concatenate(
        [
            lower_half * cosine - upper_half * sine_part,
            upper_half * cosine + lower_half * sine_part,
        ],
        axis=2,
    )
    return turned.reshape(row_count, head_count * width)


def split_keys(kv_sum, positions, kv_count, width):
    row_count = kv_sum.shape[0]
    shaped = kv_sum.reshape(row_count, kv_count, 2, width)
    key_part = rotate(
        shaped[:, :, 0, :].reshape(row_count, kv_count * width), positions, kv_count, width
    )
    key_part = key_part.reshape(row_count, kv_count, 1, width)
    return jnp.concatenate([key_part, shaped[:, :, 1:2, :]], axis=2).astype(jnp.bfloat16)


def merge_keys(
    state_in, query_tile, query_pos_tile, query_seg_tile, key_tile, key_pos_tile, key_seg_tile
):
    running_max, running_sum, weighted = state_in
    allowed = (key_pos_tile[None, :] <= query_pos_tile[:, None]) & (
        key_seg_tile[None, :] == query_seg_tile[:, None]
    )
    key_part = key_tile[:, :HD]
    value_part = key_tile[:, HD:]
    scores = lax.dot_general(
        query_tile, key_part, (((1,), (1,)), ((), ())), preferred_element_type=jnp.float32
    ) * HD ** (-0.5)
    masked = jnp.where(allowed, scores, NEG_FILL)
    new_max = jnp.maximum(running_max, jnp.max(masked, axis=1))
    weights = jnp.where(allowed, jnp.exp(masked - new_max[:, None]), 0.0)
    new_sum = jnp.sum(weights, axis=1)
    new_weighted = jnp.dot(
        weights.astype(jnp.bfloat16), value_part, preferred_element_type=jnp.float32
    )
    return (new_max, new_sum, new_weighted)


def on_device(hidden, w_query, w_keyvalue, w_output, segment_ids):
    fsdp_count = lax.axis_size("fsdp")
    seq_count = lax.axis_size("sp")
    fsdp_index = lax.axis_index("fsdp")
    seq_index = lax.axis_index("sp")
    tok_rows = hidden.shape[0]
    sub_rows = tok_rows // fsdp_count
    kv_count = seq_count // GROUP
    query_rows = seq_count * sub_rows
    offsets = jnp.arange(query_rows, dtype=jnp.int32)
    query_pos = offsets // sub_rows * tok_rows + fsdp_index * sub_rows + offsets % sub_rows
    own_positions = (
        seq_index * tok_rows + fsdp_index * sub_rows + jnp.arange(sub_rows, dtype=jnp.int32)
    )

    def project(weight_block):
        return jnp.dot(hidden, weight_block, preferred_element_type=jnp.float32)

    query_part = project(lax.all_gather(w_query, "sp", axis=1, tiled=True))
    kv_part = project(lax.all_gather(w_keyvalue, "sp", axis=1, tiled=True))
    query_sum, kv_sum = (
        lax.psum_scatter(query_part, "fsdp", scatter_dimension=0, tiled=True),
        lax.psum_scatter(kv_part, "fsdp", scatter_dimension=0, tiled=True),
    )
    query_local = rotate(query_sum, own_positions, seq_count, HD).astype(jnp.bfloat16)
    pairs = split_keys(kv_sum, own_positions, kv_count, HD)
    expanded = jnp.repeat(pairs, GROUP, axis=1).reshape(sub_rows, seq_count * 2 * HD)
    query_head, kv_head = (
        lax.all_to_all(query_local, "sp", split_axis=1, concat_axis=0, tiled=True),
        lax.all_to_all(expanded, "sp", split_axis=1, concat_axis=0, tiled=True),
    )
    segment_all = lax.all_gather(segment_ids, "sp", axis=0, tiled=True)
    query_seg = segment_all[query_pos]
    initial = (
        jnp.full((query_rows,), NEG_FILL, jnp.float32),
        jnp.zeros((query_rows,), jnp.float32),
        jnp.zeros((query_rows, HD), jnp.float32),
    )
    block_keys = lax.all_gather(kv_head, "fsdp", axis=0, tiled=True)
    piece_rows = block_keys.shape[0]
    row_ids = jnp.arange(piece_rows, dtype=jnp.int32)
    source_id = row_ids // query_rows
    within = row_ids % query_rows
    key_pos = within // sub_rows * tok_rows + source_id * sub_rows + within % sub_rows
    key_seg = segment_all[key_pos]
    final_max, final_sum, final_weighted = merge_keys(
        initial, query_head, query_pos, query_seg, block_keys, key_pos, key_seg
    )
    attention = (final_weighted / final_sum[:, None]).astype(jnp.bfloat16)
    back_rows = lax.all_to_all(attention, "sp", split_axis=0, concat_axis=1, tiled=True)
    mixed_rows = lax.all_gather(back_rows, "fsdp", axis=0, tiled=True)
    result = jnp.dot(
        mixed_rows,
        lax.all_gather(w_output, "sp", axis=0, tiled=True),
        preferred_element_type=jnp.float32,
    )
    return result.astype(jnp.bfloat16)


NEG_POS = -1
WO_CHUNKS = 4
MOVED = 4
END_CHUNKS = 3
INNER_CHUNKS = 1


def fused_kernel(
    nf, nz, nx, hid, wq, wkv, wo, seg, out,
    h_buf, wq_buf, wkv_buf, wo_buf, seg_buf,
    q_part, q_mate, q_sum, q_far, kv_part, kv_recv, kv_piece, kv_all, mix_buf, q_cos, q_sin,
    out_buf, out_away, h_end, e_part, e_mate, e_sum, e_far, e_back, q_in,
    s_loc, s_hid, r_hid, s_seg, r_seg, s_wkv, r_wkv, s_wq, r_wq,
    s_q, r_q, s_qf, r_qf, s_kvp, r_kvp, s_kv, r_kv, s_kn, s_wo, r_wo, r_rest, s_wox, r_wox, s_mix, r_mix,
    s_out, r_out, s_res, s_he, r_he, s_hx, s_ep, r_ep, s_ef, r_ef, s_eb, r_eb,
):
    f = lax.axis_index("fsdp")
    s = lax.axis_index("sp")
    z, x = s // nx, s % nx
    tok, kdim = hid.shape
    rows = tok * nx
    sub = rows // nf
    kvw = wkv.shape[0]
    other = 1 - x
    moved = kdim * MOVED // 8
    block = tok // 2
    half_cols = wo.shape[1] // nx
    chunk = half_cols // WO_CHUNKS
    f32, bf16 = jnp.float32, jnp.bfloat16
    is_end = (z == 0) | (z == nz - 1)
    is_inner = jnp.logical_not(is_end)
    low = z < nz // 2
    e = jnp.where(low, 0, nz - 1)
    n = jnp.where(low, 1, nz - 2)
    m = nz - 1 - n
    e2 = nz - 1 - e
    beside = f + 1 - 2 * lax.rem(f, 2)
    ahead = lax.rem(f + 2, nf)
    across = lax.rem(beside + 2, nf)

    def block_of(ff):
        return lax.rem(ff, 2) * 2 + ff // 2

    core = lax.rem(f, 2)
    mine, theirs = block_of(f), block_of(ahead)
    near = core == z // 2

    def dev(ff, zz, xx):
        return (ff, zz * nx + xx)

    def remote(src, dst, ss, rs, target):
        return pltpu.make_async_remote_copy(
            src_ref=src, dst_ref=dst, send_sem=ss, recv_sem=rs,
            device_id=target, device_id_type=pl.DeviceIdType.MESH,
        )

    def tile(ref, count):
        return pl.ds(pl.multiple_of(ref * count, count), count)

    here = (f, s)
    def cols(c):
        return slice(c * chunk, (c + 1) * chunk)

    own_h = pltpu.make_async_copy(hid, h_buf.at[tile(x, tok)], s_loc.at[0])
    own_wq = pltpu.make_async_copy(
        wq, wq_buf.at[z // 2, :, tile(lax.rem(z, 2), HD)], s_loc.at[1]
    )
    own_wkv = pltpu.make_async_copy(wkv, wkv_buf.at[tile(z, kvw)], s_loc.at[2])
    own_wo = [
        pltpu.make_async_copy(
            wo.at[:, h * half_cols : (h + 1) * half_cols],
            wo_buf.at[h, tile(s, HD)], s_loc.at[3 + h],
        )
        for h in range(nx)
    ]
    own_seg = pltpu.make_async_copy(seg, seg_buf.at[1, x], s_loc.at[5])
    for copy in (own_wkv, own_wq, own_h, *own_wo, own_seg):
        copy.start()

    def hid_send():
        return remote(
            h_buf.at[tile(x, tok)], h_buf.at[tile(x, tok)], s_hid, r_hid, dev(f, z, other)
        )

    def hid_wait():
        remote(
            h_buf.at[tile(other, tok)], h_buf.at[tile(other, tok)], s_hid, r_hid, here
        ).wait_recv()

    def wkv_z(j, d, target):
        ref = wkv_buf.at[tile(j, kvw)]
        return remote(ref, ref, s_wkv.at[d], r_wkv.at[j], dev(f, target, x))

    def wkv_wait(j):
        wkv_z(j, 0, z).wait_recv()

    def wq_z(j, part, d, target):
        features = slice(moved, kdim) if part == 0 else slice(0, moved)
        ref = wq_buf.at[j // 2, features, tile(lax.rem(j, 2), HD)]
        return remote(ref, ref, s_wq.at[d], r_wq.at[j, part], dev(f, target, x))

    def wq_wait(j, part):
        wq_z(j, part, 1, z).wait_recv()

    def he_z(hf):
        rows_of = pl.ds(pl.multiple_of(x * tok + hf * block, block), block)
        return remote(
            h_buf.at[rows_of, 0:moved], h_end.at[x, hf], s_he, r_he.at[x, hf], dev(f, n, x)
        )

    def he_x(hf):
        ref = h_end.at[x, hf]
        return remote(ref, ref, s_hx, r_he.at[x, hf], dev(f, z, other))

    def he_wait(xx, hf):
        ref = h_end.at[xx, hf]
        remote(ref, ref, s_hx, r_he.at[xx, hf], here).wait_recv()

    def wo_unit(h, j, xx, c):
        return wo_buf.at[h, tile(j * nx + xx, HD), cols(c)]

    def wo_z(j, xx, c, d, target):
        ref = wo_unit(x, j, xx, c)
        return remote(ref, ref, s_wo.at[d], r_wo.at[j, xx, c], dev(f, target, x))

    def wo_pair(c):
        ref = wo_unit(other, z, x, c)
        return remote(ref, ref, s_wox, r_wo.at[z, x, c], dev(f, z, other))

    def wo_wait(j, xx, c):
        ref = wo_unit(x, j, xx, c)
        remote(ref, ref, s_wox, r_wo.at[j, xx, c], here).wait_recv()

    def wo_cross(j, xx, c):
        ref = wo_unit(x, j, xx, c)
        return remote(ref, ref, s_wox, r_wox.at[c], dev(f, z, other))

    def wo_rest(c):
        ref = wo_unit(other, n, x, c)
        return remote(ref, ref, s_wo.at[0], r_rest.at[c], dev(f, e, x))

    def wo_swap(c):
        ref = wo_unit(other, n, x, c)
        remote(ref, ref, s_wox, r_rest.at[c], here).wait_recv()
        return remote(ref, ref, s_wox, r_wo.at[n, x, c], dev(f, z, other))

    def wox_wait(c, held):
        ref = wo_buf.at[other, held * HD :, cols(c)]
        remote(ref, ref, s_wox, r_wox.at[c], here).wait_recv()

    def seg_same():
        return remote(seg_buf.at[1, x], seg_buf.at[1, x], s_seg.at[0], r_seg.at[1], dev(f, z, other))

    def seg_next(xx):
        return remote(
            seg_buf.at[1, x], seg_buf.at[0, x], s_seg.at[1], r_seg.at[0], dev(f, z + 1, xx)
        )

    barrier = pltpu.get_barrier_semaphore()

    def greet(ff, zz, xx):
        pl.semaphore_signal(
            barrier, inc=1, device_id=dev(ff, zz, xx), device_id_type=pl.DeviceIdType.MESH
        )

    plane = nf * nx
    for step in (1, -1):
        @pl.when((z + step >= 0) & (z + step < nz))
        def _():
            for xx in range(nx):
                greet(f, z + step, xx)

    for d in range(1, plane):
        greet(lax.rem(f + d, nf), z, lax.rem(x + d // nf, nx))
    pl.semaphore_wait(barrier, plane - 1 + jnp.where(is_end, nx, 2 * nx))

    own_wkv.wait()
    own_wq.wait()

    @pl.when(is_end)
    def _():
        wkv_z(z, 1, n).start()
        wq_z(z, 0, 1, n).start()
        wq_z(z, 1, 1, n).start()

    @pl.when(is_inner)
    def _():
        for d, target in ((0, e), (1, m)):
            wkv_z(z, d, target).start()
            wq_z(z, 0, d, target).start()
        wq_z(z, 1, 1, m).start()

    own_h.wait()
    hid_send().start()
    own_seg.wait()
    seg_same().start()

    @pl.when(z < nz - 1)
    def _():
        for xx in range(nx):
            seg_next(xx).start()

    for copy in own_wo:
        copy.wait()

    @pl.when(is_end)
    def _():
        for hf in range(2):
            he_z(hf).start()
        for c in range(WO_CHUNKS):
            wo_z(z, x, c, 1, n).start()
        for c in range(WO_CHUNKS):
            wo_pair(c).start()
        for c in range(END_CHUNKS):
            wo_cross(z, x, c).start()

    @pl.when(is_inner)
    def _():
        for c in range(WO_CHUNKS):
            wo_z(z, x, c, 0, e).start()

    @pl.when(z == 0)
    def _():
        kv_all[0] = jnp.zeros(kv_all.shape[1:], bf16)
        seg_buf[0] = jnp.full(seg_buf.shape[1:], NEG_POS, jnp.int32)

    @pl.when(is_inner)
    def _():
        q_in[...] = jnp.zeros(q_in.shape, f32)

    def table(row_count, first, lane_index):
        position = (first + lax.broadcasted_iota(jnp.int32, (row_count, HD), 0)).astype(f32)
        frequency = jnp.exp(lane_index.astype(f32) * (-2.0 * math.log(ROPE_BASE) / HD))
        return position * frequency

    lane = lax.broadcasted_iota(jnp.int32, (1, HD), 1)
    half = HD // 2
    quarter = half // nx
    kv_angle = table(sub, z * rows + f * sub, x * quarter + lane % quarter)
    is_key = lane < half
    kv_cos = jnp.where(is_key, jnp.cos(kv_angle), 1.0)
    kv_sin = jnp.where(is_key, jnp.sin(kv_angle), 0.0)
    kv_sin = jnp.where(lane < quarter, -kv_sin, kv_sin)
    q_angle = table(rows, z * rows, lane % half)
    q_sine = jnp.sin(q_angle)
    q_cos[...] = jnp.cos(q_angle)
    q_sin[...] = jnp.where(lane < half, -q_sine, q_sine)

    same_core = lambda j: j // 2 == core

    def q_send(j):
        return remote(
            q_part.at[j], q_mate.at[lax.rem(j, 2)], s_q, r_q, dev(beside, z, x)
        )

    def q_far_copy():
        return remote(q_sum, q_far, s_qf, r_qf, dev(ahead, z, x))

    def q_project(j, first):
        both = jnp.dot(
            h_buf[:, first:], wq_buf[j // 2, first:, :], preferred_element_type=f32
        )
        for b in range(2):
            q_part[j // 2 * 2 + b] = both[:, b * HD : (b + 1) * HD]

        @pl.when(jnp.logical_not(same_core(j)))
        def _():
            for b in range(2):
                q_send(j // 2 * 2 + b).start()

    def q_relay(far):
        @pl.when(jnp.logical_not(near) if far else near)
        def _():
            remote(q_mate, q_mate, s_q, r_q, here).wait_recv()
            q_sum[...] = q_part[theirs] + q_mate[lax.rem(theirs, 2)]
            q_far_copy().start()

    def e_send(j, xx, hf):
        return remote(
            e_part.at[j, xx, hf], e_mate.at[lax.rem(j, 2), xx, hf],
            s_ep, r_ep.at[xx, hf], dev(beside, z, x)
        )

    def e_far_copy(xx, hf):
        return remote(
            e_sum.at[xx, hf], e_far.at[xx, hf], s_ef, r_ef.at[xx, hf], dev(ahead, z, x)
        )

    def e_project(xx, hf, j):
        both = jnp.dot(
            h_end[xx, hf], wq_buf[j // 2, 0:moved, :], preferred_element_type=f32
        )
        for b in range(2):
            e_part[j // 2 * 2 + b, xx, hf] = both[:, b * HD : (b + 1) * HD]

        @pl.when(jnp.logical_not(same_core(j)))
        def _():
            for b in range(2):
                e_send(j // 2 * 2 + b, xx, hf).start()

    def e_relay(xx, hf):
        ref = e_mate.at[:, xx, hf]
        remote(ref, ref, s_ep, r_ep.at[xx, hf], here).wait_recv()
        e_sum[xx, hf] = e_part[theirs, xx, hf] + e_mate[lax.rem(theirs, 2), xx, hf]
        e_far_copy(xx, hf).start()

    def e_return(xx, hf):
        return remote(
            e_back.at[xx, hf], q_in.at[xx, hf], s_eb, r_eb, dev(f, e, x)
        )

    def e_collect(xx, hf):
        ref = e_far.at[xx, hf]
        remote(ref, ref, s_ef, r_ef.at[xx, hf], here).wait_recv()
        e_back[xx, hf] = (
            e_part[mine, xx, hf] + e_mate[lax.rem(mine, 2), xx, hf] + e_far[xx, hf]
        )
        e_return(xx, hf).start()

    @pl.when(is_inner)
    def _():
        wkv_wait(e)
        wkv_z(e, 1, m).start()
        wkv_wait(m)
        wkv_z(m, 0, e).start()
        wq_wait(e, 0)
        wq_z(e, 0, 1, m).start()
        wq_wait(m, 0)
        wq_z(m, 0, 0, e).start()
        wq_wait(e, 1)
        wq_z(e, 1, 1, m).start()
        wkv_wait(e2)
        wkv_z(e2, 0, e).start()
        he_wait(x, 0)
        he_x(0).start()
        wq_wait(e2, 0)
        wq_z(e2, 0, 0, e).start()
        for c in range(WO_CHUNKS):
            wo_rest(c).start()

    hid_wait()

    @pl.when(is_end)
    def _():
        for j in (n, m, e2):
            wkv_wait(j)

    kv_part[...] = lax.dot_general(
        h_buf[...], wkv_buf[...], (((1,), (1,)), ((), ())), preferred_element_type=f32
    )

    def kvp_send(d):
        ff = lax.rem(f + d, nf)
        return remote(
            kv_part.at[tile(ff, sub)], kv_recv.at[f], s_kvp, r_kvp, (ff, s)
        )

    for d in range(1, nf):
        kvp_send(d).start()

    @pl.when(is_inner)
    def _():
        q_project(z, 0)
        he_wait(x, 1)
        he_x(1).start()
        q_relay(False)
        e_project(x, 0, z)

        @pl.when(near)
        def _():
            e_relay(x, 0)


    @pl.when(is_end)
    def _():
        wq_wait(n, 0)
        q_project(z, moved)
        q_relay(False)

    total = kv_part[tile(f, sub), :]
    arrived = kv_recv.at[1:nf]
    remote(arrived, arrived, s_kvp, r_kvp, here).wait_recv()
    for d in range(1, nf):
        total = total + kv_recv[lax.rem(f + d, nf)]
    partner = jnp.where(
        lane < quarter, pltpu.roll(total, HD - quarter, 1), pltpu.roll(total, quarter, 1)
    )
    kv_piece[...] = (total * kv_cos + partner * kv_sin).astype(bf16)
    piece_rows = tile(f, sub)
    kv_all[1, x, piece_rows] = kv_piece[...]

    def kv_of(plane, ff, xx):
        return kv_all.at[plane, xx, tile(ff, sub)]

    def kv_hop(plane, ff, xx, hop):
        target = (dev(f, z, other), dev(ahead, z, x), dev(beside, z, x))[hop]
        ref = kv_of(plane, ff, xx)
        slot = hop + (hop == 2 or xx is other)
        return remote(ref, ref, s_kv.at[plane], r_kv.at[plane, slot], target)

    def kv_first(plane):
        for hop in range(3):
            kv_hop(plane, f, x, hop).start()

    def kv_second(plane):
        kv_wait(plane, f, other, 0)
        for hop in (1, 2):
            kv_hop(plane, f, other, hop).start()
        kv_wait(plane, ahead, x, 1)
        kv_hop(plane, ahead, x, 2).start()

    def kv_third(plane):
        kv_wait(plane, ahead, other, 2)
        kv_hop(plane, ahead, other, 2).start()

    def kv_last(plane):
        ref = kv_all.at[plane, x]
        remote(ref, ref, s_kn, r_kv.at[plane, 3], here).wait_recv()

    def kv_next():
        return remote(
            kv_piece, kv_all.at[0, x, piece_rows],
            s_kn, r_kv.at[0, 4], dev(f, z + 1, x),
        )

    def kv_wait(plane, ff, xx, slot):
        ref = kv_of(plane, ff, xx)
        remote(ref, ref, s_kn, r_kv.at[plane, slot], here).wait_recv()

    kv_first(1)

    @pl.when(z < nz - 1)
    def _():
        kv_next().start()

    @pl.when(is_end)
    def _():
        for c in range(WO_CHUNKS):
            wo_wait(z, other, c)
            wo_z(z, other, c, 1, n).start()

    @pl.when(is_inner)
    def _():
        for c in range(WO_CHUNKS):
            wo_z(z, x, c, 1, m).start()
        wq_wait(m, 1)
        wq_wait(e2, 1)
        q_project(e2, 0)
        e_project(x, 0, e2)
        e_project(x, 1, z)
        e_project(x, 1, e2)

        @pl.when(jnp.logical_not(near))
        def _():
            e_relay(x, 0)

        e_relay(x, 1)
        he_wait(other, 0)
        e_project(other, 0, z)
        e_project(other, 0, e2)
        e_relay(other, 0)

    @pl.when(z > 0)
    def _():
        kv_wait(0, f, x, 4)
        kv_first(0)

    kv_second(1)

    @pl.when(is_inner)
    def _():
        for c in range(WO_CHUNKS):
            wo_pair(c).start()
        for c in range(INNER_CHUNKS):
            wo_cross(z, x, c).start()
        for c in range(WO_CHUNKS):
            wo_wait(e, x, c)
            wo_z(e, x, c, 1, m).start()
            if c < INNER_CHUNKS:
                wo_cross(e, x, c).start()
        e_collect(x, 0)
        he_wait(other, 1)
        e_project(other, 1, z)
        e_project(other, 1, e2)
        e_relay(other, 1)
        q_relay(True)
        for c in range(WO_CHUNKS):
            wo_wait(m, x, c)
            wo_z(m, x, c, 0, e).start()
            if c < INNER_CHUNKS:
                wo_cross(m, x, c).start()
        kv_third(1)

        @pl.when(z > 0)
        def _():
            kv_second(0)

        e_collect(other, 0)
        e_collect(x, 1)
        e_collect(other, 1)
        for c in range(WO_CHUNKS):
            wo_wait(e, other, c)
            wo_z(e, other, c, 1, m).start()
            if c < INNER_CHUNKS:
                wo_cross(e, other, c).start()

        @pl.when(z > 0)
        def _():
            kv_third(0)

        for c in range(WO_CHUNKS):
            wo_wait(e2, x, c)
            wo_z(e2, x, c, 0, e).start()
            if c < INNER_CHUNKS:
                wo_cross(e2, x, c).start()

    def cross(j, xx):
        for c in range(WO_CHUNKS):
            wo_wait(j, xx, c)
            if c < END_CHUNKS:
                wo_cross(j, xx, c).start()

    @pl.when(is_end)
    def _():
        cross(n, x)
        kv_third(1)

        @pl.when(z > 0)
        def _():
            kv_second(0)

        wq_wait(m, 0)
        wq_wait(e2, 0)
        q_project(e2, moved)
        q_relay(True)

        @pl.when(z > 0)
        def _():
            kv_third(0)

        for c in range(WO_CHUNKS):
            wo_swap(c).start()
        cross(m, x)
        remote(q_in, q_in, s_eb, r_eb, here).wait_recv()

    remote(q_far, q_far, s_qf, r_qf, here).wait_recv()
    q_total = q_part[mine] + q_mate[lax.rem(mine, 2)] + q_far[...]
    returned = q_in[...].reshape(rows, HD)
    q_total = q_total + jnp.where(is_end, returned, 0.0)
    q_turned = q_total * q_cos[...] + pltpu.roll(q_total, half, 1) * q_sin[...]
    q_head = q_turned.astype(bf16).astype(f32)
    quarters = []
    for xx in range(nx):
        first = q_head if xx == 0 else pltpu.roll(q_head, HD - xx * quarter, 1)
        second = pltpu.roll(q_head, (HD - half - xx * quarter + quarter) % HD, 1)
        picked = jnp.where(lane < quarter, first, jnp.where(lane < half, second, 0.0))
        quarters.append(picked.astype(bf16))

    seg_ref = seg_buf.at[1, other]
    remote(seg_ref, seg_ref, s_seg.at[0], r_seg.at[1], here).wait_recv()
    kv_last(1)

    @pl.when(z > 0)
    def _():
        before = seg_buf.at[0]
        remote(before, before, s_seg.at[1], r_seg.at[0], here).wait_recv()
        kv_last(0)

    key_seg = jnp.concatenate(
        [seg_buf[plane, xx] for plane in range(2) for xx in range(nx)], axis=1
    )
    own_seg_row = key_seg[:, rows:]
    seg_column = jnp.transpose(jnp.broadcast_to(own_seg_row, (HD, rows)))[:, :1]
    key_pos = lax.broadcasted_iota(jnp.int32, (1, 2 * rows), 1) - rows
    keys = [
        jnp.concatenate([kv_all[0, xx], kv_all[1, xx]], axis=0) for xx in range(nx)
    ]
    head = mine * nx + x
    half_rows = rows // 2

    def mix_of(ff, xx, hf):
        return mix_buf.at[
            hf * half_rows : (hf + 1) * half_rows, tile(block_of(ff) * nx + xx, HD)
        ]

    def mix_send(ff, xx, hop, hf):
        target = (dev(f, z, other), dev(ahead, z, x), dev(beside, z, x))[hop]
        ref = mix_of(ff, xx, hf)
        return remote(
            ref, ref, s_mix, r_mix.at[hf, hop + (hop == 2 or xx is other)], target
        )

    def mix_wait(ref, slot, hf):
        remote(ref, ref, s_mix, r_mix.at[hf, slot], here).wait_recv()

    step_rows = rows // nf
    for b in range(nf):
        span = slice(b * step_rows, (b + 1) * step_rows)
        query_pos = b * step_rows + lax.broadcasted_iota(jnp.int32, (step_rows, 1), 0)
        score = None
        for xx in range(nx):
            term = lax.dot_general(
                quarters[xx][span], keys[xx], (((1,), (1,)), ((), ())),
                preferred_element_type=f32,
            )
            score = term if score is None else score + term
        allowed = (key_pos <= query_pos) & (key_seg == seg_column[span])
        masked = jnp.where(allowed, score * HD ** (-0.5), NEG_FILL)
        row_max = jnp.max(masked, axis=1, keepdims=True)
        weight = jnp.where(allowed, jnp.exp(masked - row_max), 0.0)
        row_total = jnp.sum(weight, axis=1, keepdims=True)
        rounded = weight.astype(bf16)
        product = [
            jnp.dot(rounded, keys[xx], preferred_element_type=f32) for xx in range(nx)
        ]
        mixed = None
        for xx in reversed(range(nx)):
            first = pltpu.roll(product[xx], (half + xx * quarter) % HD, 1)
            second = pltpu.roll(product[xx], (HD - (nx - 1 - xx) * quarter) % HD, 1)
            lane_block = lane // quarter
            value = jnp.where(lane_block < nx, first, second)
            mixed = value if mixed is None else jnp.where(lane_block % nx == xx, value, mixed)
        mix_buf[span, tile(head, HD)] = (mixed / row_total).astype(bf16)
        if b % 2 == 1:
            for hop in range(3):
                mix_send(f, x, hop, b // 2).start()

    @pl.when(is_inner)
    def _():
        for c in range(WO_CHUNKS):
            wo_wait(z, other, c)
            wo_z(z, other, c, 1, m).start()

    def mix_relay(hf):
        mix_wait(mix_of(f, other, hf), 0, hf)
        for hop in (1, 2):
            mix_send(f, other, hop, hf).start()
        mix_wait(mix_of(ahead, x, hf), 1, hf)
        mix_send(ahead, x, 2, hf).start()

    @pl.when(is_end)
    def _():
        cross(e2, x)

    mix_relay(0)
    mix_relay(1)

    @pl.when(is_inner)
    def _():
        for c in range(WO_CHUNKS):
            wo_wait(e2, other, c)
            wo_z(e2, other, c, 0, e).start()
            if c < INNER_CHUNKS:
                wo_cross(e2, other, c).start()

    @pl.when(is_end)
    def _():
        for c in range(WO_CHUNKS):
            wo_wait(n, other, c)
        cross(e2, other)

    for hf in range(2):
        mix_wait(mix_of(ahead, other, hf), 2, hf)
        mix_send(ahead, other, 2, hf).start()

    def result(h, c):
        where = pl.ds(pl.multiple_of(h * half_cols + c * chunk, chunk), chunk)
        return pltpu.make_async_copy(out_buf.at[h, :, cols(c)], out.at[:, where], s_res)

    for hf in range(2):
        mix_wait(mix_buf.at[0:half_rows, 0 : 4 * HD], 3, hf)

    def product(h, c, row_tile):
        return jnp.dot(
            mix_buf[tile(row_tile, tok), :], wo_buf[h, :, cols(c)], preferred_element_type=f32
        ).astype(bf16)

    def away(c):
        return remote(
            out_away.at[c], out_buf.at[x, :, cols(c)], s_out, r_out.at[c], dev(f, z, other)
        )

    def away_stage(c):
        out_away[c] = product(x, c, other)
        away(c).start()

    def own_stage(h, c):
        out_buf[h, :, cols(c)] = product(h, c, x)
        result(h, c).start()

    def away_wait(c):
        ref = out_buf.at[other, :, cols(c)]
        remote(ref, ref, s_out, r_out.at[c], here).wait_recv()
        result(other, c).start()

    def drained(sem, size):
        ruler = wo_buf.at[0, 0 : size // (half_cols * 2), :]
        remote(ruler, ruler, sem, r_hid, here).wait_send()

    def settle(kind):
        inner = kind == "inner"
        unit = HD * chunk * 2
        drained(s_hid, tok * kdim * 2)
        drained(s_wkv.at[1], (2 if inner else 1) * kvw * kdim * 2)
        drained(s_wq.at[1], (2 if inner else 1) * kdim * HD * 2)
        drained(s_wo.at[1], (2 if inner else 1) * nx * WO_CHUNKS * unit)
        drained(s_hx if inner else s_he, 2 * block * moved * 2)
        drained(s_q, 2 * rows * HD * 4)
        drained(s_qf, rows * HD * 4)
        drained(s_kvp, (nf - 1) * sub * nz * kvw * 4)
        drained(s_kv.at[1], (nf * nx - 1) * sub * HD * 2)
        drained(s_mix, (nf * nx - 1) * rows * HD * 2)
        if inner:
            drained(s_wkv.at[0], 3 * kvw * kdim * 2)
            drained(s_wq.at[0], 3 * (kdim - moved) * HD * 2)
            drained(s_wo.at[0], 3 * nx * WO_CHUNKS * unit)
            drained(s_ep, 2 * rows * HD * 4)
            drained(s_ef, rows * HD * 4)
            drained(s_eb, rows * HD * 4)
        seg_same().wait_send()

        @pl.when(z < nz - 1)
        def _():
            before = seg_buf.at[0]
            remote(before, before, s_seg.at[1], r_seg.at[0], here).wait_send()
            kv_next().wait_send()

        @pl.when(z > 0)
        def _():
            drained(s_kv.at[0], (nf * nx - 1) * sub * HD * 2)

    def settle_last(kind):
        inner = kind == "inner"
        unit = HD * chunk * 2
        if inner:
            crossed = (nz * nx - 1) * INNER_CHUNKS
        else:
            crossed = (nz * nx - 2) * END_CHUNKS + WO_CHUNKS
        drained(s_wox, (WO_CHUNKS + crossed) * unit)
        drained(s_out, (WO_CHUNKS - (INNER_CHUNKS if inner else END_CHUNKS)) * tok * chunk * 2)

    order = [*range(WO_CHUNKS)]

    @pl.when(is_inner)
    def _():
        for c in order:
            wo_wait(m, other, c)
            wo_z(m, other, c, 0, e).start()
            if c < INNER_CHUNKS:
                wo_cross(m, other, c).start()
            else:
                away_stage(c)
        for c in order:
            own_stage(x, c)
        settle("inner")
        for c in range(INNER_CHUNKS):
            wox_wait(c, 1)
            own_stage(other, c)
        for c in range(INNER_CHUNKS, WO_CHUNKS):
            away_wait(c)
        settle_last("inner")

    @pl.when(is_end)
    def _():
        for c in order:
            wo_wait(m, other, c)
            if c < END_CHUNKS:
                wo_cross(m, other, c).start()
            if c >= END_CHUNKS:
                away_stage(c)
        for c in order:
            own_stage(x, c)
        settle("end")
        for c in range(END_CHUNKS):
            wox_wait(c, 2)
            own_stage(other, c)
        for c in range(END_CHUNKS, WO_CHUNKS):
            away_wait(c)
        settle_last("end")

    ruler = wo_buf.at[0, 0 : tok * nx, :]
    pltpu.make_async_copy(ruler, ruler, s_res).wait()


def fused_on_device(nf, nz, nx, hidden, w_query, w_keyvalue, w_output, segment_ids):
    tok, kdim = hidden.shape
    cols = w_output.shape[1]
    rows = tok * nx
    sub = rows // nf
    kvw = w_keyvalue.shape[1]
    heads = nz * nx
    part = cols // nx
    f32, bf16 = jnp.float32, jnp.bfloat16
    dma = pltpu.SemaphoreType.DMA
    vmem = pl.BlockSpec(memory_space=pltpu.VMEM)
    anywhere = pl.BlockSpec(memory_space=pl.ANY)
    scratch = [
        pltpu.VMEM((rows, kdim), bf16),
        pltpu.VMEM((nz // 2, kdim, 2 * HD), bf16),
        pltpu.VMEM((nz * kvw, kdim), bf16),
        pltpu.VMEM((nx, heads * HD, part), bf16),
        pltpu.VMEM((2, nx, 1, tok), jnp.int32),
        pltpu.VMEM((nz, rows, HD), f32),
        pltpu.VMEM((nf // 2, rows, HD), f32),
        pltpu.VMEM((rows, HD), f32),
        pltpu.VMEM((rows, HD), f32),
        pltpu.VMEM((rows, nz * kvw), f32),
        pltpu.VMEM((nf, sub, nz * kvw), f32),
        pltpu.VMEM((sub, HD), bf16),
        pltpu.VMEM((2, nx, rows, HD), bf16),
        pltpu.VMEM((rows, heads * HD), bf16),
        pltpu.VMEM((rows, HD), f32),
        pltpu.VMEM((rows, HD), f32),
        pltpu.VMEM((nx, tok, part), bf16),
        pltpu.VMEM((WO_CHUNKS, tok, part // WO_CHUNKS), bf16),
        pltpu.VMEM((nx, 2, tok // 2, kdim * MOVED // 8), bf16),
        pltpu.VMEM((nz, nx, 2, tok // 2, HD), f32),
        pltpu.VMEM((nf // 2, nx, 2, tok // 2, HD), f32),
        pltpu.VMEM((nx, 2, tok // 2, HD), f32),
        pltpu.VMEM((nx, 2, tok // 2, HD), f32),
        pltpu.VMEM((nx, 2, tok // 2, HD), f32),
        pltpu.VMEM((nx, 2, tok // 2, HD), f32),
        dma((6,)), dma, dma, dma((2,)), dma((2,)), dma((2,)), dma((nz,)), dma((2,)), dma((nz, 2)),
        dma, dma, dma, dma, dma, dma, dma((2,)), dma((2, 5)), dma,
        dma((2,)), dma((nz, nx, WO_CHUNKS)), dma((WO_CHUNKS,)), dma, dma((WO_CHUNKS,)), dma,
        dma((2, 4)),
        dma, dma((WO_CHUNKS,)), dma, dma, dma((nx, 2)), dma,
        dma, dma((nx, 2)), dma, dma((nx, 2)), dma, dma,
    ]
    return pl.pallas_call(
        functools.partial(fused_kernel, nf, nz, nx),
        out_shape=jax.ShapeDtypeStruct((tok, cols), bf16),
        in_specs=[anywhere] * 4 + [vmem],
        out_specs=anywhere,
        scratch_shapes=scratch,
        name="fused_sublayer",
        compiler_params=pltpu.CompilerParams(
            collective_id=0, has_side_effects=True, vmem_limit_bytes=60 * 1024 * 1024
        ),
    )(hidden, w_query, w_keyvalue.T, w_output, segment_ids.reshape(1, tok))


def solution(mesh):
    in_specs = (P("sp", "fsdp"), P("fsdp", "sp"), P("fsdp", "sp"), P("sp", "fsdp"), P("sp"))
    out_specs = P("sp", "fsdp")
    nf, sp = mesh.shape["fsdp"], mesh.shape["sp"]
    if sp == GROUP and sp == 2 * nf:
        body = functools.partial(fused_on_device, nf, nf, sp // nf)
    else:
        body = on_device
    return jax.shard_map(
        body, mesh=mesh, in_specs=in_specs, out_specs=out_specs, check_vma=False
    )
```
